32 devices in a mesh: seq: 8 (over z, y), head: 4 (over x, core).
Axes of the slice: x: 2, y: 2, z: 4, core: 2. Of those that a mesh axis runs over, the one named last changes fastest.
Arguments:
- queries: bfloat16 [2048, 4096], P('seq', 'head'), may hold values from -8 to 8
- self_keys: bfloat16 [2048, 1024], P('seq', 'head'), may hold values from -6 to 6
- self_values: bfloat16 [2048, 1024], P('seq', 'head'), may hold values from -6 to 6
- store_keys: bfloat16 [32768, 1024], P('seq', 'head'), may hold values from -6 to 6
- store_values: bfloat16 [32768, 1024], P('seq', 'head'), may hold values from -6 to 6
- kv_slot: int32 [256], replicated, may hold values from 0 to 255, as said below
- neighbours: int32 [16, 64], P('seq'), may hold values from 0 to 255, as said below
- counts: int32 [16], P('seq'), may hold values from 1 to 64, 96 in all
- out_weight: bfloat16 [4096, 4096], P('head', 'seq'), may hold values from -0.375 to 0.375
Outputs:
- mixed: bfloat16 [2048, 4096], P(('seq', 'head'))
The draws below stay inside these ranges and needn't reach their ends.
Inputs may be any that keep to these rules, and one draw needn't show every extreme that they name: A permutation of the store blocks: block b is stored at slot kv_slot[b], on index kv_slot[b] // 32 of seq. `neighbours`: each row names 64 different store blocks in no particular order; only entries e < counts of the row are listed, the rest is padding. Counting by the index of seq on which a block is stored, each row names exactly 8 blocks on every index, and the 2 rows of one index of seq name the same single block on every index of seq.
All inputs are finite; a program needn't handle non-finite values. No bound on the sum of `counts` on one device may be relied on, other than what follows from the above.
Results may differ from the reference program's by a relative error of at most 0.012.
Values may be sent and summed in bfloat16 or wider, within the bound.
A program may use at most 128 MiB of HBM per device.

```python
import math
import jax
import jax.numpy as jnp
import numpy as np
from jax import lax

D = 4096
H = 32
KVH = 8
DH = 128
BLK = 128
DEG = 64
MEAN_DEG = 6
QB_DEV = 2
KB_DEV = 32
NQB = 16
NKB = 256
TOKENS = 2048
STORE_TOKENS = 32768
CAPQ = 8
CAP = 8
N_SEQ = 8


def graph_tables(key):
    slot_scores = jax.random.randint(jax.random.fold_in(key, 101), (NKB,), 0, 1 << 16) * NKB + jnp.arange(NKB)
    kv_slot = jnp.argsort(slot_scores).astype(jnp.int32)
    stored_at = jnp.argsort(kv_slot).astype(jnp.int32)
    pick_scores = jax.random.randint(jax.random.fold_in(key, 102), (N_SEQ, N_SEQ, KB_DEV), 0, 1 << 16) * KB_DEV + jnp.arange(KB_DEV)
    kept_picks = jnp.argsort(pick_scores, axis=-1)[:, :, :CAP]
    block_ids = jnp.arange(NQB)
    position = block_ids % QB_DEV
    holder = block_ids // QB_DEV
    random_start = jax.random.randint(jax.random.fold_in(key, 103), (NQB, N_SEQ), 0, CAP)
    forced = position * CAPQ
    starting = jnp.where((forced < CAP)[:, None], forced[:, None], random_start)
    offsets = (starting[:, :, None] + jnp.arange(CAPQ)[None, None, :]) % CAP
    within = jnp.take_along_axis(kept_picks[holder], offsets, axis=-1)
    slot_ids = (jnp.arange(N_SEQ)[None, :, None] * KB_DEV + within).reshape(NQB, DEG)
    order_scores = jax.random.randint(jax.random.fold_in(key, 104), (NQB, DEG), 0, 1 << 16) * DEG + jnp.arange(DEG)
    ordering = jnp.argsort(order_scores, axis=-1)
    slot_ids = jnp.take_along_axis(slot_ids, ordering, axis=-1)
    return (kv_slot, stored_at[slot_ids].astype(jnp.int32))


def draw_kv_slot(key, part):
    return graph_tables(key)[0]


def draw_neighbours(key, part):
    return graph_tables(key)[1]


def draw_queries(key, part):
    drawn = 2.0 * jax.random.truncated_normal(jax.random.fold_in(key, 1), -4.0, 4.0, (TOKENS, H * DH), jnp.float32)
    return drawn.astype(jnp.bfloat16)


def draw_self_keys(key, part):
    drawn = jax.random.truncated_normal(jax.random.fold_in(key, 2), -6.0, 6.0, (TOKENS, KVH * DH), jnp.float32)
    return drawn.astype(jnp.bfloat16)


def block_levels(own_key, shape, cuts, low, largest):
    level, own = 1.0, jax.random.fold_in(own_key, 6)
    for axis_at, blocks in cuts:
        steps = jnp.exp(jax.random.uniform(jax.random.fold_in(own, axis_at), (blocks,), jnp.float32, low / len(cuts), largest / len(cuts)))
        level = level * jnp.repeat(steps, shape[axis_at] // blocks).reshape([-1 if axis == axis_at else 1 for axis in range(len(shape))])
    return level


def profile(number_of, total, most, lean):
    loads = [(1 << 20) // math.isqrt(grade ** lean) + 1 for grade in range(2, number_of + 1)]
    spare, given = total - most - (number_of - 1), [1] * (number_of - 1)
    while spare > 0:
        candidates = [i for i in range(number_of - 1) if given[i] < most]
        whole, remaining = sum([loads[i] for i in candidates]), spare
        for i in candidates:
            more = min(most - given[i], max(1, remaining * loads[i] // whole), spare)
            given[i] = given[i] + more
            spare = spare - more
    return np.array([most] + given)


def ragged_sizes(key, count, total, limit, slope):
    if count == 2:
        one = jax.random.randint(key, (), max(1, total - limit), min(limit, total - 1) + 1)
        return jnp.stack([one, total - one])
    sizes = jnp.asarray(profile(count, total, limit, slope), jnp.int32)
    twos = (count - 1) // 2
    giver, sink = sizes[1:1 + 2 * twos:2], sizes[2:2 + 2 * twos:2]
    slack = jnp.minimum(giver - 1, limit - sink)
    moved = jax.random.randint(jax.random.fold_in(key, 1), (twos,), 0, 1 << 20) % (slack + 1)
    sizes = sizes.at[1:1 + 2 * twos:2].set(giver - moved).at[2:2 + 2 * twos:2].set(sink + moved)
    return sizes[jax.random.permutation(jax.random.fold_in(key, 2), count)]


def scatter_about(key, shape, spread, reach, pieces=(), kind=jnp.bfloat16):
    level = block_levels(key, shape, pieces, -0.22, 0.18) if pieces else 1.0
    values = jax.random.normal(key, shape, jnp.float32) * spread * level
    return jnp.minimum(jnp.maximum(values, -reach), reach).astype(kind)


def setup_inputs(seed: int = 0) -> dict:
    arg_keys = jax.random.split(jax.random.key(seed), 10)
    queries = draw_queries(jax.random.fold_in(arg_keys[9], 71), 0)
    self_keys = draw_self_keys(jax.random.fold_in(arg_keys[9], 71), 0)
    self_values = scatter_about(arg_keys[2], (TOKENS, KVH * DH), 1.0, 6.0, ((0, 8), (1, 4)))
    store_keys = scatter_about(arg_keys[3], (STORE_TOKENS, KVH * DH), 1.0, 6.0, ((0, 8), (1, 4)))
    store_values = scatter_about(arg_keys[4], (STORE_TOKENS, KVH * DH), 1.0, 6.0, ((0, 8), (1, 4)))
    kv_slot = draw_kv_slot(jax.random.fold_in(arg_keys[9], 71), 0)
    neighbours = draw_neighbours(jax.random.fold_in(arg_keys[9], 71), 0)
    counts = ragged_sizes(arg_keys[7], NQB, NQB * MEAN_DEG, DEG, 2).astype(jnp.int32)
    out_weight = scatter_about(arg_keys[8], (H * DH, D), (H * DH // 16) ** -0.5, 0.375, ((0, 4), (1, 8)))
    return dict(queries=queries, self_keys=self_keys, self_values=self_values, store_keys=store_keys, store_values=store_values, kv_slot=kv_slot, neighbours=neighbours, counts=counts, out_weight=out_weight)


def reference(queries, self_keys, self_values, store_keys, store_values, kv_slot, neighbours, counts, out_weight):
    per_group = H // KVH
    scaling = DH ** -0.5
    stored_keys = store_keys.reshape(NKB, BLK, KVH, DH)
    stored_values = store_values.reshape(NKB, BLK, KVH, DH)
    query_blocks = queries.reshape(NQB, BLK, KVH, per_group, DH)
    own_keys = self_keys.reshape(NQB, BLK, KVH, DH)
    own_values = self_values.reshape(NQB, BLK, KVH, DH)
    causal = jnp.arange(BLK)[:, None] >= jnp.arange(BLK)[None, :]

    def rounded(weights):
        return lax.optimization_barrier(weights.astype(jnp.bfloat16)).astype(jnp.float32)

    def one_block(bundle):
        query_rows, near_keys, near_values, adjacency, how_many = bundle
        query_wide = query_rows.astype(jnp.float32)

        def scores_of(key_rows):
            return jnp.einsum("tgrd,ugd->grtu", query_wide, key_rows.astype(jnp.float32)) * scaling

        def fetched(entry):
            slot_id = kv_slot[adjacency[entry]]
            return (lax.dynamic_index_in_dim(stored_keys, slot_id, 0, keepdims=False),
                    lax.dynamic_index_in_dim(stored_values, slot_id, 0, keepdims=False))

        nearby = jnp.where(causal, scores_of(near_keys), -jnp.inf)

        def find_highest(entry, highest):
            return jnp.maximum(highest, jnp.max(scores_of(fetched(entry)[0]), axis=-1))

        highest = lax.fori_loop(jnp.int32(0), how_many, find_highest, jnp.max(nearby, axis=-1))
        near_weights = jnp.exp(nearby - highest[..., None])
        start_sum = jnp.einsum("grtu,ugd->grtd", rounded(near_weights), near_values.astype(jnp.float32))

        def accumulate(entry, carry):
            summed, totals = carry
            key_rows, value_rows = fetched(entry)
            weights = jnp.exp(scores_of(key_rows) - highest[..., None])
            summed = summed + jnp.einsum("grtu,ugd->grtd", rounded(weights), value_rows.astype(jnp.float32))
            return summed, totals + jnp.sum(weights, axis=-1)

        summed, totals = lax.fori_loop(jnp.int32(0), how_many, accumulate, (start_sum, jnp.sum(near_weights, axis=-1)))
        result = summed / totals[..., None]
        return jnp.transpose(result, (2, 0, 1, 3)).reshape(BLK, H * DH).astype(jnp.bfloat16)

    attended = lax.map(one_block, (query_blocks, own_keys, own_values, neighbours, counts))
    attended = attended.reshape(NQB * BLK, H * DH)
    return jnp.dot(attended, out_weight, preferred_element_type=jnp.float32).astype(jnp.bfloat16)
```

```python
import functools

import jax
import jax.numpy as jnp
from jax import lax
from jax.experimental import pallas as pl
from jax.experimental.pallas import tpu as pltpu
from jax.sharding import PartitionSpec as P

H = 32
KVH = 8
DH = 128
BLK = 128
NEG = -1e30
STAT = 8
MESH = pl.DeviceIdType.MESH


def part_kernel(
    local_blocks,
    store_blocks,
    slot_ref,
    near_ref,
    count_ref,
    q_ref,
    sk_ref,
    sv_ref,
    k_ref,
    v_ref,
    o_ref,
    lse_ref,
    list_ref,
    acc_ref,
    max_ref,
    sum_ref,
):
    block = pl.program_id(0)
    me = lax.axis_index("seq")
    per_group = H // KVH
    kv_here = k_ref.shape[1] // DH
    rows = per_group * BLK
    scaling = DH ** (-0.5)

    def scan_entry(e, found):
        slot = slot_ref[near_ref[block, e]]
        list_ref[found] = lax.rem(slot, store_blocks)
        return found + (slot // store_blocks == me).astype(jnp.int32)

    found = lax.fori_loop(0, count_ref[block], scan_entry, jnp.int32(0))
    home = block // local_blocks == me

    @pl.when(jnp.logical_and(found == 0, jnp.logical_not(home)))
    def _():
        o_ref[...] = jnp.zeros_like(o_ref)
        lse_ref[...] = jnp.full_like(lse_ref, NEG)

    @pl.when(jnp.logical_or(found > 0, home))
    def _():
        def group_queries(g):
            return jnp.concatenate(
                [q_ref[:, (g * per_group + r) * DH : (g * per_group + r + 1) * DH] for r in range(per_group)],
                axis=0,
            )

        def scores_of(g, keys):
            return (
                lax.dot_general(
                    group_queries(g), keys, (((1,), (1,)), ((), ())), preferred_element_type=jnp.float32
                )
                * scaling
            )

        @pl.when(home)
        def _():
            start = pl.multiple_of(lax.rem(block, local_blocks) * BLK, BLK)
            position = lax.rem(lax.broadcasted_iota(jnp.int32, (rows, BLK), 0), BLK)
            causal = position >= lax.broadcasted_iota(jnp.int32, (rows, BLK), 1)
            for g in range(kv_here):
                cols = slice(g * DH, (g + 1) * DH)
                s = jnp.where(causal, scores_of(g, sk_ref[pl.ds(start, BLK), cols]), NEG)
                m = jnp.max(s, axis=-1, keepdims=True)
                p = jnp.exp(s - m)
                max_ref[g] = jnp.broadcast_to(m, (rows, BLK))
                sum_ref[g] = jnp.broadcast_to(jnp.sum(p, axis=-1, keepdims=True), (rows, BLK))
                acc_ref[g] = jnp.dot(
                    p.astype(jnp.bfloat16), sv_ref[pl.ds(start, BLK), cols], preferred_element_type=jnp.float32
                )

        @pl.when(jnp.logical_not(home))
        def _():
            max_ref[...] = jnp.full_like(max_ref, NEG)
            sum_ref[...] = jnp.zeros_like(sum_ref)
            acc_ref[...] = jnp.zeros_like(acc_ref)

        @pl.loop(0, found)
        def _(i):
            start = pl.multiple_of(list_ref[i] * BLK, BLK)
            for g in range(kv_here):
                cols = slice(g * DH, (g + 1) * DH)
                s = scores_of(g, k_ref[pl.ds(start, BLK), cols])
                old = max_ref[g]
                new = jnp.maximum(old, jnp.max(s, axis=-1, keepdims=True))
                p = jnp.exp(s - new)
                shrink = jnp.exp(old - new)
                max_ref[g] = new
                sum_ref[g] = sum_ref[g] * shrink + jnp.sum(p, axis=-1, keepdims=True)
                acc_ref[g] = acc_ref[g] * shrink + jnp.dot(
                    p.astype(jnp.bfloat16), v_ref[pl.ds(start, BLK), cols], preferred_element_type=jnp.float32
                )

        lane = lax.broadcasted_iota(jnp.int32, (BLK, BLK), 1)
        for g in range(kv_here):
            total = sum_ref[g]
            normal = (acc_ref[g] / total).astype(jnp.bfloat16)
            lse = max_ref[g] + jnp.log(total)
            tile = jnp.full((BLK, BLK), NEG, jnp.float32)
            for r in range(per_group):
                o_ref[0, g, :, r * DH : (r + 1) * DH] = normal[r * BLK : (r + 1) * BLK]
                tile = jnp.where(lane == r, lse[r * BLK : (r + 1) * BLK], tile)
            lse_ref[0, g] = jnp.transpose(tile)[:STAT]


def ring_place(index, n):
    odd = lax.rem(index, 2)
    half = index // 2
    return (1 - odd) * half + odd * (n - 1 - half)


def ring_index(place, n):
    place = lax.rem(place + 2 * n, n)
    far = place // (n // 2)
    return (1 - far) * (2 * place) + far * (2 * (n - 1 - place) + 1)


def gather_kernel(n, pieces, with_table, *refs):
    if with_table:
        x_ref, table_ref, out_ref, tables_ref, own_sem, send_sem, recv_sem, tsend_sem, trecv_sem = refs
    else:
        x_ref, out_ref, own_sem, send_sem, recv_sem = refs
    me = lax.axis_index("seq")
    place = ring_place(me, n)
    rows = x_ref.shape[0]
    sub = rows // pieces
    half = n // 2
    ways = (1, -1)
    beside = [ring_index(place + way, n) for way in ways]
    barrier = pltpu.get_barrier_semaphore()
    if with_table:
        for k in range(1, n):
            pl.semaphore_signal(barrier, inc=1, device_id={"seq": lax.rem(me + k, n)}, device_id_type=MESH)
    else:
        for other in beside:
            pl.semaphore_signal(barrier, inc=1, device_id={"seq": other}, device_id_type=MESH)
    own = pltpu.make_async_copy(x_ref, out_ref.at[pl.ds(pl.multiple_of(me * rows, rows), rows)], own_sem.at[0])
    own.start()
    pl.semaphore_wait(barrier, n - 1 if with_table else 2)

    def copy(way, step, piece):
        owner = ring_index(place - ways[way] * step, n)
        there = pl.ds(pl.multiple_of(owner * rows + piece * sub, sub), sub)
        source = x_ref.at[pl.ds(piece * sub, sub)] if step == 0 else out_ref.at[there]
        return pltpu.make_async_remote_copy(
            src_ref=source,
            dst_ref=out_ref.at[there],
            send_sem=send_sem.at[way, step, piece],
            recv_sem=recv_sem.at[way, step, piece],
            device_id={"seq": beside[way]},
            device_id_type=MESH,
        )

    table_copies = []
    if with_table:
        tables_ref[pl.ds(me, 1)] = table_ref[...][None]
        for k in range(1, n):
            table_copies.append(
                pltpu.make_async_remote_copy(
                    src_ref=table_ref,
                    dst_ref=tables_ref.at[me],
                    send_sem=tsend_sem.at[k],
                    recv_sem=trecv_sem.at[k],
                    device_id={"seq": lax.rem(me + k, n)},
                    device_id_type=MESH,
                )
            )
        for one in table_copies:
            one.start()
    started = []
    for step in range(half):
        for spot in range(pieces):
            for way in range(2):
                piece = spot if way == 0 else pieces - 1 - spot
                if step > 0:
                    copy(way, step - 1, piece).wait_recv()
                if step < half - 1 or spot < pieces // 2:
                    one = copy(way, step, piece)
                    one.start()
                    started.append(one)
    for spot in range(pieces // 2):
        for way in range(2):
            copy(way, half - 1, spot if way == 0 else pieces - 1 - spot).wait_recv()
    for one in started:
        one.wait_send()
    for one in table_copies:
        one.wait()
    own.wait()


def gathered(x, n, pieces, number, table=None):
    rows, width = x.shape
    with_table = table is not None
    vmem = pl.BlockSpec(memory_space=pltpu.VMEM)
    out_shape = [jax.ShapeDtypeStruct((n * rows, width), x.dtype)]
    scratch = [
        pltpu.SemaphoreType.DMA((1,)),
        pltpu.SemaphoreType.DMA((2, n // 2, pieces)),
        pltpu.SemaphoreType.DMA((2, n // 2, pieces)),
    ]
    if with_table:
        out_shape.append(jax.ShapeDtypeStruct((n,) + table.shape, table.dtype))
        scratch += [pltpu.SemaphoreType.DMA((n,)), pltpu.SemaphoreType.DMA((n,))]
    return pl.pallas_call(
        functools.partial(gather_kernel, n, pieces, with_table),
        in_specs=[vmem] * (1 + with_table),
        out_specs=[vmem] * (1 + with_table),
        out_shape=out_shape,
        scratch_shapes=scratch,
        compiler_params=pltpu.CompilerParams(
            collective_id=number, has_side_effects=True, vmem_limit_bytes=50 << 20
        ),
    )(*([x, table] if with_table else [x]))


def merge(lse_a, lse_b):
    top = jnp.maximum(lse_a, lse_b)
    a = jnp.exp(lse_a - top)
    b = jnp.exp(lse_b - top)
    total = a + b
    both = jnp.concatenate([a / total, b / total, jnp.zeros((BLK - 2 * STAT, BLK), jnp.float32)], axis=0)
    return jnp.transpose(both), top + jnp.log(total)


def reduce_kernel(n, o_ref, lse_ref, out_ref, got, got_lse, own, own_sem, send_sem, recv_sem, lsend_sem, lrecv_sem):
    me = lax.axis_index("seq")
    place = ring_place(me, n)
    groups, width = got.shape[2], got.shape[4]
    ways = (1, -1)
    beside = [ring_index(place + way, n) for way in ways]
    barrier = pltpu.get_barrier_semaphore()
    for other in beside:
        pl.semaphore_signal(barrier, inc=1, device_id={"seq": other}, device_id_type=MESH)

    def home(way, step):
        return ring_index(place - ways[way] * (1 + step), n)

    def fetch(way, step):
        return pltpu.make_async_copy(
            o_ref.at[home(way, step) * 2 + way], own.at[way, lax.rem(step, 2)], own_sem.at[way, lax.rem(step, 2)]
        )

    def copies(way, step, g, before):
        at = home(way, step) * 2 + way
        first = before is None
        return (
            pltpu.make_async_remote_copy(
                src_ref=lse_ref.at[at, g] if first else got_lse.at[way, before, g],
                dst_ref=got_lse.at[way, step, g],
                send_sem=lsend_sem.at[way, step, g],
                recv_sem=lrecv_sem.at[way, step, g],
                device_id={"seq": beside[way]},
                device_id_type=MESH,
            ),
            pltpu.make_async_remote_copy(
                src_ref=o_ref.at[at, g] if first else got.at[way, before, g],
                dst_ref=got.at[way, step, g],
                send_sem=send_sem.at[way, step, g],
                recv_sem=recv_sem.at[way, step, g],
                device_id={"seq": beside[way]},
                device_id_type=MESH,
            ),
        )

    def merged(way, step, g):
        for one in copies(way, step - 1, g, step - 1):
            one.wait_recv()
        if g == 0:
            fetch(way, step).wait()
        at = home(way, step) * 2 + way
        shares, lse = merge(got_lse[way, step - 1, g], lse_ref[at, g])
        columns = []
        for r in range(width // DH):
            cols = slice(r * DH, (r + 1) * DH)
            columns.append(
                got[way, step - 1, g, :, cols].astype(jnp.float32) * shares[:, r : r + 1]
                + own[way, lax.rem(step, 2), g, :, cols].astype(jnp.float32) * shares[:, STAT + r : STAT + r + 1]
            )
        return columns, lse

    for way in range(2):
        fetch(way, 1).start()
    pl.semaphore_wait(barrier, 2)
    for g in range(groups):
        for way in range(2):
            for one in copies(way, 0, g, None):
                one.start()

    def one_step(step, carry):
        for way in range(2):
            fetch(way, step + 1).start()
        for g in range(groups):
            for way in range(2):
                columns, lse = merged(way, step, g)
                got_lse[way, step - 1, g] = lse
                for r, value in enumerate(columns):
                    got[way, step - 1, g, :, r * DH : (r + 1) * DH] = value.astype(jnp.bfloat16)
            for way in range(2):
                for one in copies(way, step, g, step - 1):
                    one.start()
        return carry

    lax.fori_loop(1, n - 1, one_step, 0)
    for g in range(groups):
        for way in range(2):
            columns, _ = merged(way, n - 1, g)
            for r, value in enumerate(columns):
                at = g * width + r * DH
                out_ref[way * BLK : (way + 1) * BLK, at : at + DH] = value.astype(jnp.bfloat16)
    for g in range(groups):
        for way in range(2):
            for one in copies(way, 0, g, None):
                one.wait_send()

    def drain(step, carry):
        for g in range(groups):
            for way in range(2):
                for one in copies(way, step, g, step - 1):
                    one.wait_send()
        return carry

    lax.fori_loop(1, n - 1, drain, 0)


def project_kernel(
    n,
    heads,
    pieces,
    x_ref,
    w_hbm,
    out_ref,
    w_ref,
    blocks,
    split,
    got,
    summed,
    landed,
    w_sem,
    send_sem,
    recv_sem,
    hsend,
    hrecv,
    fsend,
    frecv,
):
    me = lax.axis_index("seq")
    mine = lax.axis_index("head")
    place = ring_place(me, n)
    rows = x_ref.shape[0]
    sub = rows // pieces
    share = rows // heads
    columns = w_ref.shape[1]
    half = n // 2
    ways = (1, -1)
    beside = [ring_index(place + way, n) for way in ways]
    weights = pltpu.make_async_copy(w_hbm, w_ref, w_sem.at[0])
    weights.start()
    barrier = pltpu.get_barrier_semaphore()
    for k in range(1, heads):
        pl.semaphore_signal(barrier, inc=1, device_id={"head": lax.rem(mine + k, heads)}, device_id_type=MESH)
    for k in range(1, n):
        pl.semaphore_signal(barrier, inc=1, device_id={"seq": lax.rem(me + k, n)}, device_id_type=MESH)
    pl.semaphore_wait(barrier, heads + n - 2)

    def owner_of(way, step):
        return ring_index(place - ways[way] * step, n)

    def copy(way, step, piece, first):
        there = (owner_of(way, step), pl.ds(piece * sub, sub))
        return pltpu.make_async_remote_copy(
            src_ref=x_ref.at[pl.ds(piece * sub, sub)] if first else blocks.at[there],
            dst_ref=blocks.at[there],
            send_sem=send_sem.at[way, step, piece],
            recv_sem=recv_sem.at[way, step, piece],
            device_id={"seq": beside[way]},
            device_id_type=MESH,
        )

    def to_head(i, k):
        to = lax.rem(mine + k, heads)
        return pltpu.make_async_remote_copy(
            src_ref=split.at[i, to],
            dst_ref=got.at[i, k],
            send_sem=hsend.at[i, k],
            recv_sem=hrecv.at[i, k],
            device_id={"head": to},
            device_id_type=MESH,
        )

    def to_row(k):
        to = lax.rem(me + k, n)
        return pltpu.make_async_remote_copy(
            src_ref=summed.at[to],
            dst_ref=landed.at[me],
            send_sem=fsend.at[k],
            recv_sem=frecv.at[k],
            device_id={"seq": to},
            device_id_type=MESH,
        )

    def multiply(i, piece, value):
        product = jnp.dot(value, w_ref[...], preferred_element_type=jnp.float32).astype(jnp.bfloat16)
        for s in range(sub // share):
            split[i, piece * (sub // share) + s] = product[s * share : (s + 1) * share]

    def give(i):
        for k in range(1, heads):
            to_head(i, k).start()

    def total_of(i):
        total = split[i, mine].astype(jnp.float32)
        for k in range(1, heads):
            to_head(i, k).wait_recv()
            total = total + got[i, k].astype(jnp.float32)
        return total.astype(jnp.bfloat16)

    def settle(i):
        summed[i] = total_of(i)
        to_row(lax.rem(i - me + n, n)).start()

    for spot in range(pieces):
        for way in range(2):
            copy(way, 0, spot if way == 0 else pieces - 1 - spot, True).start()
    weights.wait()
    for piece in range(pieces):
        multiply(me, piece, x_ref[piece * sub : (piece + 1) * sub])
    give(me)

    def take(way, step, piece, forward):
        copy(way, step - 1, piece, False).wait_recv()
        if forward:
            copy(way, step, piece, False).start()
        i = owner_of(way, step)
        multiply(i, piece, blocks[i, piece * sub : (piece + 1) * sub])

    def one_step(step, last):
        for spot in range(pieces):
            for way in range(2):
                take(way, step, spot if way == 0 else pieces - 1 - spot, not last or spot < pieces // 2)
        for way in range(2):
            give(owner_of(way, step))

    one_step(1, half == 2)
    landed[me] = total_of(me)

    def middle(step, carry):
        one_step(step, False)
        for way in range(2):
            settle(owner_of(way, step - 1))
        return carry

    lax.fori_loop(2, half - 1, middle, 0)
    if half > 2:
        one_step(half - 1, True)
        for way in range(2):
            settle(owner_of(way, half - 2))
    for spot in range(pieces // 2):
        for way in range(2):
            take(way, half, spot if way == 0 else pieces - 1 - spot, False)
    give(owner_of(0, half))
    for way in range(2):
        settle(owner_of(way, half - 1))
    settle(owner_of(0, half))

    for spot in range(pieces):
        for way in range(2):
            copy(way, 0, spot if way == 0 else pieces - 1 - spot, True).wait_send()

    def drain(step, carry):
        for piece in range(pieces):
            for way in range(2):
                copy(way, step, piece, False).wait_send()
        return carry

    lax.fori_loop(1, half - 1, drain, 0)
    if half > 1:
        for spot in range(pieces // 2):
            for way in range(2):
                copy(way, half - 1, spot if way == 0 else pieces - 1 - spot, False).wait_send()

    def drain_heads(i, carry):
        for k in range(1, heads):
            to_head(i, k).wait_send()
        return carry

    lax.fori_loop(0, n, drain_heads, 0)
    for k in range(1, n):
        to_row(k).wait()
    for i in range(n):
        out_ref[:, i * columns : (i + 1) * columns] = landed[i]


def projected(x, weight, n, heads, pieces):
    rows, width = x.shape
    columns = weight.shape[1]
    share = rows // heads
    vmem = pl.BlockSpec(memory_space=pltpu.VMEM)
    dma = pltpu.SemaphoreType.DMA
    return pl.pallas_call(
        functools.partial(project_kernel, n, heads, pieces),
        in_specs=[vmem, pl.BlockSpec(memory_space=pl.ANY)],
        out_specs=vmem,
        out_shape=jax.ShapeDtypeStruct((share, n * columns), x.dtype),
        scratch_shapes=[
            pltpu.VMEM(weight.shape, weight.dtype),
            pltpu.VMEM((n, rows, width), x.dtype),
            pltpu.VMEM((n, heads, share, columns), x.dtype),
            pltpu.VMEM((n, heads, share, columns), x.dtype),
            pltpu.VMEM((n, share, columns), x.dtype),
            pltpu.VMEM((n, share, columns), x.dtype),
            dma((1,)),
            dma((2, n // 2, pieces)),
            dma((2, n // 2, pieces)),
            dma((n, heads)),
            dma((n, heads)),
            dma((n,)),
            dma((n,)),
        ],
        compiler_params=pltpu.CompilerParams(
            collective_id=2, has_side_effects=True, vmem_limit_bytes=56 << 20
        ),
    )(x, weight)


def body(
    queries,
    self_keys,
    self_values,
    store_keys,
    store_values,
    kv_slot,
    neighbours,
    counts,
    out_weight,
):
    n = lax.axis_size("seq")
    head_count = lax.axis_size("head")
    local_blocks, degree = neighbours.shape
    local_rows, width = queries.shape
    store_blocks = store_keys.shape[0] // BLK
    all_blocks = local_blocks * n
    kv_here = store_keys.shape[1] // DH
    group_width = (H // KVH) * DH
    rows = (H // KVH) * BLK
    table = jnp.concatenate([neighbours, counts[:, None]], axis=1)
    table = jnp.pad(table, ((0, 8 - local_blocks), (0, 2 * BLK - table.shape[1] - BLK)))
    all_queries, tables = gathered(queries, n, 2, 0, table)
    near = tables[:, :local_blocks, :degree].reshape(all_blocks, degree)
    count = tables[:, :local_blocks, degree].reshape(all_blocks)
    smem = pl.BlockSpec(memory_space=pltpu.SMEM)

    def whole(a):
        return pl.BlockSpec(a.shape, lambda i: (0, 0))

    parts, lse = pl.pallas_call(
        functools.partial(part_kernel, local_blocks, store_blocks),
        grid=(all_blocks,),
        in_specs=[smem, smem, smem, pl.BlockSpec((BLK, width), lambda i: (i, 0))]
        + [whole(a) for a in (self_keys, self_values, store_keys, store_values)],
        out_specs=[
            pl.BlockSpec((1, kv_here, BLK, group_width), lambda i: (i, 0, 0, 0)),
            pl.BlockSpec((1, kv_here, STAT, BLK), lambda i: (i, 0, 0, 0)),
        ],
        out_shape=[
            jax.ShapeDtypeStruct((all_blocks, kv_here, BLK, group_width), jnp.bfloat16),
            jax.ShapeDtypeStruct((all_blocks, kv_here, STAT, BLK), jnp.float32),
        ],
        scratch_shapes=[
            pltpu.SMEM((degree + 1,), jnp.int32),
            pltpu.VMEM((kv_here, rows, DH), jnp.float32),
            pltpu.VMEM((kv_here, rows, BLK), jnp.float32),
            pltpu.VMEM((kv_here, rows, BLK), jnp.float32),
        ],
        compiler_params=pltpu.CompilerParams(vmem_limit_bytes=40 << 20),
        cost_estimate=pl.CostEstimate(flops=2_000_000_000, bytes_accessed=12 << 20, transcendentals=4_000_000),
    )(kv_slot, near, count, all_queries, self_keys, self_values, store_keys, store_values)
    dma = pltpu.SemaphoreType.DMA((2, n - 1, kv_here))
    attended = pl.pallas_call(
        functools.partial(reduce_kernel, n),
        in_specs=[pl.BlockSpec(memory_space=pl.ANY), pl.BlockSpec(memory_space=pltpu.VMEM)],
        out_specs=pl.BlockSpec(memory_space=pltpu.VMEM),
        out_shape=jax.ShapeDtypeStruct((local_rows, width), jnp.bfloat16),
        scratch_shapes=[
            pltpu.VMEM((2, n - 1, kv_here, BLK, group_width), jnp.bfloat16),
            pltpu.VMEM((2, n - 1, kv_here, STAT, BLK), jnp.float32),
            pltpu.VMEM((2, 2, kv_here, BLK, group_width), jnp.bfloat16),
            pltpu.SemaphoreType.DMA((2, 2)),
            dma,
            dma,
            dma,
            dma,
        ],
        compiler_params=pltpu.CompilerParams(
            collective_id=1, has_side_effects=True, vmem_limit_bytes=50 << 20
        ),
    )(parts, lse)
    return projected(attended, out_weight, n, head_count, 2)


def solution(mesh):
    placed = (
        P("seq", "head"),
        P("seq", "head"),
        P("seq", "head"),
        P("seq", "head"),
        P("seq", "head"),
        P(),
        P("seq", None),
        P("seq"),
        P("head", "seq"),
    )
    return jax.shard_map(
        body, mesh=mesh, in_specs=placed, out_specs=P(("seq", "head"), None), check_vma=False
    )
```

```python
import functools

import jax
import jax.numpy as jnp
from jax import lax
from jax.experimental import pallas as pl
from jax.experimental.pallas import tpu as pltpu
from jax.sharding import PartitionSpec as P

H = 32
KVH = 8
DH = 128
BLK = 128
NEG = -1e30
STAT = 8
LOG2E = 1.4426950408889634
MESH = pl.DeviceIdType.MESH


def part_kernel(
    local_blocks,
    store_blocks,
    small,
    slot_ref,
    near_ref,
    count_ref,
    q_ref,
    sk_ref,
    sv_ref,
    k_ref,
    v_ref,
    o_ref,
    lse_ref,
    list_ref,
    acc_ref,
    max_ref,
    sum_ref,
):
    block = pl.program_id(0)
    me = lax.axis_index("seq")
    per_group = H // KVH
    kv_here = k_ref.shape[1] // DH
    rows = per_group * BLK
    scaling = DH ** (-0.5) * LOG2E
    here = block if small else 0
    owner, inner = block // local_blocks, lax.rem(block, local_blocks)
    first_row = pl.multiple_of(block * BLK, BLK) if small else 0

    def scan_entry(e, found):
        slot = slot_ref[near_ref[owner, inner, e]]
        list_ref[found] = lax.rem(slot, store_blocks)
        return found + (slot // store_blocks == me).astype(jnp.int32)

    found = lax.fori_loop(0, count_ref[owner, 0, inner], scan_entry, jnp.int32(0))
    home = block // local_blocks == me

    @pl.when(jnp.logical_and(found == 0, jnp.logical_not(home)))
    def _():
        o_ref[here] = jnp.zeros(o_ref.shape[1:], o_ref.dtype)
        lse_ref[here] = jnp.full(lse_ref.shape[1:], NEG, lse_ref.dtype)

    @pl.when(jnp.logical_or(found > 0, home))
    def _():
        def scores_of(g, keys):
            asked = jnp.concatenate(
                [
                    q_ref[pl.ds(first_row, BLK), (g * per_group + r) * DH : (g * per_group + r + 1) * DH]
                    for r in range(per_group)
                ],
                axis=0,
            )
            return (
                lax.dot_general(keys, asked, (((1,), (1,)), ((), ())), preferred_element_type=jnp.float32)
                * scaling
            )

        def weighed(values, p):
            return lax.dot_general(
                values, p.astype(jnp.bfloat16), (((0,), (0,)), ((), ())), preferred_element_type=jnp.float32
            )

        @pl.when(home)
        def _():
            start = pl.multiple_of(lax.rem(block, local_blocks) * BLK, BLK)
            position = lax.rem(lax.broadcasted_iota(jnp.int32, (BLK, rows), 1), BLK)
            causal = position >= lax.broadcasted_iota(jnp.int32, (BLK, rows), 0)
            for g in range(kv_here):
                cols = slice(g * DH, (g + 1) * DH)
                s = jnp.where(causal, scores_of(g, sk_ref[pl.ds(start, BLK), cols]), NEG)
                m = jnp.max(s, axis=0, keepdims=True)
                p = jnp.exp2(s - m)
                max_ref[g : g + 1] = m
                sum_ref[g : g + 1] = jnp.sum(p, axis=0, keepdims=True)
                acc_ref[g] = weighed(sv_ref[pl.ds(start, BLK), cols], p)

        @pl.when(jnp.logical_not(home))
        def _():
            max_ref[...] = jnp.full_like(max_ref, NEG)
            sum_ref[...] = jnp.zeros_like(sum_ref)
            acc_ref[...] = jnp.zeros_like(acc_ref)

        @pl.loop(0, found)
        def _(i):
            start = pl.multiple_of(list_ref[i] * BLK, BLK)
            for g in range(kv_here):
                cols = slice(g * DH, (g + 1) * DH)
                s = scores_of(g, k_ref[pl.ds(start, BLK), cols])
                old = max_ref[g : g + 1]
                new = jnp.maximum(old, jnp.max(s, axis=0, keepdims=True))
                p = jnp.exp2(s - new)
                shrink = jnp.exp2(old - new)
                max_ref[g : g + 1] = new
                sum_ref[g : g + 1] = sum_ref[g : g + 1] * shrink + jnp.sum(p, axis=0, keepdims=True)
                acc_ref[g] = acc_ref[g] * shrink + weighed(v_ref[pl.ds(start, BLK), cols], p)

        for g in range(kv_here):
            total = sum_ref[g : g + 1]
            lse = max_ref[g : g + 1] + jnp.log2(total)
            o_ref[here, g] = (acc_ref[g] * (1.0 / total)).astype(jnp.bfloat16)
            for r in range(STAT):
                at = (r % per_group) * BLK
                lse_ref[here, g, r : r + 1] = lse[:, at : at + BLK]


def grant(*arrays):
    size = 0
    for shape, dtype in arrays:
        cells = 1
        for d in shape:
            cells = cells * d
        size += cells * jnp.dtype(dtype).itemsize
    return min(size + (4 << 20), 60 << 20)


def long_cost():
    return pl.CostEstimate(flops=200_000_000_000, bytes_accessed=1 << 20, transcendentals=0)


def ring_place(index, n):
    odd = lax.rem(index, 2)
    half = index // 2
    return (1 - odd) * half + odd * (n - 1 - half)


def ring_index(place, n):
    place = lax.rem(place + 2 * n, n)
    far = place // (n // 2)
    return (1 - far) * (2 * place) + far * (2 * (n - 1 - place) + 1)


def gather_kernel(
    n,
    pieces,
    x_ref,
    near_ref,
    count_ref,
    out_ref,
    nears_ref,
    counts_ref,
    own_sem,
    send_sem,
    recv_sem,
    tsend_sem,
    trecv_sem,
):
    me = lax.axis_index("seq")
    place = ring_place(me, n)
    rows = x_ref.shape[0]
    sub = rows // pieces
    half = n // 2
    ways = (1, -1)
    beside = [ring_index(place + way, n) for way in ways]
    own = [
        pltpu.make_async_copy(source, target, own_sem.at[i])
        for i, (source, target) in enumerate(
            (
                (x_ref, out_ref.at[pl.ds(pl.multiple_of(me * rows, rows), rows)]),
                (near_ref, nears_ref.at[me]),
                (count_ref, counts_ref.at[me]),
            )
        )
    ]
    for one in own:
        one.start()
    barrier = pltpu.get_barrier_semaphore()
    for k in range(1, n):
        pl.semaphore_signal(barrier, inc=1, device_id={"seq": lax.rem(me + k, n)}, device_id_type=MESH)
    for one in own:
        one.wait()
    pl.semaphore_wait(barrier, n - 1)

    def copy(way, step, piece):
        owner = ring_index(place - ways[way] * step, n)
        there = pl.ds(pl.multiple_of(owner * rows + piece * sub, sub), sub)
        return pltpu.make_async_remote_copy(
            src_ref=out_ref.at[there],
            dst_ref=out_ref.at[there],
            send_sem=send_sem.at[way, step, piece],
            recv_sem=recv_sem.at[way, step, piece],
            device_id={"seq": beside[way]},
            device_id_type=MESH,
        )

    started = []
    for spot in range(pieces):
        for way in range(2):
            one = copy(way, 0, spot if way == 0 else pieces - 1 - spot)
            one.start()
            started.append(one)
    table_copies = []
    for t, target in enumerate((nears_ref, counts_ref)):
        for k in range(1, n):
            table_copies.append(
                pltpu.make_async_remote_copy(
                    src_ref=target.at[me],
                    dst_ref=target.at[me],
                    send_sem=tsend_sem.at[t, k],
                    recv_sem=trecv_sem.at[t, k],
                    device_id={"seq": lax.rem(me + k, n)},
                    device_id_type=MESH,
                )
            )
    for one in table_copies:
        one.start()
    for step in range(1, half):
        for spot in range(pieces):
            for way in range(2):
                piece = spot if way == 0 else pieces - 1 - spot
                copy(way, step - 1, piece).wait_recv()
                if step < half - 1 or spot < pieces // 2:
                    one = copy(way, step, piece)
                    one.start()
                    started.append(one)
    for spot in range(pieces // 2):
        for way in range(2):
            copy(way, half - 1, spot if way == 0 else pieces - 1 - spot).wait_recv()
    for one in started:
        one.wait_send()
    for one in table_copies:
        one.wait()


def gathered(x, near, count, n, pieces):
    rows, width = x.shape
    vmem = pl.BlockSpec(memory_space=pltpu.VMEM)
    size = n * rows * width * x.dtype.itemsize
    kind = pltpu.VMEM if size <= 8 << 20 else jax.ShapeDtypeStruct
    return pl.pallas_call(
        functools.partial(gather_kernel, n, pieces),
        in_specs=[pl.BlockSpec(memory_space=pltpu.HBM)] * 3,
        out_specs=[vmem] * 3,
        out_shape=[
            kind((n * rows, width), x.dtype),
            jax.ShapeDtypeStruct((n,) + near.shape, near.dtype),
            jax.ShapeDtypeStruct((n,) + count.shape, count.dtype),
        ],
        scratch_shapes=[
            pltpu.SemaphoreType.DMA((3,)),
            pltpu.SemaphoreType.DMA((2, n // 2, pieces)),
            pltpu.SemaphoreType.DMA((2, n // 2, pieces)),
            pltpu.SemaphoreType.DMA((2, n)),
            pltpu.SemaphoreType.DMA((2, n)),
        ],
        compiler_params=pltpu.CompilerParams(
            collective_id=0,
            has_side_effects=True,
            vmem_limit_bytes=grant((x.shape, x.dtype), ((n * rows, width), x.dtype)),
        ),
        cost_estimate=long_cost(),
    )(x, near, count)


def merge(lse_a, lse_b):
    top = jnp.maximum(lse_a, lse_b)
    a = jnp.exp2(lse_a - top)
    b = jnp.exp2(lse_b - top)
    total = a + b
    return a / total, b / total, top + jnp.log2(total)


def reduce_kernel(
    n, small, o_ref, lse_ref, out_ref, got, got_lse, own, own_sem, send_sem, recv_sem, lsend_sem, lrecv_sem
):
    me = lax.axis_index("seq")
    place = ring_place(me, n)
    groups, width = got.shape[2], got.shape[4]
    ways = (1, -1)
    beside = [ring_index(place + way, n) for way in ways]
    barrier = pltpu.get_barrier_semaphore()
    for other in beside:
        pl.semaphore_signal(barrier, inc=1, device_id={"seq": other}, device_id_type=MESH)

    def home(way, step):
        return ring_index(place - ways[way] * (1 + step), n)

    def fetch(way, step):
        return pltpu.make_async_copy(
            o_ref.at[home(way, step) * 2 + way], own.at[way, lax.rem(step, 2)], own_sem.at[way, lax.rem(step, 2)]
        )

    def copies(way, step, g, before):
        at = home(way, step) * 2 + way
        first = before is None
        return (
            pltpu.make_async_remote_copy(
                src_ref=lse_ref.at[at, g] if first else got_lse.at[way, before, g],
                dst_ref=got_lse.at[way, step, g],
                send_sem=lsend_sem.at[way, step, g],
                recv_sem=lrecv_sem.at[way, step, g],
                device_id={"seq": beside[way]},
                device_id_type=MESH,
            ),
            pltpu.make_async_remote_copy(
                src_ref=o_ref.at[at, g] if first else got.at[way, before, g],
                dst_ref=got.at[way, step, g],
                send_sem=send_sem.at[way, step, g],
                recv_sem=recv_sem.at[way, step, g],
                device_id={"seq": beside[way]},
                device_id_type=MESH,
            ),
        )

    def merged(way, step, g):
        for one in copies(way, step - 1, g, step - 1):
            one.wait_recv()
        if g == 0 and not small:
            fetch(way, step).wait()
        at = home(way, step) * 2 + way
        theirs, ours, lse = merge(got_lse[way, step - 1, g], lse_ref[at, g])
        columns = []
        for r in range(width // DH):
            cols = slice(r * DH, (r + 1) * DH)
            mine = o_ref[at, g, :, cols] if small else own[way, lax.rem(step, 2), g, :, cols]
            columns.append(
                got[way, step - 1, g, :, cols].astype(jnp.float32) * theirs[r : r + 1]
                + mine.astype(jnp.float32) * ours[r : r + 1]
            )
        return columns, lse

    if not small:
        for way in range(2):
            fetch(way, 1).start()
    pl.semaphore_wait(barrier, 2)
    for g in range(groups):
        for way in range(2):
            for one in copies(way, 0, g, None):
                one.start()

    def one_step(step, carry):
        if not small:
            for way in range(2):
                fetch(way, step + 1).start()
        for g in range(groups):
            for way in range(2):
                columns, lse = merged(way, step, g)
                got_lse[way, step - 1, g] = lse
                for r, value in enumerate(columns):
                    got[way, step - 1, g, :, r * DH : (r + 1) * DH] = value.astype(jnp.bfloat16)
                for one in copies(way, step, g, step - 1):
                    one.start()
        return carry

    lax.fori_loop(1, n - 1, one_step, 0)
    for g in range(groups):
        for way in range(2):
            columns, _ = merged(way, n - 1, g)
            for r, value in enumerate(columns):
                at = g * width + r * DH
                out_ref[way * BLK : (way + 1) * BLK, at : at + DH] = jnp.transpose(value).astype(jnp.bfloat16)
    for g in range(groups):
        for way in range(2):
            for one in copies(way, 0, g, None):
                one.wait_send()

    def drain(step, carry):
        for g in range(groups):
            for way in range(2):
                for one in copies(way, step, g, step - 1):
                    one.wait_send()
        return carry

    lax.fori_loop(1, n - 1, drain, 0)


def project_kernel(
    n,
    heads,
    pieces,
    x_ref,
    w_hbm,
    out_ref,
    w_ref,
    blocks,
    split,
    got,
    summed,
    landed,
    w_sem,
    send_sem,
    recv_sem,
    hsend,
    hrecv,
    fsend,
    frecv,
):
    me = lax.axis_index("seq")
    mine = lax.axis_index("head")
    place = ring_place(me, n)
    rows = x_ref.shape[0]
    sub = rows // pieces
    share = rows // heads
    columns = w_ref.shape[1]
    half = n // 2
    ways = (1, -1)
    beside = [ring_index(place + way, n) for way in ways]
    weights = pltpu.make_async_copy(w_hbm, w_ref, w_sem.at[0])
    weights.start()
    barrier = pltpu.get_barrier_semaphore()
    for k in range(1, heads):
        pl.semaphore_signal(barrier, inc=1, device_id={"head": lax.rem(mine + k, heads)}, device_id_type=MESH)
    for k in range(1, n):
        pl.semaphore_signal(barrier, inc=1, device_id={"seq": lax.rem(me + k, n)}, device_id_type=MESH)
    pl.semaphore_wait(barrier, heads + n - 2)

    def owner_of(way, step):
        return ring_index(place - ways[way] * step, n)

    def copy(way, step, piece, first):
        there = (owner_of(way, step), pl.ds(piece * sub, sub))
        return pltpu.make_async_remote_copy(
            src_ref=x_ref.at[pl.ds(piece * sub, sub)] if first else blocks.at[there],
            dst_ref=blocks.at[there],
            send_sem=send_sem.at[way, step, piece],
            recv_sem=recv_sem.at[way, step, piece],
            device_id={"seq": beside[way]},
            device_id_type=MESH,
        )

    def to_head(i, k):
        to = lax.rem(mine + k, heads)
        return pltpu.make_async_remote_copy(
            src_ref=split.at[i, to],
            dst_ref=got.at[i, k],
            send_sem=hsend.at[i, k],
            recv_sem=hrecv.at[i, k],
            device_id={"head": to},
            device_id_type=MESH,
        )

    def to_row(k):
        to = lax.rem(me + k, n)
        return pltpu.make_async_remote_copy(
            src_ref=summed.at[to],
            dst_ref=landed.at[me],
            send_sem=fsend.at[k],
            recv_sem=frecv.at[k],
            device_id={"seq": to},
            device_id_type=MESH,
        )

    def multiply(i, piece, value):
        product = jnp.dot(value, w_ref[...], preferred_element_type=jnp.float32).astype(jnp.bfloat16)
        for s in range(sub // share):
            split[i, piece * (sub // share) + s] = product[s * share : (s + 1) * share]

    def give(i):
        for k in range(1, heads):
            to_head(i, k).start()

    def total_of(i):
        total = split[i, mine].astype(jnp.float32)
        for k in range(1, heads):
            to_head(i, k).wait_recv()
            total = total + got[i, k].astype(jnp.float32)
        return total.astype(jnp.bfloat16)

    def settle(i):
        summed[i] = total_of(i)
        to_row(lax.rem(i - me + n, n)).start()

    for spot in range(pieces):
        for way in range(2):
            copy(way, 0, spot if way == 0 else pieces - 1 - spot, True).start()
    weights.wait()
    for piece in range(pieces):
        multiply(me, piece, x_ref[piece * sub : (piece + 1) * sub])
    give(me)

    def take(way, step, piece, forward):
        copy(way, step - 1, piece, False).wait_recv()
        if forward:
            copy(way, step, piece, False).start()
        i = owner_of(way, step)
        multiply(i, piece, blocks[i, piece * sub : (piece + 1) * sub])

    def one_step(step, last):
        for spot in range(pieces):
            for way in range(2):
                take(way, step, spot if way == 0 else pieces - 1 - spot, not last or spot < pieces // 2)
        for way in range(2):
            give(owner_of(way, step))

    one_step(1, half == 2)
    landed[me] = total_of(me)

    def middle(step, carry):
        one_step(step, False)
        for way in range(2):
            settle(owner_of(way, step - 1))
        return carry

    lax.fori_loop(2, half - 1, middle, 0)
    if half > 2:
        one_step(half - 1, True)
        for way in range(2):
            settle(owner_of(way, half - 2))
    for spot in range(pieces // 2):
        for way in range(2):
            take(way, half, spot if way == 0 else pieces - 1 - spot, False)
    give(owner_of(0, half))
    for way in range(2):
        settle(owner_of(way, half - 1))
    settle(owner_of(0, half))

    for spot in range(pieces):
        for way in range(2):
            copy(way, 0, spot if way == 0 else pieces - 1 - spot, True).wait_send()

    def drain(step, carry):
        for piece in range(pieces):
            for way in range(2):
                copy(way, step, piece, False).wait_send()
        return carry

    lax.fori_loop(1, half - 1, drain, 0)
    if half > 1:
        for spot in range(pieces // 2):
            for way in range(2):
                copy(way, half - 1, spot if way == 0 else pieces - 1 - spot, False).wait_send()

    def drain_heads(i, carry):
        for k in range(1, heads):
            to_head(i, k).wait_send()
        return carry

    lax.fori_loop(0, n, drain_heads, 0)
    for k in range(1, n):
        to_row(k).wait()
    for i in range(n):
        out_ref[:, i * columns : (i + 1) * columns] = landed[i]


def projected(x, weight, n, heads, pieces):
    rows, width = x.shape
    columns = weight.shape[1]
    share = rows // heads
    vmem = pl.BlockSpec(memory_space=pltpu.VMEM)
    dma = pltpu.SemaphoreType.DMA
    return pl.pallas_call(
        functools.partial(project_kernel, n, heads, pieces),
        in_specs=[vmem, pl.BlockSpec(memory_space=pltpu.HBM)],
        out_specs=vmem,
        out_shape=jax.ShapeDtypeStruct((share, n * columns), x.dtype),
        scratch_shapes=[
            pltpu.VMEM(weight.shape, weight.dtype),
            pltpu.VMEM((n, rows, width), x.dtype),
            pltpu.VMEM((n, heads, share, columns), x.dtype),
            pltpu.VMEM((n, heads, share, columns), x.dtype),
            pltpu.VMEM((n, share, columns), x.dtype),
            pltpu.VMEM((n, share, columns), x.dtype),
            dma((1,)),
            dma((2, n // 2, pieces)),
            dma((2, n // 2, pieces)),
            dma((n, heads)),
            dma((n, heads)),
            dma((n,)),
            dma((n,)),
        ],
        compiler_params=pltpu.CompilerParams(
            collective_id=2,
            has_side_effects=True,
            vmem_limit_bytes=grant(
                (weight.shape, x.dtype),
                ((n + 2, rows, width), x.dtype),
                ((2, n, heads, share, max(columns, BLK)), x.dtype),
                ((3, n, share, max(columns, BLK)), x.dtype),
            ),
        ),
        cost_estimate=long_cost(),
    )(x, weight)


def body(
    queries,
    self_keys,
    self_values,
    store_keys,
    store_values,
    kv_slot,
    neighbours,
    counts,
    out_weight,
):
    n = lax.axis_size("seq")
    head_count = lax.axis_size("head")
    local_blocks, degree = neighbours.shape
    local_rows, width = queries.shape
    store_blocks = store_keys.shape[0] // BLK
    all_blocks = local_blocks * n
    kv_here = store_keys.shape[1] // DH
    group_width = (H // KVH) * DH
    rows = (H // KVH) * BLK
    all_queries, near, count = gathered(queries, neighbours, counts.reshape(1, local_blocks), n, 2)
    smem = pl.BlockSpec(memory_space=pltpu.SMEM)
    small = queries.size * n * queries.dtype.itemsize <= 8 << 20
    kind = pltpu.VMEM if small else jax.ShapeDtypeStruct
    q_spec = pl.BlockSpec((BLK, width), lambda i: (i, 0))
    o_spec = pl.BlockSpec((1, kv_here, BLK, group_width), lambda i: (i, 0, 0, 0))
    lse_spec = pl.BlockSpec((1, kv_here, STAT, BLK), lambda i: (i, 0, 0, 0))
    if small:
        q_spec = o_spec = lse_spec = pl.BlockSpec(memory_space=pltpu.VMEM)

    parts, lse = pl.pallas_call(
        functools.partial(part_kernel, local_blocks, store_blocks, small),
        grid=(all_blocks,),
        in_specs=[smem, smem, smem, q_spec]
        + [pl.BlockSpec(memory_space=pltpu.VMEM)] * 4,
        out_specs=[o_spec, lse_spec],
        out_shape=[
            kind((all_blocks, kv_here, BLK, group_width), jnp.bfloat16),
            kind((all_blocks, kv_here, STAT, BLK), jnp.float32),
        ],
        scratch_shapes=[
            pltpu.SMEM((degree + 1,), jnp.int32),
            pltpu.VMEM((kv_here, DH, rows), jnp.float32),
            pltpu.VMEM((kv_here, rows), jnp.float32),
            pltpu.VMEM((kv_here, rows), jnp.float32),
        ],
        compiler_params=pltpu.CompilerParams(vmem_limit_bytes=28 << 20),
        cost_estimate=pl.CostEstimate(flops=2_000_000_000, bytes_accessed=12 << 20, transcendentals=4_000_000),
    )(kv_slot, near, count, all_queries, self_keys, self_values, store_keys, store_values)
    dma = pltpu.SemaphoreType.DMA((2, n - 1, kv_here))
    attended = pl.pallas_call(
        functools.partial(reduce_kernel, n, small),
        in_specs=[pl.BlockSpec(memory_space=pltpu.VMEM if small else pl.ANY), pl.BlockSpec(memory_space=pltpu.VMEM)],
        out_specs=pl.BlockSpec(memory_space=pltpu.VMEM),
        out_shape=jax.ShapeDtypeStruct((local_rows, width), jnp.bfloat16),
        scratch_shapes=[
            pltpu.VMEM((2, n - 1, kv_here, BLK, group_width), jnp.bfloat16),
            pltpu.VMEM((2, n - 1, kv_here, STAT, BLK), jnp.float32),
            pltpu.VMEM((2, 2, 1 if small else kv_here, BLK, group_width), jnp.bfloat16),
            pltpu.SemaphoreType.DMA((2, 2)),
            dma,
            dma,
            dma,
            dma,
        ],
        compiler_params=pltpu.CompilerParams(
            collective_id=1,
            has_side_effects=True,
            vmem_limit_bytes=grant(
                ((2, n + 1, kv_here, BLK, group_width), jnp.bfloat16),
                ((2, n - 1, kv_here, STAT, BLK), jnp.float32),
                (lse.shape, lse.dtype),
                ((local_rows, width), jnp.bfloat16),
            ),
        ),
        cost_estimate=long_cost(),
    )(parts, lse)
    return projected(attended, out_weight, n, head_count, 2)


def solution(mesh):
    placed = (
        P("seq", "head"),
        P("seq", "head"),
        P("seq", "head"),
        P("seq", "head"),
        P("seq", "head"),
        P(),
        P("seq", None),
        P("seq"),
        P("head", "seq"),
    )
    return jax.shard_map(
        body, mesh=mesh, in_specs=placed, out_specs=P(("seq", "head"), None), check_vma=False
    )
```

```python
import functools

import jax
import jax.numpy as jnp
from jax import lax
from jax.experimental import pallas as pl
from jax.experimental.pallas import tpu as pltpu
from jax.sharding import PartitionSpec as P

H = 32
KVH = 8
DH = 128
BLK = 128
NEG = -1e30
STAT = 8
LOG2E = 1.4426950408889634
MESH = pl.DeviceIdType.MESH


def part_kernel(
    local_blocks,
    store_blocks,
    small,
    slot_ref,
    near_ref,
    count_ref,
    q_ref,
    sk_ref,
    sv_ref,
    k_ref,
    v_ref,
    o_ref,
    lse_ref,
    list_ref,
    acc_ref,
    max_ref,
    sum_ref,
):
    block = pl.program_id(0)
    me = lax.axis_index("seq")
    per_group = H // KVH
    kv_here = k_ref.shape[1] // DH
    rows = per_group * BLK
    scaling = DH ** (-0.5) * LOG2E
    here = block if small else 0
    owner, inner = block // local_blocks, lax.rem(block, local_blocks)
    first_row = pl.multiple_of(block * BLK, BLK) if small else 0

    def scan_entry(e, found):
        slot = slot_ref[near_ref[owner, inner, e]]
        list_ref[found] = lax.rem(slot, store_blocks)
        return found + (slot // store_blocks == me).astype(jnp.int32)

    found = lax.fori_loop(0, count_ref[owner, 0, inner], scan_entry, jnp.int32(0))
    home = block // local_blocks == me

    @pl.when(jnp.logical_and(found == 0, jnp.logical_not(home)))
    def _():
        o_ref[here] = jnp.zeros(o_ref.shape[1:], o_ref.dtype)
        lse_ref[here] = jnp.full(lse_ref.shape[1:], NEG, lse_ref.dtype)

    @pl.when(jnp.logical_or(found > 0, home))
    def _():
        def scores_of(g, keys):
            asked = jnp.concatenate(
                [
                    q_ref[pl.ds(first_row, BLK), (g * per_group + r) * DH : (g * per_group + r + 1) * DH]
                    for r in range(per_group)
                ],
                axis=0,
            )
            return (
                lax.dot_general(keys, asked, (((1,), (1,)), ((), ())), preferred_element_type=jnp.float32)
                * scaling
            )

        def weighed(values, p):
            return lax.dot_general(
                values, p.astype(jnp.bfloat16), (((0,), (0,)), ((), ())), preferred_element_type=jnp.float32
            )

        @pl.when(home)
        def _():
            start = pl.multiple_of(lax.rem(block, local_blocks) * BLK, BLK)
            position = lax.rem(lax.broadcasted_iota(jnp.int32, (BLK, rows), 1), BLK)
            causal = position >= lax.broadcasted_iota(jnp.int32, (BLK, rows), 0)
            for g in range(kv_here):
                cols = slice(g * DH, (g + 1) * DH)
                s = jnp.where(causal, scores_of(g, sk_ref[pl.ds(start, BLK), cols]), NEG)
                m = jnp.max(s, axis=0, keepdims=True)
                p = jnp.exp2(s - m)
                max_ref[g : g + 1] = m
                sum_ref[g : g + 1] = jnp.sum(p, axis=0, keepdims=True)
                acc_ref[g] = weighed(sv_ref[pl.ds(start, BLK), cols], p)

        @pl.when(jnp.logical_not(home))
        def _():
            max_ref[...] = jnp.full_like(max_ref, NEG)
            sum_ref[...] = jnp.zeros_like(sum_ref)
            acc_ref[...] = jnp.zeros_like(acc_ref)

        @pl.loop(0, found)
        def _(i):
            start = pl.multiple_of(list_ref[i] * BLK, BLK)
            for g in range(kv_here):
                cols = slice(g * DH, (g + 1) * DH)
                s = scores_of(g, k_ref[pl.ds(start, BLK), cols])
                old = max_ref[g : g + 1]
                new = jnp.maximum(old, jnp.max(s, axis=0, keepdims=True))
                p = jnp.exp2(s - new)
                shrink = jnp.exp2(old - new)
                max_ref[g : g + 1] = new
                sum_ref[g : g + 1] = sum_ref[g : g + 1] * shrink + jnp.sum(p, axis=0, keepdims=True)
                acc_ref[g] = acc_ref[g] * shrink + weighed(v_ref[pl.ds(start, BLK), cols], p)

        for g in range(kv_here):
            total = sum_ref[g : g + 1]
            lse = max_ref[g : g + 1] + jnp.log2(total)
            o_ref[here, g] = (acc_ref[g] * (1.0 / total)).astype(jnp.bfloat16)
            for r in range(STAT):
                at = (r % per_group) * BLK
                lse_ref[here, g, r : r + 1] = lse[:, at : at + BLK]


def grant(*arrays):
    size = 0
    for shape, dtype in arrays:
        cells = 1
        for d in shape:
            cells = cells * d
        size += cells * jnp.dtype(dtype).itemsize
    return min(size + (4 << 20), 60 << 20)


def long_cost():
    return pl.CostEstimate(flops=200_000_000_000, bytes_accessed=1 << 20, transcendentals=0)


def ring_place(index, n):
    odd = lax.rem(index, 2)
    half = index // 2
    return (1 - odd) * half + odd * (n - 1 - half)


def ring_index(place, n):
    place = lax.rem(place + 2 * n, n)
    far = place // (n // 2)
    return (1 - far) * (2 * place) + far * (2 * (n - 1 - place) + 1)


def gather_kernel(
    n,
    pieces,
    x_ref,
    near_ref,
    count_ref,
    out_ref,
    nears_ref,
    counts_ref,
    own_sem,
    send_sem,
    recv_sem,
    tsend_sem,
    trecv_sem,
):
    me = lax.axis_index("seq")
    place = ring_place(me, n)
    rows = x_ref.shape[0]
    sub = rows // pieces
    half = n // 2
    ways = (1, -1)
    beside = [ring_index(place + way, n) for way in ways]
    own = [
        pltpu.make_async_copy(source, target, own_sem.at[i])
        for i, (source, target) in enumerate(
            (
                (x_ref, out_ref.at[pl.ds(pl.multiple_of(me * rows, rows), rows)]),
                (near_ref, nears_ref.at[me]),
                (count_ref, counts_ref.at[me]),
            )
        )
    ]
    for one in own:
        one.start()
    barrier = pltpu.get_barrier_semaphore()
    for k in range(1, n):
        pl.semaphore_signal(barrier, inc=1, device_id={"seq": lax.rem(me + k, n)}, device_id_type=MESH)
    for one in own:
        one.wait()
    pl.semaphore_wait(barrier, n - 1)

    def copy(way, step, piece):
        owner = ring_index(place - ways[way] * step, n)
        there = pl.ds(pl.multiple_of(owner * rows + piece * sub, sub), sub)
        return pltpu.make_async_remote_copy(
            src_ref=out_ref.at[there],
            dst_ref=out_ref.at[there],
            send_sem=send_sem.at[way, step, piece],
            recv_sem=recv_sem.at[way, step, piece],
            device_id={"seq": beside[way]},
            device_id_type=MESH,
        )

    started = []
    for spot in range(pieces):
        for way in range(2):
            one = copy(way, 0, spot if way == 0 else pieces - 1 - spot)
            one.start()
            started.append(one)
    table_copies = []
    for t, target in enumerate((nears_ref, counts_ref)):
        for k in range(1, n):
            table_copies.append(
                pltpu.make_async_remote_copy(
                    src_ref=target.at[me],
                    dst_ref=target.at[me],
                    send_sem=tsend_sem.at[t, k],
                    recv_sem=trecv_sem.at[t, k],
                    device_id={"seq": lax.rem(me + k, n)},
                    device_id_type=MESH,
                )
            )
    for one in table_copies:
        one.start()
    for step in range(1, half):
        for spot in range(pieces):
            for way in range(2):
                piece = spot if way == 0 else pieces - 1 - spot
                copy(way, step - 1, piece).wait_recv()
                if step < half - 1 or spot < pieces // 2:
                    one = copy(way, step, piece)
                    one.start()
                    started.append(one)
    for spot in range(pieces // 2):
        for way in range(2):
            copy(way, half - 1, spot if way == 0 else pieces - 1 - spot).wait_recv()
    for one in started:
        one.wait_send()
    for one in table_copies:
        one.wait()


def gathered(x, near, count, n, pieces):
    rows, width = x.shape
    vmem = pl.BlockSpec(memory_space=pltpu.VMEM)
    size = n * rows * width * x.dtype.itemsize
    kind = pltpu.VMEM if size <= 8 << 20 else jax.ShapeDtypeStruct
    return pl.pallas_call(
        functools.partial(gather_kernel, n, pieces),
        in_specs=[pl.BlockSpec(memory_space=pltpu.HBM)] * 3,
        out_specs=[vmem] * 3,
        out_shape=[
            kind((n * rows, width), x.dtype),
            jax.ShapeDtypeStruct((n,) + near.shape, near.dtype),
            jax.ShapeDtypeStruct((n,) + count.shape, count.dtype),
        ],
        scratch_shapes=[
            pltpu.SemaphoreType.DMA((3,)),
            pltpu.SemaphoreType.DMA((2, n // 2, pieces)),
            pltpu.SemaphoreType.DMA((2, n // 2, pieces)),
            pltpu.SemaphoreType.DMA((2, n)),
            pltpu.SemaphoreType.DMA((2, n)),
        ],
        compiler_params=pltpu.CompilerParams(
            collective_id=0,
            has_side_effects=True,
            vmem_limit_bytes=grant((x.shape, x.dtype), ((n * rows, width), x.dtype)),
        ),
        cost_estimate=long_cost(),
    )(*(pltpu.with_memory_space_constraint(a, pltpu.HBM) for a in (x, near, count)))


def merge(lse_a, lse_b):
    top = jnp.maximum(lse_a, lse_b)
    a = jnp.exp2(lse_a - top)
    b = jnp.exp2(lse_b - top)
    total = a + b
    return a / total, b / total, top + jnp.log2(total)


def reduce_kernel(
    n, small, o_ref, lse_ref, out_ref, got, got_lse, own, own_sem, send_sem, recv_sem, lsend_sem, lrecv_sem
):
    me = lax.axis_index("seq")
    place = ring_place(me, n)
    groups, width = got.shape[2], got.shape[4]
    ways = (1, -1)
    beside = [ring_index(place + way, n) for way in ways]
    barrier = pltpu.get_barrier_semaphore()
    for other in beside:
        pl.semaphore_signal(barrier, inc=1, device_id={"seq": other}, device_id_type=MESH)

    def home(way, step):
        return ring_index(place - ways[way] * (1 + step), n)

    def fetch(way, step):
        return pltpu.make_async_copy(
            o_ref.at[home(way, step) * 2 + way], own.at[way, lax.rem(step, 2)], own_sem.at[way, lax.rem(step, 2)]
        )

    def copies(way, step, g, before):
        at = home(way, step) * 2 + way
        first = before is None
        return (
            pltpu.make_async_remote_copy(
                src_ref=lse_ref.at[at, g] if first else got_lse.at[way, before, g],
                dst_ref=got_lse.at[way, step, g],
                send_sem=lsend_sem.at[way, step, g],
                recv_sem=lrecv_sem.at[way, step, g],
                device_id={"seq": beside[way]},
                device_id_type=MESH,
            ),
            pltpu.make_async_remote_copy(
                src_ref=o_ref.at[at, g] if first else got.at[way, before, g],
                dst_ref=got.at[way, step, g],
                send_sem=send_sem.at[way, step, g],
                recv_sem=recv_sem.at[way, step, g],
                device_id={"seq": beside[way]},
                device_id_type=MESH,
            ),
        )

    def merged(way, step, g):
        for one in copies(way, step - 1, g, step - 1):
            one.wait_recv()
        if g == 0 and not small:
            fetch(way, step).wait()
        at = home(way, step) * 2 + way
        theirs, ours, lse = merge(got_lse[way, step - 1, g], lse_ref[at, g])
        columns = []
        for r in range(width // DH):
            cols = slice(r * DH, (r + 1) * DH)
            mine = o_ref[at, g, :, cols] if small else own[way, lax.rem(step, 2), g, :, cols]
            columns.append(
                got[way, step - 1, g, :, cols].astype(jnp.float32) * theirs[r : r + 1]
                + mine.astype(jnp.float32) * ours[r : r + 1]
            )
        return columns, lse

    if not small:
        for way in range(2):
            fetch(way, 1).start()
    pl.semaphore_wait(barrier, 2)
    for g in range(groups):
        for way in range(2):
            for one in copies(way, 0, g, None):
                one.start()

    def one_step(step, carry):
        if not small:
            for way in range(2):
                fetch(way, step + 1).start()
        for g in range(groups):
            for way in range(2):
                columns, lse = merged(way, step, g)
                got_lse[way, step - 1, g] = lse
                for r, value in enumerate(columns):
                    got[way, step - 1, g, :, r * DH : (r + 1) * DH] = value.astype(jnp.bfloat16)
                for one in copies(way, step, g, step - 1):
                    one.start()
        return carry

    lax.fori_loop(1, n - 1, one_step, 0)
    for g in range(groups):
        for way in range(2):
            columns, _ = merged(way, n - 1, g)
            for r, value in enumerate(columns):
                at = g * width + r * DH
                out_ref[way * BLK : (way + 1) * BLK, at : at + DH] = jnp.transpose(value).astype(jnp.bfloat16)
    for g in range(groups):
        for way in range(2):
            for one in copies(way, 0, g, None):
                one.wait_send()

    def drain(step, carry):
        for g in range(groups):
            for way in range(2):
                for one in copies(way, step, g, step - 1):
                    one.wait_send()
        return carry

    lax.fori_loop(1, n - 1, drain, 0)


def project_kernel(
    n,
    heads,
    x_ref,
    w_hbm,
    out_ref,
    w_ref,
    blocks,
    split,
    got,
    summed,
    landed,
    w_sem,
    wsend,
    wrecv,
    send_sem,
    recv_sem,
    hsend,
    hrecv,
    fsend,
    frecv,
):
    me = lax.axis_index("seq")
    mine = lax.axis_index("head")
    line = n // 2
    at, side = me // 2, lax.rem(me, 2)
    share = x_ref.shape[0] // heads
    columns = w_ref.shape[2]
    ways = (1, -1)
    early = min(2, line - 1)
    weights = pltpu.make_async_copy(w_hbm, w_ref.at[0], w_sem.at[0])
    weights.start()
    barrier = pltpu.get_barrier_semaphore()
    for k in range(1, heads):
        pl.semaphore_signal(barrier, inc=1, device_id={"head": lax.rem(mine + k, heads)}, device_id_type=MESH)
    for k in range(1, line):
        other = lax.rem(at + k, line) * 2 + side
        pl.semaphore_signal(barrier, inc=1, device_id={"seq": other}, device_id_type=MESH)
    partner = at * 2 + 1 - side
    pl.semaphore_signal(barrier, inc=1, device_id={"seq": partner}, device_id_type=MESH)
    pl.semaphore_wait(barrier, heads + line - 1)

    def inside(place):
        return jnp.logical_and(place >= 0, place < line)

    def copy(way, step, piece, first):
        there = (at - ways[way] * step, pl.ds(pl.multiple_of(piece * share, share), share))
        return pltpu.make_async_remote_copy(
            src_ref=x_ref.at[there[1]] if first else blocks.at[there],
            dst_ref=blocks.at[there],
            send_sem=send_sem.at[way, step, piece],
            recv_sem=recv_sem.at[way, step, piece],
            device_id={"seq": (at + ways[way]) * 2 + side},
            device_id_type=MESH,
        )

    def leaves(way, step):
        return jnp.logical_and(inside(at - ways[way] * step), inside(at + ways[way]))

    def to_head(i, j, source, to):
        return pltpu.make_async_remote_copy(
            src_ref=split.at[i, j, to],
            dst_ref=got.at[i, j, source],
            send_sem=hsend.at[i, j, to],
            recv_sem=hrecv.at[i, j, source],
            device_id={"head": to},
            device_id_type=MESH,
        )

    def to_row(i, j, source):
        owner = source * 2 + (side if j == 0 else 1 - side)
        return pltpu.make_async_remote_copy(
            src_ref=summed.at[i, j],
            dst_ref=landed.at[owner],
            send_sem=fsend.at[i, j],
            recv_sem=frecv.at[source, j],
            device_id={"seq": i * 2 + side},
            device_id_type=MESH,
        )

    def unit(i, c, js, own):
        rows = pl.ds(pl.multiple_of(c * share, share), share)
        value = x_ref[rows] if own else blocks[i, rows]
        for j in js:
            split[i, j, c] = jnp.dot(value, w_ref[j], preferred_element_type=jnp.float32).astype(jnp.bfloat16)

            @pl.when(mine != c)
            def _():
                to_head(i, j, mine, c).start()

    def visit(step, c, js, arriving):
        for way in range(2):
            i = at - ways[way] * step

            @pl.when(inside(i))
            def _():
                if arriving:
                    copy(way, step - 1, c, False).wait_recv()

                    @pl.when(inside(at + ways[way]))
                    def _():
                        copy(way, step, c, False).start()

                unit(i, c, js, False)

    def total_of(i, j):
        total = split[i, j, mine].astype(jnp.float32)
        for k in range(1, heads):
            source = lax.rem(mine + k, heads)
            to_head(i, j, source, mine).wait_recv()
            total = total + got[i, j, source].astype(jnp.float32)
        return total.astype(jnp.bfloat16)

    def settle_own(j):
        landed[at * 2 + (side if j == 0 else 1 - side)] = total_of(at, j)

    def settle(step, js):
        for way in range(2):
            i = at - ways[way] * step

            @pl.when(inside(i))
            def _():
                for j in js:
                    summed[i, j] = total_of(i, j)
                    to_row(i, j, at).start()

    def each(function):
        lax.fori_loop(0, heads, lambda c, carry: (function(c), carry)[1], 0)

    def start_own(c):
        for way in range(2):

            @pl.when(inside(at + ways[way]))
            def _():
                copy(way, 0, c, True).start()

    each(start_own)
    weights.wait()
    exchange = pltpu.make_async_remote_copy(
        src_ref=w_ref.at[0],
        dst_ref=w_ref.at[1],
        send_sem=wsend.at[0],
        recv_sem=wrecv.at[0],
        device_id={"seq": partner},
        device_id_type=MESH,
    )
    exchange.start()
    each(lambda c: unit(at, c, (0,), True))

    def first_steps(step, carry):
        each(lambda c: visit(step, c, (0,), True))

        @pl.when(step == 1)
        def _():
            settle_own(0)

        @pl.when(step > 1)
        def _():
            settle(step - 1, (0,))

        return carry

    lax.fori_loop(1, early + 1, first_steps, 0)
    exchange.wait()
    each(lambda c: unit(at, c, (1,), True))
    lax.fori_loop(1, early + 1, lambda t, carry: (each(lambda c: visit(t, c, (1,), False)), carry)[1], 0)
    settle(early, (0,))

    def late_step(step, carry):
        each(lambda c: visit(step, c, (0, 1), True))

        @pl.when(step == early + 1)
        def _():
            settle_own(1)
            lax.fori_loop(1, early + 1, lambda t, inner: (settle(t, (1,)), inner)[1], 0)

        @pl.when(step > early + 1)
        def _():
            settle(step - 1, (0, 1))

        return carry

    if line - 1 > early:
        lax.fori_loop(early + 1, line, late_step, 0)
        settle(line - 1, (0, 1))
    else:
        settle_own(1)
        lax.fori_loop(1, early + 1, lambda t, inner: (settle(t, (1,)), inner)[1], 0)

    for way in range(2):
        for step in range(2):

            def finish(c):
                @pl.when(leaves(way, step))
                def _():
                    copy(way, step, c, step == 0).wait_send()

            if step == 0:
                each(finish)
            else:

                def finish_rest(t, carry):
                    def one(c):
                        @pl.when(leaves(way, t))
                        def _():
                            copy(way, t, c, False).wait_send()

                    each(one)
                    return carry

                lax.fori_loop(1, line, finish_rest, 0)

    def drain(i, carry):
        for j in range(2):
            for k in range(1, heads):
                to_head(i, j, mine, lax.rem(mine + k, heads)).wait_send()

            @pl.when(i != at)
            def _():
                to_row(i, j, at).wait_send()
                to_row(at, j, i).wait_recv()

        return carry

    lax.fori_loop(0, line, drain, 0)
    for i in range(n):
        out_ref[:, i * columns : (i + 1) * columns] = landed[i]


def projected(x, weight, n, heads):
    rows, width = x.shape
    columns = weight.shape[1]
    share = rows // heads
    line = n // 2
    vmem = pl.BlockSpec(memory_space=pltpu.VMEM)
    dma = pltpu.SemaphoreType.DMA
    return pl.pallas_call(
        functools.partial(project_kernel, n, heads),
        in_specs=[vmem, pl.BlockSpec(memory_space=pl.ANY)],
        out_specs=vmem,
        out_shape=jax.ShapeDtypeStruct((share, n * columns), x.dtype),
        scratch_shapes=[
            pltpu.VMEM((2,) + weight.shape, weight.dtype),
            pltpu.VMEM((line, rows, width), x.dtype),
            pltpu.VMEM((line, 2, heads, share, columns), x.dtype),
            pltpu.VMEM((line, 2, heads, share, columns), x.dtype),
            pltpu.VMEM((line, 2, share, columns), x.dtype),
            pltpu.VMEM((n, share, columns), x.dtype),
            dma((1,)),
            dma((1,)),
            dma((1,)),
            dma((2, line, heads)),
            dma((2, line, heads)),
            dma((line, 2, heads)),
            dma((line, 2, heads)),
            dma((line, 2)),
            dma((line, 2)),
        ],
        compiler_params=pltpu.CompilerParams(
            collective_id=2,
            has_side_effects=True,
            vmem_limit_bytes=grant(
                ((2, width, max(columns, BLK)), x.dtype),
                ((line + 2, rows, width), x.dtype),
                ((2, n, heads, share, max(columns, BLK)), x.dtype),
                ((3, n, share, max(columns, BLK)), x.dtype),
            ),
        ),
        cost_estimate=long_cost(),
    )(x, weight)


def body(
    queries,
    self_keys,
    self_values,
    store_keys,
    store_values,
    kv_slot,
    neighbours,
    counts,
    out_weight,
):
    n = lax.axis_size("seq")
    head_count = lax.axis_size("head")
    local_blocks, degree = neighbours.shape
    local_rows, width = queries.shape
    store_blocks = store_keys.shape[0] // BLK
    all_blocks = local_blocks * n
    kv_here = store_keys.shape[1] // DH
    group_width = (H // KVH) * DH
    rows = (H // KVH) * BLK
    all_queries, near, count = gathered(queries, neighbours, counts.reshape(1, local_blocks), n, 2)
    smem = pl.BlockSpec(memory_space=pltpu.SMEM)
    small = queries.size * n * queries.dtype.itemsize <= 8 << 20
    kind = pltpu.VMEM if small else jax.ShapeDtypeStruct
    q_spec = pl.BlockSpec((BLK, width), lambda i: (i, 0))
    o_spec = pl.BlockSpec((1, kv_here, BLK, group_width), lambda i: (i, 0, 0, 0))
    lse_spec = pl.BlockSpec((1, kv_here, STAT, BLK), lambda i: (i, 0, 0, 0))
    if small:
        q_spec = o_spec = lse_spec = pl.BlockSpec(memory_space=pltpu.VMEM)

    parts, lse = pl.pallas_call(
        functools.partial(part_kernel, local_blocks, store_blocks, small),
        grid=(all_blocks,),
        in_specs=[smem, smem, smem, q_spec]
        + [pl.BlockSpec(memory_space=pltpu.VMEM)] * 4,
        out_specs=[o_spec, lse_spec],
        out_shape=[
            kind((all_blocks, kv_here, BLK, group_width), jnp.bfloat16),
            kind((all_blocks, kv_here, STAT, BLK), jnp.float32),
        ],
        scratch_shapes=[
            pltpu.SMEM((degree + 1,), jnp.int32),
            pltpu.VMEM((kv_here, DH, rows), jnp.float32),
            pltpu.VMEM((kv_here, rows), jnp.float32),
            pltpu.VMEM((kv_here, rows), jnp.float32),
        ],
        compiler_params=pltpu.CompilerParams(vmem_limit_bytes=28 << 20),
        cost_estimate=pl.CostEstimate(flops=2_000_000_000, bytes_accessed=12 << 20, transcendentals=4_000_000),
    )(kv_slot, near, count, all_queries, self_keys, self_values, store_keys, store_values)
    dma = pltpu.SemaphoreType.DMA((2, n - 1, kv_here))
    attended = pl.pallas_call(
        functools.partial(reduce_kernel, n, small),
        in_specs=[pl.BlockSpec(memory_space=pltpu.VMEM if small else pl.ANY), pl.BlockSpec(memory_space=pltpu.VMEM)],
        out_specs=pl.BlockSpec(memory_space=pltpu.VMEM),
        out_shape=jax.ShapeDtypeStruct((local_rows, width), jnp.bfloat16),
        scratch_shapes=[
            pltpu.VMEM((2, n - 1, kv_here, BLK, group_width), jnp.bfloat16),
            pltpu.VMEM((2, n - 1, kv_here, STAT, BLK), jnp.float32),
            pltpu.VMEM((2, 2, 1 if small else kv_here, BLK, group_width), jnp.bfloat16),
            pltpu.SemaphoreType.DMA((2, 2)),
            dma,
            dma,
            dma,
            dma,
        ],
        compiler_params=pltpu.CompilerParams(
            collective_id=1,
            has_side_effects=True,
            vmem_limit_bytes=grant(
                ((2, n + 1, kv_here, BLK, group_width), jnp.bfloat16),
                ((2, n - 1, kv_here, STAT, BLK), jnp.float32),
                (lse.shape, lse.dtype),
                ((local_rows, width), jnp.bfloat16),
            ),
        ),
        cost_estimate=long_cost(),
    )(parts, lse)
    return projected(attended, out_weight, n, head_count)


def solution(mesh):
    placed = (
        P("seq", "head"),
        P("seq", "head"),
        P("seq", "head"),
        P("seq", "head"),
        P("seq", "head"),
        P(),
        P("seq", None),
        P("seq"),
        P("head", "seq"),
    )
    return jax.shard_map(
        body, mesh=mesh, in_specs=placed, out_specs=P(("seq", "head"), None), check_vma=False
    )
```

```python
import functools

import jax
import jax.numpy as jnp
from jax import lax
from jax.experimental import pallas as pl
from jax.experimental.pallas import tpu as pltpu
from jax.sharding import PartitionSpec as P

H = 32
KVH = 8
DH = 128
BLK = 128
NEG = -1e30
STAT = 8
SCAN = 4
LOG2E = 1.4426950408889634
MESH = pl.DeviceIdType.MESH


def part_kernel(
    local_blocks,
    store_blocks,
    small,
    slot_ref,
    near_ref,
    count_ref,
    q_ref,
    sk_ref,
    sv_ref,
    k_ref,
    v_ref,
    o_ref,
    lse_ref,
    list_ref,
    acc_ref,
    max_ref,
    sum_ref,
):
    block = pl.program_id(0)
    me = lax.axis_index("seq")
    per_group = H // KVH
    kv_here = k_ref.shape[1] // DH
    rows = per_group * BLK
    scaling = DH ** (-0.5) * LOG2E
    here = block if small else 0
    owner, inner = block // local_blocks, lax.rem(block, local_blocks)
    first_row = pl.multiple_of(block * BLK, BLK) if small else 0

    listed = count_ref[owner, 0, inner]
    first_slot = me * store_blocks

    def scan_entries(i, found):
        places = [slot_ref[near_ref[owner, inner, i * SCAN + u]] - first_slot for u in range(SCAN)]
        for u, place in enumerate(places):
            list_ref[found] = place
            kept = (place >= 0) & (place < store_blocks) & (i * SCAN + u < listed)
            found = found + kept.astype(jnp.int32)
        return found

    found = lax.fori_loop(0, lax.div(listed + (SCAN - 1), SCAN), scan_entries, jnp.int32(0))
    home = block // local_blocks == me

    @pl.when(jnp.logical_and(found == 0, jnp.logical_not(home)))
    def _():
        o_ref[here] = jnp.zeros(o_ref.shape[1:], o_ref.dtype)
        lse_ref[here] = jnp.full(lse_ref.shape[1:], NEG, lse_ref.dtype)

    @pl.when(jnp.logical_or(found > 0, home))
    def _():
        def scores_of(g, keys):
            asked = jnp.concatenate(
                [
                    q_ref[pl.ds(first_row, BLK), (g * per_group + r) * DH : (g * per_group + r + 1) * DH]
                    for r in range(per_group)
                ],
                axis=0,
            )
            return (
                lax.dot_general(keys, asked, (((1,), (1,)), ((), ())), preferred_element_type=jnp.float32)
                * scaling
            )

        def weighed(values, p):
            return lax.dot_general(
                values, p.astype(jnp.bfloat16), (((0,), (0,)), ((), ())), preferred_element_type=jnp.float32
            )

        @pl.when(home)
        def _():
            start = pl.multiple_of(lax.rem(block, local_blocks) * BLK, BLK)
            position = lax.rem(lax.broadcasted_iota(jnp.int32, (BLK, rows), 1), BLK)
            causal = position >= lax.broadcasted_iota(jnp.int32, (BLK, rows), 0)
            for g in range(kv_here):
                cols = slice(g * DH, (g + 1) * DH)
                s = jnp.where(causal, scores_of(g, sk_ref[pl.ds(start, BLK), cols]), NEG)
                m = jnp.max(s, axis=0, keepdims=True)
                p = jnp.exp2(s - m)
                max_ref[g : g + 1] = m
                sum_ref[g : g + 1] = jnp.sum(p, axis=0, keepdims=True)
                acc_ref[g] = weighed(sv_ref[pl.ds(start, BLK), cols], p)

        @pl.when(jnp.logical_not(home))
        def _():
            max_ref[...] = jnp.full_like(max_ref, NEG)
            sum_ref[...] = jnp.zeros_like(sum_ref)
            acc_ref[...] = jnp.zeros_like(acc_ref)

        def take(*places):
            starts = [pl.multiple_of(place * BLK, BLK) for place in places]

            def rows_of(ref, cols):
                return jnp.concatenate([ref[pl.ds(start, BLK), cols] for start in starts], axis=0)

            for g in range(kv_here):
                cols = slice(g * DH, (g + 1) * DH)
                s = scores_of(g, rows_of(k_ref, cols))
                old = max_ref[g : g + 1]
                new = jnp.maximum(old, jnp.max(s, axis=0, keepdims=True))
                p = jnp.exp2(s - new)
                shrink = jnp.exp2(old - new)
                max_ref[g : g + 1] = new
                sum_ref[g : g + 1] = sum_ref[g : g + 1] * shrink + jnp.sum(p, axis=0, keepdims=True)
                acc_ref[g] = acc_ref[g] * shrink + weighed(rows_of(v_ref, cols), p)

        @pl.loop(0, lax.div(found, 2))
        def _(i):
            take(list_ref[2 * i], list_ref[2 * i + 1])

        @pl.when(lax.rem(found, 2) == 1)
        def _():
            take(list_ref[found - 1])

        for g in range(kv_here):
            total = sum_ref[g : g + 1]
            lse = max_ref[g : g + 1] + jnp.log2(total)
            o_ref[here, g] = (acc_ref[g] * (1.0 / total)).astype(jnp.bfloat16)
            for r in range(STAT):
                at = (r % per_group) * BLK
                lse_ref[here, g, r : r + 1] = lse[:, at : at + BLK]


def grant(*arrays):
    size = 0
    for shape, dtype in arrays:
        cells = 1
        for d in shape:
            cells = cells * d
        size += cells * jnp.dtype(dtype).itemsize
    return min(size + (4 << 20), 60 << 20)


def long_cost():
    return pl.CostEstimate(flops=200_000_000_000, bytes_accessed=1 << 20, transcendentals=0)


def ring_place(index, n):
    odd = lax.rem(index, 2)
    half = index // 2
    return (1 - odd) * half + odd * (n - 1 - half)


def ring_index(place, n):
    place = lax.rem(place + 2 * n, n)
    far = place // (n // 2)
    return (1 - far) * (2 * place) + far * (2 * (n - 1 - place) + 1)


def gather_kernel(
    n,
    pieces,
    x_ref,
    near_ref,
    count_ref,
    out_ref,
    nears_ref,
    counts_ref,
    own_sem,
    send_sem,
    recv_sem,
    tsend_sem,
    trecv_sem,
):
    me = lax.axis_index("seq")
    place = ring_place(me, n)
    rows = x_ref.shape[0]
    sub = rows // pieces
    half = n // 2
    ways = (1, -1)
    beside = [ring_index(place + way, n) for way in ways]
    own = [
        pltpu.make_async_copy(source, target, own_sem.at[i])
        for i, (source, target) in enumerate(
            (
                (x_ref, out_ref.at[pl.ds(pl.multiple_of(me * rows, rows), rows)]),
                (near_ref, nears_ref.at[me]),
                (count_ref, counts_ref.at[me]),
            )
        )
    ]
    for one in own:
        one.start()
    barrier = pltpu.get_barrier_semaphore()
    for k in range(1, n):
        pl.semaphore_signal(barrier, inc=1, device_id={"seq": lax.rem(me + k, n)}, device_id_type=MESH)
    for one in own:
        one.wait()
    pl.semaphore_wait(barrier, n - 1)

    def copy(way, step, piece):
        owner = ring_index(place - ways[way] * step, n)
        there = pl.ds(pl.multiple_of(owner * rows + piece * sub, sub), sub)
        return pltpu.make_async_remote_copy(
            src_ref=out_ref.at[there],
            dst_ref=out_ref.at[there],
            send_sem=send_sem.at[way, step, piece],
            recv_sem=recv_sem.at[way, step, piece],
            device_id={"seq": beside[way]},
            device_id_type=MESH,
        )

    started = []
    for spot in range(pieces):
        for way in range(2):
            one = copy(way, 0, spot if way == 0 else pieces - 1 - spot)
            one.start()
            started.append(one)
    table_copies = []
    for t, target in enumerate((nears_ref, counts_ref)):
        for k in range(1, n):
            table_copies.append(
                pltpu.make_async_remote_copy(
                    src_ref=target.at[me],
                    dst_ref=target.at[me],
                    send_sem=tsend_sem.at[t, k],
                    recv_sem=trecv_sem.at[t, k],
                    device_id={"seq": lax.rem(me + k, n)},
                    device_id_type=MESH,
                )
            )
    for one in table_copies:
        one.start()
    for step in range(1, half):
        for spot in range(pieces):
            for way in range(2):
                piece = spot if way == 0 else pieces - 1 - spot
                copy(way, step - 1, piece).wait_recv()
                if step < half - 1 or spot < pieces // 2:
                    one = copy(way, step, piece)
                    one.start()
                    started.append(one)
    for spot in range(pieces // 2):
        for way in range(2):
            copy(way, half - 1, spot if way == 0 else pieces - 1 - spot).wait_recv()
    for one in started:
        one.wait_send()
    for one in table_copies:
        one.wait()


def gathered(x, near, count, n, pieces):
    rows, width = x.shape
    vmem = pl.BlockSpec(memory_space=pltpu.VMEM)
    size = n * rows * width * x.dtype.itemsize
    kind = pltpu.VMEM if size <= 8 << 20 else jax.ShapeDtypeStruct
    return pl.pallas_call(
        functools.partial(gather_kernel, n, pieces),
        in_specs=[pl.BlockSpec(memory_space=pltpu.HBM)] * 3,
        out_specs=[vmem] * 3,
        out_shape=[
            kind((n * rows, width), x.dtype),
            jax.ShapeDtypeStruct((n,) + near.shape, near.dtype),
            jax.ShapeDtypeStruct((n,) + count.shape, count.dtype),
        ],
        scratch_shapes=[
            pltpu.SemaphoreType.DMA((3,)),
            pltpu.SemaphoreType.DMA((2, n // 2, pieces)),
            pltpu.SemaphoreType.DMA((2, n // 2, pieces)),
            pltpu.SemaphoreType.DMA((2, n)),
            pltpu.SemaphoreType.DMA((2, n)),
        ],
        compiler_params=pltpu.CompilerParams(
            collective_id=0,
            has_side_effects=True,
            vmem_limit_bytes=grant((x.shape, x.dtype), ((n * rows, width), x.dtype)),
        ),
        cost_estimate=long_cost(),
    )(*(pltpu.with_memory_space_constraint(a, pltpu.HBM) for a in (x, near, count)))


def merge(lse_a, lse_b):
    top = jnp.maximum(lse_a, lse_b)
    a = jnp.exp2(lse_a - top)
    b = jnp.exp2(lse_b - top)
    total = a + b
    return a / total, b / total, top + jnp.log2(total)


def reduce_kernel(
    n,
    small,
    o_ref,
    lse_ref,
    out_ref,
    got,
    got_lse,
    own,
    own_sem,
    send_sem,
    recv_sem,
    lsend_sem,
    lrecv_sem,
    ready=None,
):
    me = lax.axis_index("seq")
    place = ring_place(me, n)
    groups, width = got.shape[2], got.shape[4]
    ways = (1, -1)
    beside = [ring_index(place + way, n) for way in ways]
    if ready is None:
        barrier = pltpu.get_barrier_semaphore()
        for other in beside:
            pl.semaphore_signal(barrier, inc=1, device_id={"seq": other}, device_id_type=MESH)

    def home(way, step):
        return ring_index(place - ways[way] * (1 + step), n)

    def fetch(way, step):
        return pltpu.make_async_copy(
            o_ref.at[home(way, step) * 2 + way], own.at[way, lax.rem(step, 2)], own_sem.at[way, lax.rem(step, 2)]
        )

    def copies(way, step, g, before):
        at = home(way, step) * 2 + way
        first = before is None
        return (
            pltpu.make_async_remote_copy(
                src_ref=lse_ref.at[at, g] if first else got_lse.at[way, before, g],
                dst_ref=got_lse.at[way, step, g],
                send_sem=lsend_sem.at[way, step, g],
                recv_sem=lrecv_sem.at[way, step, g],
                device_id={"seq": beside[way]},
                device_id_type=MESH,
            ),
            pltpu.make_async_remote_copy(
                src_ref=o_ref.at[at, g] if first else got.at[way, before, g],
                dst_ref=got.at[way, step, g],
                send_sem=send_sem.at[way, step, g],
                recv_sem=recv_sem.at[way, step, g],
                device_id={"seq": beside[way]},
                device_id_type=MESH,
            ),
        )

    def merged(way, step, g):
        for one in copies(way, step - 1, g, step - 1):
            one.wait_recv()
        if g == 0 and not small:
            fetch(way, step).wait()
        at = home(way, step) * 2 + way
        theirs, ours, lse = merge(got_lse[way, step - 1, g], lse_ref[at, g])
        columns = []
        for r in range(width // DH):
            cols = slice(r * DH, (r + 1) * DH)
            mine = o_ref[at, g, :, cols] if small else own[way, lax.rem(step, 2), g, :, cols]
            columns.append(
                got[way, step - 1, g, :, cols].astype(jnp.float32) * theirs[r : r + 1]
                + mine.astype(jnp.float32) * ours[r : r + 1]
            )
        return columns, lse

    if not small:
        for way in range(2):
            fetch(way, 1).start()
    if ready is None:
        pl.semaphore_wait(barrier, 2)
    for g in range(groups):
        for way in range(2):
            for one in copies(way, 0, g, None):
                one.start()

    def one_step(step, carry):
        if not small:
            for way in range(2):
                fetch(way, step + 1).start()
        for g in range(groups):
            for way in range(2):
                columns, lse = merged(way, step, g)
                got_lse[way, step - 1, g] = lse
                for r, value in enumerate(columns):
                    got[way, step - 1, g, :, r * DH : (r + 1) * DH] = value.astype(jnp.bfloat16)
                for one in copies(way, step, g, step - 1):
                    one.start()
        return carry

    lax.fori_loop(1, n - 1, one_step, 0)
    for way in range(2):
        for g in range(groups):
            columns, _ = merged(way, n - 1, g)
            for r, value in enumerate(columns):
                at = g * width + r * DH
                out_ref[way * BLK : (way + 1) * BLK, at : at + DH] = jnp.transpose(value).astype(jnp.bfloat16)
        if ready is not None:
            ready(way)

    def drain_all():
        for g in range(groups):
            for way in range(2):
                for one in copies(way, 0, g, None):
                    one.wait_send()

        def drain(step, carry):
            for g in range(groups):
                for way in range(2):
                    for one in copies(way, step, g, step - 1):
                        one.wait_send()
            return carry

        lax.fori_loop(1, n - 1, drain, 0)

    if ready is None:
        drain_all()
    return drain_all


def project_stages(
    n,
    heads,
    x_ref,
    w_hbm,
    out_ref,
    w_ref,
    blocks,
    split,
    got,
    summed,
    landed,
    w_sem,
    wsend,
    wrecv,
    send_sem,
    recv_sem,
    hsend,
    hrecv,
    fsend,
    frecv,
):
    me = lax.axis_index("seq")
    mine = lax.axis_index("head")
    line = n // 2
    at, side = me // 2, lax.rem(me, 2)
    share = x_ref.shape[0] // heads
    columns = w_ref.shape[2]
    ways = (1, -1)
    early = min(2, line - 1)
    weights = pltpu.make_async_copy(w_hbm, w_ref.at[0], w_sem.at[0])
    weights.start()
    barrier = pltpu.get_barrier_semaphore()
    place = ring_place(me, n)
    for way in ways:
        other = ring_index(place + way, n)
        pl.semaphore_signal(barrier, inc=1, device_id={"seq": other}, device_id_type=MESH)
    for k in range(1, heads):
        pl.semaphore_signal(barrier, inc=1, device_id={"head": lax.rem(mine + k, heads)}, device_id_type=MESH)
    for k in range(1, line):
        other = lax.rem(at + k, line) * 2 + side
        pl.semaphore_signal(barrier, inc=1, device_id={"seq": other}, device_id_type=MESH)
    partner = at * 2 + 1 - side
    pl.semaphore_signal(barrier, inc=1, device_id={"seq": partner}, device_id_type=MESH)
    pl.semaphore_wait(barrier, heads + line + 1)

    def inside(spot):
        return jnp.logical_and(spot >= 0, spot < line)

    def copy(way, step, piece, first):
        there = (at - ways[way] * step, pl.ds(pl.multiple_of(piece * share, share), share))
        return pltpu.make_async_remote_copy(
            src_ref=x_ref.at[there[1]] if first else blocks.at[there],
            dst_ref=blocks.at[there],
            send_sem=send_sem.at[way, step, piece],
            recv_sem=recv_sem.at[way, step, piece],
            device_id={"seq": (at + ways[way]) * 2 + side},
            device_id_type=MESH,
        )

    def leaves(way, step):
        return jnp.logical_and(inside(at - ways[way] * step), inside(at + ways[way]))

    def to_head(i, j, source, to):
        return pltpu.make_async_remote_copy(
            src_ref=split.at[i, j, to],
            dst_ref=got.at[i, j, source],
            send_sem=hsend.at[i, j, to],
            recv_sem=hrecv.at[i, j, source],
            device_id={"head": to},
            device_id_type=MESH,
        )

    def to_row(i, j, source):
        owner = source * 2 + (side if j == 0 else 1 - side)
        return pltpu.make_async_remote_copy(
            src_ref=summed.at[i, j],
            dst_ref=landed.at[owner],
            send_sem=fsend.at[i, j],
            recv_sem=frecv.at[source, j],
            device_id={"seq": i * 2 + side},
            device_id_type=MESH,
        )

    def unit(i, c, js, own):
        rows = pl.ds(pl.multiple_of(c * share, share), share)
        value = x_ref[rows] if own else blocks[i, rows]
        for j in js:
            split[i, j, c] = jnp.dot(value, w_ref[j], preferred_element_type=jnp.float32).astype(jnp.bfloat16)

            @pl.when(mine != c)
            def _():
                to_head(i, j, mine, c).start()

    def visit(step, c, js, arriving):
        for way in range(2):
            i = at - ways[way] * step

            @pl.when(inside(i))
            def _():
                if arriving:
                    copy(way, step - 1, c, False).wait_recv()

                    @pl.when(inside(at + ways[way]))
                    def _():
                        copy(way, step, c, False).start()

                unit(i, c, js, False)

    def total_of(i, j):
        total = split[i, j, mine].astype(jnp.float32)
        for k in range(1, heads):
            source = lax.rem(mine + k, heads)
            to_head(i, j, source, mine).wait_recv()
            total = total + got[i, j, source].astype(jnp.float32)
        return total.astype(jnp.bfloat16)

    def settle_own(j):
        landed[at * 2 + (side if j == 0 else 1 - side)] = total_of(at, j)

    def settle(step, js):
        for way in range(2):
            i = at - ways[way] * step

            @pl.when(inside(i))
            def _():
                for j in js:
                    summed[i, j] = total_of(i, j)
                    to_row(i, j, at).start()

    def each(function):
        lax.fori_loop(0, heads, lambda c, carry: (function(c), carry)[1], 0)

    def start_own(c):
        for way in range(2):

            @pl.when(inside(at + ways[way]))
            def _():
                copy(way, 0, c, True).start()

    def run():
        weights.wait()
        exchange = pltpu.make_async_remote_copy(
            src_ref=w_ref.at[0],
            dst_ref=w_ref.at[1],
            send_sem=wsend.at[0],
            recv_sem=wrecv.at[0],
            device_id={"seq": partner},
            device_id_type=MESH,
        )
        exchange.start()
        each(lambda c: unit(at, c, (0,), True))

        def first_steps(step, carry):
            each(lambda c: visit(step, c, (0,), True))

            @pl.when(step == 1)
            def _():
                settle_own(0)

            @pl.when(step > 1)
            def _():
                settle(step - 1, (0,))

            return carry

        lax.fori_loop(1, early + 1, first_steps, 0)
        exchange.wait()
        each(lambda c: unit(at, c, (1,), True))
        lax.fori_loop(1, early + 1, lambda t, carry: (each(lambda c: visit(t, c, (1,), False)), carry)[1], 0)
        settle(early, (0,))

        def late_step(step, carry):
            each(lambda c: visit(step, c, (0, 1), True))

            @pl.when(step == early + 1)
            def _():
                settle_own(1)
                lax.fori_loop(1, early + 1, lambda t, inner: (settle(t, (1,)), inner)[1], 0)

            @pl.when(step > early + 1)
            def _():
                settle(step - 1, (0, 1))

            return carry

        if line - 1 > early:
            lax.fori_loop(early + 1, line, late_step, 0)
            settle(line - 1, (0, 1))
        else:
            settle_own(1)
            lax.fori_loop(1, early + 1, lambda t, inner: (settle(t, (1,)), inner)[1], 0)

        for way in range(2):
            for step in range(2):

                def finish(c):
                    @pl.when(leaves(way, step))
                    def _():
                        copy(way, step, c, step == 0).wait_send()

                if step == 0:
                    each(finish)
                else:

                    def finish_rest(t, carry):
                        def one(c):
                            @pl.when(leaves(way, t))
                            def _():
                                copy(way, t, c, False).wait_send()

                        each(one)
                        return carry

                    lax.fori_loop(1, line, finish_rest, 0)

        def drain(i, carry):
            for j in range(2):
                for k in range(1, heads):
                    to_head(i, j, mine, lax.rem(mine + k, heads)).wait_send()

                @pl.when(i != at)
                def _():
                    to_row(i, j, at).wait_send()
                    to_row(at, j, i).wait_recv()

            return carry

        lax.fori_loop(0, line, drain, 0)
        for i in range(n):
            out_ref[:, i * columns : (i + 1) * columns] = landed[i]

    return start_own, each, run


def project_kernel(n, heads, *refs):
    start_own, each, run = project_stages(n, heads, *refs)
    each(start_own)
    run()


def join_kernel(n, heads, o_ref, lse_ref, w_hbm, out_ref, x_ref, *refs):
    start_own, _, run = project_stages(n, heads, x_ref, w_hbm, out_ref, *refs[8:])
    per_way = BLK * heads // x_ref.shape[0]

    def ready(way):
        for c in range(per_way):
            start_own(way * per_way + c)

    drain = reduce_kernel(n, True, o_ref, lse_ref, x_ref, *refs[:8], ready=ready)
    run()
    drain()


def project_plan(n, heads, rows, width, columns, dtype):
    share = rows // heads
    line = n // 2
    dma = pltpu.SemaphoreType.DMA
    scratch = [
        pltpu.VMEM((2, width, columns), dtype),
        pltpu.VMEM((line, rows, width), dtype),
        pltpu.VMEM((line, 2, heads, share, columns), dtype),
        pltpu.VMEM((line, 2, heads, share, columns), dtype),
        pltpu.VMEM((line, 2, share, columns), dtype),
        pltpu.VMEM((n, share, columns), dtype),
        dma((1,)),
        dma((1,)),
        dma((1,)),
        dma((2, line, heads)),
        dma((2, line, heads)),
        dma((line, 2, heads)),
        dma((line, 2, heads)),
        dma((line, 2)),
        dma((line, 2)),
    ]
    padded = max(columns, BLK)
    held = [
        ((2, width, padded), dtype),
        ((line + 2, rows, width), dtype),
        ((2, n, heads, share, padded), dtype),
        ((3, n, share, padded), dtype),
    ]
    return scratch, held


def reduce_plan(n, small, kv_here, group_width):
    dma = pltpu.SemaphoreType.DMA((2, n - 1, kv_here))
    scratch = [
        pltpu.VMEM((2, n - 1, kv_here, BLK, group_width), jnp.bfloat16),
        pltpu.VMEM((2, n - 1, kv_here, STAT, BLK), jnp.float32),
        pltpu.VMEM((2, 2, 1 if small else kv_here, BLK, group_width), jnp.bfloat16),
        pltpu.SemaphoreType.DMA((2, 2)),
        dma,
        dma,
        dma,
        dma,
    ]
    held = [
        ((2, n + 1, kv_here, BLK, group_width), jnp.bfloat16),
        ((2, 2 * n - 1, kv_here, STAT, BLK), jnp.float32),
    ]
    return scratch, held


def mixed_from(parts, lse, weight, n, heads, rows, width, small):
    _, kv_here, _, group_width = parts.shape
    columns = weight.shape[1]
    vmem = pl.BlockSpec(memory_space=pltpu.VMEM)
    anywhere = pl.BlockSpec(memory_space=pl.ANY)
    reduce_scratch, reduce_held = reduce_plan(n, small, kv_here, group_width)
    project_scratch, project_held = project_plan(n, heads, rows, width, columns, parts.dtype)
    attended = jax.ShapeDtypeStruct((rows, width), parts.dtype)
    out = jax.ShapeDtypeStruct((rows // heads, n * columns), parts.dtype)

    def call(kernel, number, in_specs, out_shape, scratch, held):
        return pl.pallas_call(
            kernel,
            in_specs=in_specs,
            out_specs=vmem,
            out_shape=out_shape,
            scratch_shapes=scratch,
            compiler_params=pltpu.CompilerParams(
                collective_id=number, has_side_effects=True, vmem_limit_bytes=grant(*held)
            ),
            cost_estimate=long_cost(),
        )

    if small:
        scratch = [pltpu.VMEM((rows, width), parts.dtype)] + reduce_scratch + project_scratch
        held = reduce_held + project_held + [(parts.shape, parts.dtype)]
        kernel = functools.partial(join_kernel, n, heads)
        return call(kernel, 1, [vmem, vmem, anywhere], out, scratch, held)(parts, lse, weight)

    def kernel(*refs):
        reduce_kernel(n, small, *refs)

    x = call(kernel, 1, [anywhere, vmem], attended, reduce_scratch, reduce_held)(parts, lse)
    kernel = functools.partial(project_kernel, n, heads)
    return call(kernel, 2, [vmem, anywhere], out, project_scratch, project_held)(x, weight)


def body(
    queries,
    self_keys,
    self_values,
    store_keys,
    store_values,
    kv_slot,
    neighbours,
    counts,
    out_weight,
):
    n = lax.axis_size("seq")
    head_count = lax.axis_size("head")
    local_blocks, degree = neighbours.shape
    local_rows, width = queries.shape
    store_blocks = store_keys.shape[0] // BLK
    all_blocks = local_blocks * n
    kv_here = store_keys.shape[1] // DH
    group_width = (H // KVH) * DH
    rows = (H // KVH) * BLK
    all_queries, near, count = gathered(queries, neighbours, counts.reshape(1, local_blocks), n, 2)
    smem = pl.BlockSpec(memory_space=pltpu.SMEM)
    small = queries.size * n * queries.dtype.itemsize <= 8 << 20
    kind = pltpu.VMEM if small else jax.ShapeDtypeStruct
    q_spec = pl.BlockSpec((BLK, width), lambda i: (i, 0))
    o_spec = pl.BlockSpec((1, kv_here, BLK, group_width), lambda i: (i, 0, 0, 0))
    lse_spec = pl.BlockSpec((1, kv_here, STAT, BLK), lambda i: (i, 0, 0, 0))
    if small:
        q_spec = o_spec = lse_spec = pl.BlockSpec(memory_space=pltpu.VMEM)

    parts, lse = pl.pallas_call(
        functools.partial(part_kernel, local_blocks, store_blocks, small),
        grid=(all_blocks,),
        in_specs=[smem, smem, smem, q_spec]
        + [pl.BlockSpec(memory_space=pltpu.VMEM)] * 4,
        out_specs=[o_spec, lse_spec],
        out_shape=[
            kind((all_blocks, kv_here, BLK, group_width), jnp.bfloat16),
            kind((all_blocks, kv_here, STAT, BLK), jnp.float32),
        ],
        scratch_shapes=[
            pltpu.SMEM((degree + 1,), jnp.int32),
            pltpu.VMEM((kv_here, DH, rows), jnp.float32),
            pltpu.VMEM((kv_here, rows), jnp.float32),
            pltpu.VMEM((kv_here, rows), jnp.float32),
        ],
        compiler_params=pltpu.CompilerParams(vmem_limit_bytes=28 << 20),
        cost_estimate=pl.CostEstimate(flops=2_000_000_000, bytes_accessed=12 << 20, transcendentals=4_000_000),
    )(kv_slot, near, count, all_queries, self_keys, self_values, store_keys, store_values)
    return mixed_from(parts, lse, out_weight, n, head_count, local_rows, width, small)


def solution(mesh):
    placed = (
        P("seq", "head"),
        P("seq", "head"),
        P("seq", "head"),
        P("seq", "head"),
        P("seq", "head"),
        P(),
        P("seq", None),
        P("seq"),
        P("head", "seq"),
    )
    return jax.shard_map(
        body, mesh=mesh, in_specs=placed, out_specs=P(("seq", "head"), None), check_vma=False
    )
```

```python
import functools

import jax
import jax.numpy as jnp
from jax import lax
from jax.experimental import pallas as pl
from jax.experimental.pallas import tpu as pltpu
from jax.sharding import PartitionSpec as P

H = 32
KVH = 8
DH = 128
BLK = 128
NEG = -1e30
STAT = 8
SCAN = 4
LOG2E = 1.4426950408889634
MESH = pl.DeviceIdType.MESH


def asked_rows(q_ref, first_row, g, per_group):
    return jnp.concatenate(
        [
            q_ref[pl.ds(first_row, BLK), (g * per_group + r) * DH : (g * per_group + r + 1) * DH]
            for r in range(per_group)
        ],
        axis=0,
    )


def scores_of(keys, asked):
    scaling = DH ** (-0.5) * LOG2E
    return lax.dot_general(keys, asked, (((1,), (1,)), ((), ())), preferred_element_type=jnp.float32) * scaling


def weighed(values, p):
    return lax.dot_general(
        values, p.astype(jnp.bfloat16), (((0,), (0,)), ((), ())), preferred_element_type=jnp.float32
    )


def causal_mask(rows):
    position = lax.rem(lax.broadcasted_iota(jnp.int32, (BLK, rows), 1), BLK)
    return position >= lax.broadcasted_iota(jnp.int32, (BLK, rows), 0)


def write_part(o_ref, lse_ref, here, g, acc, total, lse):
    per_group = lse.shape[1] // BLK
    o_ref[here, g] = (acc * (1.0 / total)).astype(jnp.bfloat16)
    for r in range(STAT):
        at = (r % per_group) * BLK
        lse_ref[here, g, r : r + 1] = lse[:, at : at + BLK]


def part_row(
    block,
    here,
    first_row,
    done,
    local_blocks,
    store_blocks,
    slot_ref,
    near_ref,
    count_ref,
    q_ref,
    sk_ref,
    sv_ref,
    k_ref,
    v_ref,
    o_ref,
    lse_ref,
    list_ref,
    acc_ref,
    max_ref,
    sum_ref,
):
    owner, inner = lax.div(block, local_blocks), lax.rem(block, local_blocks)
    me = lax.axis_index("seq")
    per_group = H // KVH
    kv_here = k_ref.shape[1] // DH
    rows = per_group * BLK
    listed = count_ref[owner, 0, inner]
    first_slot = me * store_blocks

    def scan_entries(i, found):
        places = [slot_ref[near_ref[owner, inner, i * SCAN + u]] - first_slot for u in range(SCAN)]
        for u, place in enumerate(places):
            list_ref[found] = place
            kept = (place >= 0) & (place < store_blocks) & (i * SCAN + u < listed)
            found = found + kept.astype(jnp.int32)
        return found

    found = lax.fori_loop(0, lax.div(listed + (SCAN - 1), SCAN), scan_entries, jnp.int32(0))
    home = owner == me
    if not done:

        @pl.when(jnp.logical_and(found == 0, jnp.logical_not(home)))
        def _():
            o_ref[here] = jnp.zeros(o_ref.shape[1:], o_ref.dtype)
            lse_ref[here] = jnp.full(lse_ref.shape[1:], NEG, lse_ref.dtype)

    @pl.when(found > done if done else jnp.logical_or(found > 0, home))
    def _():
        if done:
            for g in range(kv_here):
                max_ref[g : g + 1] = jnp.concatenate(
                    [lse_ref[here, g, r : r + 1] for r in range(per_group)], axis=1
                )
                sum_ref[g : g + 1] = jnp.ones((1, rows), jnp.float32)
                acc_ref[g] = o_ref[here, g].astype(jnp.float32)
        else:

            @pl.when(home)
            def _():
                start = pl.multiple_of(inner * BLK, BLK)
                for g in range(kv_here):
                    cols = slice(g * DH, (g + 1) * DH)
                    asked = asked_rows(q_ref, first_row, g, per_group)
                    s = jnp.where(causal_mask(rows), scores_of(sk_ref[pl.ds(start, BLK), cols], asked), NEG)
                    m = jnp.max(s, axis=0, keepdims=True)
                    p = jnp.exp2(s - m)
                    max_ref[g : g + 1] = m
                    sum_ref[g : g + 1] = jnp.sum(p, axis=0, keepdims=True)
                    acc_ref[g] = weighed(sv_ref[pl.ds(start, BLK), cols], p)

            @pl.when(jnp.logical_not(home))
            def _():
                max_ref[...] = jnp.full_like(max_ref, NEG)
                sum_ref[...] = jnp.zeros_like(sum_ref)
                acc_ref[...] = jnp.zeros_like(acc_ref)

        def take(*places):
            starts = [pl.multiple_of(place * BLK, BLK) for place in places]

            def rows_of(ref, cols):
                return jnp.concatenate([ref[pl.ds(start, BLK), cols] for start in starts], axis=0)

            for g in range(kv_here):
                cols = slice(g * DH, (g + 1) * DH)
                s = scores_of(rows_of(k_ref, cols), asked_rows(q_ref, first_row, g, per_group))
                old = max_ref[g : g + 1]
                new = jnp.maximum(old, jnp.max(s, axis=0, keepdims=True))
                p = jnp.exp2(s - new)
                shrink = jnp.exp2(old - new)
                max_ref[g : g + 1] = new
                sum_ref[g : g + 1] = sum_ref[g : g + 1] * shrink + jnp.sum(p, axis=0, keepdims=True)
                acc_ref[g] = acc_ref[g] * shrink + weighed(rows_of(v_ref, cols), p)

        left = found - done

        @pl.loop(0, lax.div(left, 2))
        def _(i):
            take(list_ref[done + 2 * i], list_ref[done + 2 * i + 1])

        @pl.when(lax.rem(left, 2) == 1)
        def _():
            take(list_ref[found - 1])

        for g in range(kv_here):
            total = sum_ref[g : g + 1]
            write_part(o_ref, lse_ref, here, g, acc_ref[g], total, max_ref[g : g + 1] + jnp.log2(total))


def part_kernel(local_blocks, store_blocks, *refs):
    block = pl.program_id(0)
    part_row(block, 0, 0, 0, local_blocks, store_blocks, *refs)


def rest_kernel(local_blocks, store_blocks, *refs):
    def row(block, carry):
        first_row = pl.multiple_of(block * BLK, BLK)
        part_row(block, block, first_row, 1, local_blocks, store_blocks, *refs[:8], *refs[10:])
        return carry

    lax.fori_loop(0, refs[10].shape[0], row, 0)


def grant(*arrays):
    size = 0
    for shape, dtype in arrays:
        cells = 1
        for d in shape:
            cells = cells * d
        size += cells * jnp.dtype(dtype).itemsize
    return min(size + (4 << 20), 60 << 20)


def long_cost():
    return pl.CostEstimate(flops=200_000_000_000, bytes_accessed=1 << 20, transcendentals=0)


def ring_place(index, n):
    odd = lax.rem(index, 2)
    half = index // 2
    return (1 - odd) * half + odd * (n - 1 - half)


def ring_index(place, n):
    place = lax.rem(place + 2 * n, n)
    far = place // (n // 2)
    return (1 - far) * (2 * place) + far * (2 * (n - 1 - place) + 1)


def gather_kernel(n, pieces, early, *refs):
    refs = list(refs)

    def some(count):
        return [refs.pop(0) for _ in range(count)]

    x_ref, near_ref, count_ref = some(3)
    if early:
        slot_hbm, *store_hbm = some(5)
    out_ref, nears_ref, counts_ref = some(3)
    if early:
        o_ref, lse_ref, slot_ref, near_smem, count_smem, sk_ref, sv_ref, k_ref, v_ref, load_sem = some(10)
    own_sem, send_sem, recv_sem, tsend_sem, trecv_sem = refs
    me = lax.axis_index("seq")
    place = ring_place(me, n)
    rows = x_ref.shape[0]
    sub = rows // pieces
    half = n // 2
    ways = (1, -1)
    beside = [ring_index(place + way, n) for way in ways]
    own = [
        pltpu.make_async_copy(source, target, own_sem.at[i])
        for i, (source, target) in enumerate(
            (
                (x_ref, out_ref.at[pl.ds(pl.multiple_of(me * rows, rows), rows)]),
                (near_ref, nears_ref.at[me]),
                (count_ref, counts_ref.at[me]),
            )
        )
    ]
    for one in own:
        one.start()
    loads = []
    if early:
        sources = [slot_hbm] + store_hbm
        for i, (source, target) in enumerate(zip(sources, (slot_ref, sk_ref, sv_ref, k_ref, v_ref))):
            loads.append(pltpu.make_async_copy(source, target, load_sem.at[i]))
    for one in loads:
        one.start()
    barrier = pltpu.get_barrier_semaphore()
    for k in range(1, n):
        pl.semaphore_signal(barrier, inc=1, device_id={"seq": lax.rem(me + k, n)}, device_id_type=MESH)
    for one in own:
        one.wait()
    pl.semaphore_wait(barrier, n - 1)

    def copy(way, step, piece):
        owner = ring_index(place - ways[way] * step, n)
        there = pl.ds(pl.multiple_of(owner * rows + piece * sub, sub), sub)
        return pltpu.make_async_remote_copy(
            src_ref=out_ref.at[there],
            dst_ref=out_ref.at[there],
            send_sem=send_sem.at[way, step, piece],
            recv_sem=recv_sem.at[way, step, piece],
            device_id={"seq": beside[way]},
            device_id_type=MESH,
        )

    def piece_of(way, spot):
        return spot if way == 0 else pieces - 1 - spot

    started = []
    for spot in range(pieces):
        for way in range(2):
            one = copy(way, 0, piece_of(way, spot))
            one.start()
            started.append(one)
    table_copies = []
    for t, target in enumerate((nears_ref, counts_ref)):
        for k in range(1, n):
            table_copies.append(
                pltpu.make_async_remote_copy(
                    src_ref=target.at[me],
                    dst_ref=target.at[me],
                    send_sem=tsend_sem.at[t, k],
                    recv_sem=trecv_sem.at[t, k],
                    device_id={"seq": lax.rem(me + k, n)},
                    device_id_type=MESH,
                )
            )
    for one in table_copies:
        one.start()

    def first_listed(owner, inner):
        degree = near_ref.shape[1]
        store_blocks = k_ref.shape[0]
        listed = count_smem[owner, 0, inner]

        def look(i, best):
            e = degree - SCAN * (i + 1)
            for u in range(SCAN - 1, -1, -1):
                spot = slot_ref[near_smem[owner, inner, e + u]] - me * store_blocks
                kept = ((spot >= 0) & (spot < store_blocks) & (e + u < listed)).astype(jnp.int32)
                best = best + kept * (spot - best)
            return best

        return lax.fori_loop(0, degree // SCAN, look, jnp.int32(-1))

    def row_work(owner, inner, mine):
        per_group = H // KVH
        spot = first_listed(owner, inner)
        taken = jnp.maximum(spot, 0)
        missing = jnp.minimum(spot, 0).astype(jnp.float32) * -NEG
        first_row = pl.multiple_of(owner * rows + inner * BLK, BLK)
        for g in range(k_ref.shape[2] // DH):
            cols = slice(g * DH, (g + 1) * DH)
            asked = asked_rows(out_ref, first_row, g, per_group)
            keys, values = k_ref[taken, :, cols], v_ref[taken, :, cols]
            if mine:
                near = pl.ds(pl.multiple_of(inner * BLK, BLK), BLK)
                keys = jnp.concatenate([sk_ref[near, cols], keys], axis=0)
                values = jnp.concatenate([sv_ref[near, cols], values], axis=0)
            s = scores_of(keys, asked)
            if mine:
                inside = jnp.where(causal_mask(s.shape[1]), s[:BLK], NEG)
                s = jnp.concatenate([inside, s[BLK:] + missing], axis=0)
            m = jnp.max(s, axis=0, keepdims=True)
            p = jnp.exp2(s - m)
            total = jnp.sum(p, axis=0, keepdims=True)
            lse = m + jnp.log2(total)
            if not mine:
                lse = lse + missing
            write_part(o_ref, lse_ref, owner * pieces + inner, g, weighed(values, p), total, lse)

    def arrived(step, spot):
        if not early:
            return

        def one(way, carry):
            owner = ring_index(place - (1 - 2 * way) * step, n)
            row_work(owner, spot + way * (pieces - 1 - 2 * spot), False)
            return carry

        lax.fori_loop(0, 2, one, 0)

    if early:
        for one in table_copies:
            one.wait_recv()
        tables = [
            pltpu.make_async_copy(source, target, load_sem.at[5 + i])
            for i, (source, target) in enumerate(((nears_ref, near_smem), (counts_ref, count_smem)))
        ]
        for one in tables:
            one.start()
        for one in loads + tables:
            one.wait()
        lax.fori_loop(0, pieces, lambda inner, carry: (row_work(me, inner, True), carry)[1], 0)
    for step in range(1, half):
        for spot in range(pieces):
            for way in range(2):
                copy(way, step - 1, piece_of(way, spot)).wait_recv()
                if step < half - 1 or spot < pieces // 2:
                    one = copy(way, step, piece_of(way, spot))
                    one.start()
                    started.append(one)
            arrived(step, spot)
    for spot in range(pieces // 2):
        for way in range(2):
            copy(way, half - 1, piece_of(way, spot)).wait_recv()
        arrived(half, spot)
    for one in started:
        one.wait_send()
    for one in table_copies:
        if early:
            one.wait_send()
        else:
            one.wait()


def gathered(x, near, count, n, early):
    rows, width = x.shape
    pieces = rows // BLK
    vmem = pl.BlockSpec(memory_space=pltpu.VMEM)
    dma = pltpu.SemaphoreType.DMA
    kind = pltpu.VMEM if early else jax.ShapeDtypeStruct
    inputs = [x, near, count] + list(early)
    out_shape = [
        kind((n * rows, width), x.dtype),
        jax.ShapeDtypeStruct((n,) + near.shape, near.dtype),
        jax.ShapeDtypeStruct((n,) + count.shape, count.dtype),
    ]
    scratch = []
    held = [((n + 1, rows, width), x.dtype)]
    if early:
        slot, *stores = early
        kv_here = stores[2].shape[2] // DH
        part_shape = (n * pieces, kv_here, BLK, (H // KVH) * DH)
        out_shape += [kind(part_shape, x.dtype), kind((n * pieces, kv_here, STAT, BLK), jnp.float32)]
        scratch += [pltpu.SMEM(slot.shape, slot.dtype)]
        scratch += [pltpu.SMEM(out_shape[1].shape, near.dtype), pltpu.SMEM(out_shape[2].shape, count.dtype)]
        scratch += [pltpu.VMEM(a.shape, a.dtype) for a in stores]
        scratch += [dma((7,))]
        held += [(part_shape, x.dtype)] + [(a.shape, a.dtype) for a in stores]
    scratch += [
        dma((3,)),
        dma((2, n // 2, pieces)),
        dma((2, n // 2, pieces)),
        dma((2, n)),
        dma((2, n)),
    ]
    return pl.pallas_call(
        functools.partial(gather_kernel, n, pieces, bool(early)),
        in_specs=[pl.BlockSpec(memory_space=pltpu.HBM)] * len(inputs),
        out_specs=[vmem] * len(out_shape),
        out_shape=out_shape,
        scratch_shapes=scratch,
        compiler_params=pltpu.CompilerParams(
            collective_id=0,
            has_side_effects=True,
            vmem_limit_bytes=grant(*held),
        ),
        cost_estimate=long_cost(),
    )(*(pltpu.with_memory_space_constraint(a, pltpu.HBM) for a in inputs))


def merge(lse_a, lse_b):
    top = jnp.maximum(lse_a, lse_b)
    a = jnp.exp2(lse_a - top)
    b = jnp.exp2(lse_b - top)
    total = a + b
    return a / total, b / total, top + jnp.log2(total)


def reduce_kernel(
    n,
    small,
    o_ref,
    lse_ref,
    out_ref,
    got,
    got_lse,
    own,
    own_sem,
    send_sem,
    recv_sem,
    lsend_sem,
    lrecv_sem,
    ready=None,
):
    me = lax.axis_index("seq")
    place = ring_place(me, n)
    groups, width = got.shape[2], got.shape[4]
    ways = (1, -1)
    beside = [ring_index(place + way, n) for way in ways]
    if ready is None:
        barrier = pltpu.get_barrier_semaphore()
        for other in beside:
            pl.semaphore_signal(barrier, inc=1, device_id={"seq": other}, device_id_type=MESH)

    def home(way, step):
        return ring_index(place - ways[way] * (1 + step), n)

    def fetch(way, step):
        return pltpu.make_async_copy(
            o_ref.at[home(way, step) * 2 + way], own.at[way, lax.rem(step, 2)], own_sem.at[way, lax.rem(step, 2)]
        )

    def copies(way, step, g, before):
        at = home(way, step) * 2 + way
        first = before is None
        return (
            pltpu.make_async_remote_copy(
                src_ref=lse_ref.at[at, g] if first else got_lse.at[way, before, g],
                dst_ref=got_lse.at[way, step, g],
                send_sem=lsend_sem.at[way, step, g],
                recv_sem=lrecv_sem.at[way, step, g],
                device_id={"seq": beside[way]},
                device_id_type=MESH,
            ),
            pltpu.make_async_remote_copy(
                src_ref=o_ref.at[at, g] if first else got.at[way, before, g],
                dst_ref=got.at[way, step, g],
                send_sem=send_sem.at[way, step, g],
                recv_sem=recv_sem.at[way, step, g],
                device_id={"seq": beside[way]},
                device_id_type=MESH,
            ),
        )

    def merged(way, step, g):
        for one in copies(way, step - 1, g, step - 1):
            one.wait_recv()
        if g == 0 and not small:
            fetch(way, step).wait()
        at = home(way, step) * 2 + way
        theirs, ours, lse = merge(got_lse[way, step - 1, g], lse_ref[at, g])
        columns = []
        for r in range(width // DH):
            cols = slice(r * DH, (r + 1) * DH)
            mine = o_ref[at, g, :, cols] if small else own[way, lax.rem(step, 2), g, :, cols]
            columns.append(
                got[way, step - 1, g, :, cols].astype(jnp.float32) * theirs[r : r + 1]
                + mine.astype(jnp.float32) * ours[r : r + 1]
            )
        return columns, lse

    if not small:
        for way in range(2):
            fetch(way, 1).start()
    if ready is None:
        pl.semaphore_wait(barrier, 2)
    for g in range(groups):
        for way in range(2):
            for one in copies(way, 0, g, None):
                one.start()

    def one_step(step, carry):
        if not small:
            for way in range(2):
                fetch(way, step + 1).start()
        for g in range(groups):
            for way in range(2):
                columns, lse = merged(way, step, g)
                got_lse[way, step - 1, g] = lse
                for r, value in enumerate(columns):
                    got[way, step - 1, g, :, r * DH : (r + 1) * DH] = value.astype(jnp.bfloat16)
                for one in copies(way, step, g, step - 1):
                    one.start()
        return carry

    lax.fori_loop(1, n - 1, one_step, 0)
    for way in range(2):
        for g in range(groups):
            columns, _ = merged(way, n - 1, g)
            for r, value in enumerate(columns):
                at = g * width + r * DH
                out_ref[way * BLK : (way + 1) * BLK, at : at + DH] = jnp.transpose(value).astype(jnp.bfloat16)
        if ready is not None:
            ready(way)

    def drain_all():
        for g in range(groups):
            for way in range(2):
                for one in copies(way, 0, g, None):
                    one.wait_send()

        def drain(step, carry):
            for g in range(groups):
                for way in range(2):
                    for one in copies(way, step, g, step - 1):
                        one.wait_send()
            return carry

        lax.fori_loop(1, n - 1, drain, 0)

    if ready is None:
        drain_all()
    return drain_all


def project_stages(
    n,
    heads,
    x_ref,
    w_hbm,
    out_ref,
    w_ref,
    blocks,
    split,
    got,
    summed,
    landed,
    w_sem,
    wsend,
    wrecv,
    send_sem,
    recv_sem,
    hsend,
    hrecv,
    fsend,
    frecv,
):
    me = lax.axis_index("seq")
    mine = lax.axis_index("head")
    line = n // 2
    at, side = me // 2, lax.rem(me, 2)
    share = x_ref.shape[0] // heads
    columns = w_ref.shape[2]
    ways = (1, -1)
    early = min(2, line - 1)
    weights = pltpu.make_async_copy(w_hbm, w_ref.at[0], w_sem.at[0])
    weights.start()
    barrier = pltpu.get_barrier_semaphore()
    place = ring_place(me, n)
    for way in ways:
        other = ring_index(place + way, n)
        pl.semaphore_signal(barrier, inc=1, device_id={"seq": other}, device_id_type=MESH)
    for k in range(1, heads):
        pl.semaphore_signal(barrier, inc=1, device_id={"head": lax.rem(mine + k, heads)}, device_id_type=MESH)
    for k in range(1, line):
        other = lax.rem(at + k, line) * 2 + side
        pl.semaphore_signal(barrier, inc=1, device_id={"seq": other}, device_id_type=MESH)
    partner = at * 2 + 1 - side
    pl.semaphore_signal(barrier, inc=1, device_id={"seq": partner}, device_id_type=MESH)
    pl.semaphore_wait(barrier, heads + line + 1)

    def inside(spot):
        return jnp.logical_and(spot >= 0, spot < line)

    def copy(way, step, piece, first):
        there = (at - ways[way] * step, pl.ds(pl.multiple_of(piece * share, share), share))
        return pltpu.make_async_remote_copy(
            src_ref=x_ref.at[there[1]] if first else blocks.at[there],
            dst_ref=blocks.at[there],
            send_sem=send_sem.at[way, step, piece],
            recv_sem=recv_sem.at[way, step, piece],
            device_id={"seq": (at + ways[way]) * 2 + side},
            device_id_type=MESH,
        )

    def leaves(way, step):
        return jnp.logical_and(inside(at - ways[way] * step), inside(at + ways[way]))

    def to_head(i, j, source, to):
        return pltpu.make_async_remote_copy(
            src_ref=split.at[i, j, to],
            dst_ref=got.at[i, j, source],
            send_sem=hsend.at[i, j, to],
            recv_sem=hrecv.at[i, j, source],
            device_id={"head": to},
            device_id_type=MESH,
        )

    def to_row(i, j, source):
        owner = source * 2 + (side if j == 0 else 1 - side)
        return pltpu.make_async_remote_copy(
            src_ref=summed.at[i, j],
            dst_ref=landed.at[owner],
            send_sem=fsend.at[i, j],
            recv_sem=frecv.at[source, j],
            device_id={"seq": i * 2 + side},
            device_id_type=MESH,
        )

    def unit(i, c, js, own):
        rows = pl.ds(pl.multiple_of(c * share, share), share)
        value = x_ref[rows] if own else blocks[i, rows]
        for j in js:
            split[i, j, c] = jnp.dot(value, w_ref[j], preferred_element_type=jnp.float32).astype(jnp.bfloat16)

            @pl.when(mine != c)
            def _():
                to_head(i, j, mine, c).start()

    def visit(step, c, js, arriving):
        for way in range(2):
            i = at - ways[way] * step

            @pl.when(inside(i))
            def _():
                if arriving:
                    copy(way, step - 1, c, False).wait_recv()

                    @pl.when(inside(at + ways[way]))
                    def _():
                        copy(way, step, c, False).start()

                unit(i, c, js, False)

    def total_of(i, j):
        total = split[i, j, mine].astype(jnp.float32)
        for k in range(1, heads):
            source = lax.rem(mine + k, heads)
            to_head(i, j, source, mine).wait_recv()
            total = total + got[i, j, source].astype(jnp.float32)
        return total.astype(jnp.bfloat16)

    def settle_own(j):
        landed[at * 2 + (side if j == 0 else 1 - side)] = total_of(at, j)

    def settle(step, js):
        for way in range(2):
            i = at - ways[way] * step

            @pl.when(inside(i))
            def _():
                for j in js:
                    summed[i, j] = total_of(i, j)
                    to_row(i, j, at).start()

    def each(function):
        lax.fori_loop(0, heads, lambda c, carry: (function(c), carry)[1], 0)

    def start_own(c):
        for way in range(2):

            @pl.when(inside(at + ways[way]))
            def _():
                copy(way, 0, c, True).start()

    def run():
        weights.wait()
        exchange = pltpu.make_async_remote_copy(
            src_ref=w_ref.at[0],
            dst_ref=w_ref.at[1],
            send_sem=wsend.at[0],
            recv_sem=wrecv.at[0],
            device_id={"seq": partner},
            device_id_type=MESH,
        )
        exchange.start()
        each(lambda c: unit(at, c, (0,), True))

        def first_steps(step, carry):
            each(lambda c: visit(step, c, (0,), True))

            @pl.when(step == 1)
            def _():
                settle_own(0)

            @pl.when(step > 1)
            def _():
                settle(step - 1, (0,))

            return carry

        lax.fori_loop(1, early + 1, first_steps, 0)
        exchange.wait()
        each(lambda c: unit(at, c, (1,), True))
        lax.fori_loop(1, early + 1, lambda t, carry: (each(lambda c: visit(t, c, (1,), False)), carry)[1], 0)
        settle(early, (0,))

        def late_step(step, carry):
            each(lambda c: visit(step, c, (0, 1), True))

            @pl.when(step == early + 1)
            def _():
                settle_own(1)
                lax.fori_loop(1, early + 1, lambda t, inner: (settle(t, (1,)), inner)[1], 0)

            @pl.when(step > early + 1)
            def _():
                settle(step - 1, (0, 1))

            return carry

        if line - 1 > early:
            lax.fori_loop(early + 1, line, late_step, 0)
            settle(line - 1, (0, 1))
        else:
            settle_own(1)
            lax.fori_loop(1, early + 1, lambda t, inner: (settle(t, (1,)), inner)[1], 0)

        for way in range(2):
            for step in range(2):

                def finish(c):
                    @pl.when(leaves(way, step))
                    def _():
                        copy(way, step, c, step == 0).wait_send()

                if step == 0:
                    each(finish)
                else:

                    def finish_rest(t, carry):
                        def one(c):
                            @pl.when(leaves(way, t))
                            def _():
                                copy(way, t, c, False).wait_send()

                        each(one)
                        return carry

                    lax.fori_loop(1, line, finish_rest, 0)

        def drain(i, carry):
            for j in range(2):
                for k in range(1, heads):
                    to_head(i, j, mine, lax.rem(mine + k, heads)).wait_send()

                @pl.when(i != at)
                def _():
                    to_row(i, j, at).wait_send()
                    to_row(at, j, i).wait_recv()

            return carry

        lax.fori_loop(0, line, drain, 0)
        for i in range(n):
            out_ref[:, i * columns : (i + 1) * columns] = landed[i]

    return start_own, each, run


def project_kernel(n, heads, *refs):
    start_own, each, run = project_stages(n, heads, *refs)
    each(start_own)
    run()


def join_kernel(n, heads, o_ref, lse_ref, w_hbm, out_ref, x_ref, *refs):
    start_own, _, run = project_stages(n, heads, x_ref, w_hbm, out_ref, *refs[8:])
    per_way = BLK * heads // x_ref.shape[0]

    def ready(way):
        for c in range(per_way):
            start_own(way * per_way + c)

    drain = reduce_kernel(n, True, o_ref, lse_ref, x_ref, *refs[:8], ready=ready)
    run()
    drain()


def project_plan(n, heads, rows, width, columns, dtype):
    share = rows // heads
    line = n // 2
    dma = pltpu.SemaphoreType.DMA
    scratch = [
        pltpu.VMEM((2, width, columns), dtype),
        pltpu.VMEM((line, rows, width), dtype),
        pltpu.VMEM((line, 2, heads, share, columns), dtype),
        pltpu.VMEM((line, 2, heads, share, columns), dtype),
        pltpu.VMEM((line, 2, share, columns), dtype),
        pltpu.VMEM((n, share, columns), dtype),
        dma((1,)),
        dma((1,)),
        dma((1,)),
        dma((2, line, heads)),
        dma((2, line, heads)),
        dma((line, 2, heads)),
        dma((line, 2, heads)),
        dma((line, 2)),
        dma((line, 2)),
    ]
    padded = max(columns, BLK)
    held = [
        ((2, width, padded), dtype),
        ((line + 2, rows, width), dtype),
        ((2, n, heads, share, padded), dtype),
        ((3, n, share, padded), dtype),
    ]
    return scratch, held


def reduce_plan(n, small, kv_here, group_width):
    dma = pltpu.SemaphoreType.DMA((2, n - 1, kv_here))
    scratch = [
        pltpu.VMEM((2, n - 1, kv_here, BLK, group_width), jnp.bfloat16),
        pltpu.VMEM((2, n - 1, kv_here, STAT, BLK), jnp.float32),
        pltpu.VMEM((2, 2, 1 if small else kv_here, BLK, group_width), jnp.bfloat16),
        pltpu.SemaphoreType.DMA((2, 2)),
        dma,
        dma,
        dma,
        dma,
    ]
    held = [
        ((2, n + 1, kv_here, BLK, group_width), jnp.bfloat16),
        ((2, 2 * n - 1, kv_here, STAT, BLK), jnp.float32),
    ]
    return scratch, held


def mixed_from(parts, lse, weight, n, heads, rows, width, small):
    _, kv_here, _, group_width = parts.shape
    columns = weight.shape[1]
    vmem = pl.BlockSpec(memory_space=pltpu.VMEM)
    anywhere = pl.BlockSpec(memory_space=pl.ANY)
    reduce_scratch, reduce_held = reduce_plan(n, small, kv_here, group_width)
    project_scratch, project_held = project_plan(n, heads, rows, width, columns, parts.dtype)
    attended = jax.ShapeDtypeStruct((rows, width), parts.dtype)
    out = jax.ShapeDtypeStruct((rows // heads, n * columns), parts.dtype)

    def call(kernel, number, in_specs, out_shape, scratch, held):
        return pl.pallas_call(
            kernel,
            in_specs=in_specs,
            out_specs=vmem,
            out_shape=out_shape,
            scratch_shapes=scratch,
            compiler_params=pltpu.CompilerParams(
                collective_id=number, has_side_effects=True, vmem_limit_bytes=grant(*held)
            ),
            cost_estimate=long_cost(),
        )

    if small:
        scratch = [pltpu.VMEM((rows, width), parts.dtype)] + reduce_scratch + project_scratch
        held = reduce_held + project_held + [(parts.shape, parts.dtype)]
        kernel = functools.partial(join_kernel, n, heads)
        return call(kernel, 1, [vmem, vmem, anywhere], out, scratch, held)(parts, lse, weight)

    def kernel(*refs):
        reduce_kernel(n, small, *refs)

    x = call(kernel, 1, [anywhere, vmem], attended, reduce_scratch, reduce_held)(parts, lse)
    kernel = functools.partial(project_kernel, n, heads)
    return call(kernel, 2, [vmem, anywhere], out, project_scratch, project_held)(x, weight)


def body(
    queries,
    self_keys,
    self_values,
    store_keys,
    store_values,
    kv_slot,
    neighbours,
    counts,
    out_weight,
):
    n = lax.axis_size("seq")
    head_count = lax.axis_size("head")
    local_blocks, degree = neighbours.shape
    local_rows, width = queries.shape
    store_blocks = store_keys.shape[0] // BLK
    all_blocks = local_blocks * n
    kv_here = store_keys.shape[1] // DH
    group_width = (H // KVH) * DH
    rows = (H // KVH) * BLK
    small = queries.size * n * queries.dtype.itemsize <= 8 << 20
    count_row = counts.reshape(1, local_blocks)
    stores = (self_keys, self_values, store_keys, store_values)
    cut = tuple(a.reshape(store_blocks, BLK, -1) for a in stores[2:])
    smem = pl.BlockSpec(memory_space=pltpu.SMEM)
    vmem = pl.BlockSpec(memory_space=pltpu.VMEM)
    params = pltpu.CompilerParams(vmem_limit_bytes=28 << 20)
    cost = pl.CostEstimate(flops=2_000_000_000, bytes_accessed=12 << 20, transcendentals=4_000_000)
    scratch = [
        pltpu.SMEM((degree + 1,), jnp.int32),
        pltpu.VMEM((kv_here, DH, rows), jnp.float32),
        pltpu.VMEM((kv_here, rows), jnp.float32),
        pltpu.VMEM((kv_here, rows), jnp.float32),
    ]
    part_shape = (all_blocks, kv_here, BLK, group_width)
    lse_shape = (all_blocks, kv_here, STAT, BLK)
    if small:
        all_queries, near, count, parts, lse = gathered(queries, neighbours, count_row, n, (kv_slot,) + stores[:2] + cut)
        parts, lse = pl.pallas_call(
            functools.partial(rest_kernel, local_blocks, store_blocks),
            in_specs=[smem] * 3 + [vmem] * 7,
            out_specs=[vmem, vmem],
            out_shape=[pltpu.VMEM(part_shape, jnp.bfloat16), pltpu.VMEM(lse_shape, jnp.float32)],
            scratch_shapes=scratch,
            input_output_aliases={8: 0, 9: 1},
            compiler_params=params,
            cost_estimate=cost,
        )(kv_slot, near, count, all_queries, *stores, parts, lse)
    else:
        all_queries, near, count = gathered(queries, neighbours, count_row, n, ())
        parts, lse = pl.pallas_call(
            functools.partial(part_kernel, local_blocks, store_blocks),
            grid=(all_blocks,),
            in_specs=[smem] * 3 + [pl.BlockSpec((BLK, width), lambda i: (i, 0))] + [vmem] * 4,
            out_specs=[
                pl.BlockSpec((1, kv_here, BLK, group_width), lambda i: (i, 0, 0, 0)),
                pl.BlockSpec((1, kv_here, STAT, BLK), lambda i: (i, 0, 0, 0)),
            ],
            out_shape=[
                jax.ShapeDtypeStruct(part_shape, jnp.bfloat16),
                jax.ShapeDtypeStruct(lse_shape, jnp.float32),
            ],
            scratch_shapes=scratch,
            compiler_params=params,
            cost_estimate=cost,
        )(kv_slot, near, count, all_queries, *stores)
    return mixed_from(parts, lse, out_weight, n, head_count, local_rows, width, small)


def solution(mesh):
    placed = (
        P("seq", "head"),
        P("seq", "head"),
        P("seq", "head"),
        P("seq", "head"),
        P("seq", "head"),
        P(),
        P("seq", None),
        P("seq"),
        P("head", "seq"),
    )
    return jax.shard_map(
        body, mesh=mesh, in_specs=placed, out_specs=P(("seq", "head"), None), check_vma=False
    )
```

```python
import functools

import jax
import jax.numpy as jnp
from jax import lax
from jax.experimental import pallas as pl
from jax.experimental.pallas import tpu as pltpu
from jax.sharding import PartitionSpec as P

H = 32
KVH = 8
DH = 128
BLK = 128
NEG = -1e30
STAT = 8
SCAN = 4
CUTS = 2
LOG2E = 1.4426950408889634
MESH = pl.DeviceIdType.MESH


def asked_rows(q_ref, first_row, g, per_group):
    return jnp.concatenate(
        [
            q_ref[pl.ds(first_row, BLK), (g * per_group + r) * DH : (g * per_group + r + 1) * DH]
            for r in range(per_group)
        ],
        axis=0,
    )


def scores_of(keys, asked):
    scaling = DH ** (-0.5) * LOG2E
    return lax.dot_general(keys, asked, (((1,), (1,)), ((), ())), preferred_element_type=jnp.float32) * scaling


def weighed(values, p):
    return lax.dot_general(
        values, p.astype(jnp.bfloat16), (((0,), (0,)), ((), ())), preferred_element_type=jnp.float32
    )


def causal_mask(rows):
    position = lax.rem(lax.broadcasted_iota(jnp.int32, (BLK, rows), 1), BLK)
    return position >= lax.broadcasted_iota(jnp.int32, (BLK, rows), 0)


def write_part(o_ref, lse_ref, here, g, acc, total, lse):
    per_group = lse.shape[1] // BLK
    o_ref[here, g] = (acc * (1.0 / total)).astype(jnp.bfloat16)
    for r in range(STAT):
        at = (r % per_group) * BLK
        lse_ref[here, g, r : r + 1] = lse[:, at : at + BLK]


def part_row(
    block,
    here,
    first_row,
    done,
    local_blocks,
    store_blocks,
    slot_ref,
    near_ref,
    count_ref,
    q_ref,
    sk_ref,
    sv_ref,
    k_ref,
    v_ref,
    o_ref,
    lse_ref,
    list_ref,
    acc_ref,
    max_ref,
    sum_ref,
):
    owner, inner = lax.div(block, local_blocks), lax.rem(block, local_blocks)
    me = lax.axis_index("seq")
    per_group = H // KVH
    kv_here = k_ref.shape[1] // DH
    rows = per_group * BLK
    listed = count_ref[owner, 0, inner]
    first_slot = me * store_blocks

    def scan_entries(i, found):
        places = [slot_ref[near_ref[owner, inner, i * SCAN + u]] - first_slot for u in range(SCAN)]
        for u, place in enumerate(places):
            list_ref[found] = place
            kept = (place >= 0) & (place < store_blocks) & (i * SCAN + u < listed)
            found = found + kept.astype(jnp.int32)
        return found

    found = lax.fori_loop(0, lax.div(listed + (SCAN - 1), SCAN), scan_entries, jnp.int32(0))
    home = owner == me
    if not done:

        @pl.when(jnp.logical_and(found == 0, jnp.logical_not(home)))
        def _():
            o_ref[here] = jnp.zeros(o_ref.shape[1:], o_ref.dtype)
            lse_ref[here] = jnp.full(lse_ref.shape[1:], NEG, lse_ref.dtype)

    @pl.when(found > done if done else jnp.logical_or(found > 0, home))
    def _():
        if done:
            for g in range(kv_here):
                max_ref[g : g + 1] = jnp.concatenate(
                    [lse_ref[here, g, r : r + 1] for r in range(per_group)], axis=1
                )
                sum_ref[g : g + 1] = jnp.ones((1, rows), jnp.float32)
                acc_ref[g] = o_ref[here, g].astype(jnp.float32)
        else:

            @pl.when(home)
            def _():
                start = pl.multiple_of(inner * BLK, BLK)
                for g in range(kv_here):
                    cols = slice(g * DH, (g + 1) * DH)
                    asked = asked_rows(q_ref, first_row, g, per_group)
                    s = jnp.where(causal_mask(rows), scores_of(sk_ref[pl.ds(start, BLK), cols], asked), NEG)
                    m = jnp.max(s, axis=0, keepdims=True)
                    p = jnp.exp2(s - m)
                    max_ref[g : g + 1] = m
                    sum_ref[g : g + 1] = jnp.sum(p, axis=0, keepdims=True)
                    acc_ref[g] = weighed(sv_ref[pl.ds(start, BLK), cols], p)

            @pl.when(jnp.logical_not(home))
            def _():
                max_ref[...] = jnp.full_like(max_ref, NEG)
                sum_ref[...] = jnp.zeros_like(sum_ref)
                acc_ref[...] = jnp.zeros_like(acc_ref)

        def take(*places):
            starts = [pl.multiple_of(place * BLK, BLK) for place in places]

            def rows_of(ref, cols):
                return jnp.concatenate([ref[pl.ds(start, BLK), cols] for start in starts], axis=0)

            for g in range(kv_here):
                cols = slice(g * DH, (g + 1) * DH)
                s = scores_of(rows_of(k_ref, cols), asked_rows(q_ref, first_row, g, per_group))
                old = max_ref[g : g + 1]
                new = jnp.maximum(old, jnp.max(s, axis=0, keepdims=True))
                p = jnp.exp2(s - new)
                shrink = jnp.exp2(old - new)
                max_ref[g : g + 1] = new
                sum_ref[g : g + 1] = sum_ref[g : g + 1] * shrink + jnp.sum(p, axis=0, keepdims=True)
                acc_ref[g] = acc_ref[g] * shrink + weighed(rows_of(v_ref, cols), p)

        left = found - done

        @pl.loop(0, lax.div(left, 2))
        def _(i):
            take(list_ref[done + 2 * i], list_ref[done + 2 * i + 1])

        @pl.when(lax.rem(left, 2) == 1)
        def _():
            take(list_ref[found - 1])

        for g in range(kv_here):
            total = sum_ref[g : g + 1]
            write_part(o_ref, lse_ref, here, g, acc_ref[g], total, max_ref[g : g + 1] + jnp.log2(total))


def part_kernel(local_blocks, store_blocks, *refs):
    block = pl.program_id(0)
    part_row(block, 0, 0, 0, local_blocks, store_blocks, *refs)


def rest_kernel(local_blocks, store_blocks, *refs):
    def row(block, carry):
        first_row = pl.multiple_of(block * BLK, BLK)
        part_row(block, block, first_row, 1, local_blocks, store_blocks, *refs[:8], *refs[10:])
        return carry

    lax.fori_loop(0, refs[10].shape[0], row, 0)


def grant(*arrays):
    size = 0
    for shape, dtype in arrays:
        cells = 1
        for d in shape:
            cells = cells * d
        size += cells * jnp.dtype(dtype).itemsize
    return min(size + (4 << 20), 60 << 20)


def long_cost():
    return pl.CostEstimate(flops=200_000_000_000, bytes_accessed=1 << 20, transcendentals=0)


def ring_place(index, n):
    odd = lax.rem(index, 2)
    half = index // 2
    return (1 - odd) * half + odd * (n - 1 - half)


def ring_index(place, n):
    place = lax.rem(place + 2 * n, n)
    far = place // (n // 2)
    return (1 - far) * (2 * place) + far * (2 * (n - 1 - place) + 1)


def gather_kernel(n, pieces, early, *refs):
    refs = list(refs)

    def some(count):
        return [refs.pop(0) for _ in range(count)]

    x_ref, near_ref, count_ref = some(3)
    if early:
        slot_hbm, *store_hbm = some(5)
    out_ref, nears_ref, counts_ref = some(3)
    if early:
        o_ref, lse_ref, slot_ref, near_smem, count_smem, sk_ref, sv_ref, k_ref, v_ref, load_sem = some(10)
    own_sem, send_sem, recv_sem, tsend_sem, trecv_sem = refs
    me = lax.axis_index("seq")
    place = ring_place(me, n)
    rows = x_ref.shape[0]
    sub = rows // pieces
    half = n // 2
    ways = (1, -1)
    beside = [ring_index(place + way, n) for way in ways]
    own = [
        pltpu.make_async_copy(source, target, own_sem.at[i])
        for i, (source, target) in enumerate(
            (
                (x_ref, out_ref.at[pl.ds(pl.multiple_of(me * rows, rows), rows)]),
                (near_ref, nears_ref.at[me]),
                (count_ref, counts_ref.at[me]),
            )
        )
    ]
    for one in own:
        one.start()
    loads = []
    if early:
        sources = [slot_hbm] + store_hbm
        for i, (source, target) in enumerate(zip(sources, (slot_ref, sk_ref, sv_ref, k_ref, v_ref))):
            loads.append(pltpu.make_async_copy(source, target, load_sem.at[i]))
    for one in loads:
        one.start()
    barrier = pltpu.get_barrier_semaphore()
    for k in range(1, n):
        pl.semaphore_signal(barrier, inc=1, device_id={"seq": lax.rem(me + k, n)}, device_id_type=MESH)
    for one in own:
        one.wait()
    pl.semaphore_wait(barrier, n - 1)

    def copy(way, step, piece):
        owner = ring_index(place - ways[way] * step, n)
        there = pl.ds(pl.multiple_of(owner * rows + piece * sub, sub), sub)
        return pltpu.make_async_remote_copy(
            src_ref=out_ref.at[there],
            dst_ref=out_ref.at[there],
            send_sem=send_sem.at[way, step, piece],
            recv_sem=recv_sem.at[way, step, piece],
            device_id={"seq": beside[way]},
            device_id_type=MESH,
        )

    def piece_of(way, spot):
        return spot if way == 0 else pieces - 1 - spot

    table_copies = []
    for t, target in enumerate((nears_ref, counts_ref)):
        for k in range(1, n):
            table_copies.append(
                pltpu.make_async_remote_copy(
                    src_ref=target.at[me],
                    dst_ref=target.at[me],
                    send_sem=tsend_sem.at[t, k],
                    recv_sem=trecv_sem.at[t, k],
                    device_id={"seq": lax.rem(me + k, n)},
                    device_id_type=MESH,
                )
            )
    for one in table_copies:
        one.start()
    started = []
    for spot in range(pieces):
        for way in range(2):
            one = copy(way, 0, piece_of(way, spot))
            one.start()
            started.append(one)

    def first_listed(owner, inner):
        degree = near_ref.shape[1]
        store_blocks = k_ref.shape[0]
        listed = count_smem[owner, 0, inner]

        def look(i, best):
            e = degree - SCAN * (i + 1)
            for u in range(SCAN - 1, -1, -1):
                spot = slot_ref[near_smem[owner, inner, e + u]] - me * store_blocks
                kept = ((spot >= 0) & (spot < store_blocks) & (e + u < listed)).astype(jnp.int32)
                best = best + kept * (spot - best)
            return best

        return lax.fori_loop(0, degree // SCAN, look, jnp.int32(-1))

    def row_work(owner, inner, spot, mine):
        per_group = H // KVH
        taken = jnp.maximum(spot, 0)
        missing = jnp.minimum(spot, 0).astype(jnp.float32) * -NEG
        first_row = pl.multiple_of(owner * rows + inner * BLK, BLK)
        for g in range(k_ref.shape[2] // DH):
            cols = slice(g * DH, (g + 1) * DH)
            asked = asked_rows(out_ref, first_row, g, per_group)
            keys, values = k_ref[taken, :, cols], v_ref[taken, :, cols]
            if mine:
                near = pl.ds(pl.multiple_of(inner * BLK, BLK), BLK)
                keys = jnp.concatenate([sk_ref[near, cols], keys], axis=0)
                values = jnp.concatenate([sv_ref[near, cols], values], axis=0)
            s = scores_of(keys, asked)
            if mine:
                inside = jnp.where(causal_mask(s.shape[1]), s[:BLK], NEG)
                s = jnp.concatenate([inside, s[BLK:] + missing], axis=0)
            m = jnp.max(s, axis=0, keepdims=True)
            p = jnp.exp2(s - m)
            total = jnp.sum(p, axis=0, keepdims=True)
            lse = m + jnp.log2(total)
            if not mine:
                lse = lse + missing
            write_part(o_ref, lse_ref, owner * pieces + inner, g, weighed(values, p), total, lse)

    def row_at(way, step, spot):
        return ring_index(place - ways[way] * step, n), piece_of(way, spot)

    def scanned(step, spot):
        return [first_listed(*row_at(way, step, spot)) for way in range(2)] if early else None

    def arrived(step, spot, found):
        if early:
            for way in range(2):
                row_work(*row_at(way, step, spot), found[way], False)

    def own_rows():
        for one in table_copies:
            one.wait_recv()
        tables = [
            pltpu.make_async_copy(source, target, load_sem.at[5 + i])
            for i, (source, target) in enumerate(((nears_ref, near_smem), (counts_ref, count_smem)))
        ]
        for one in tables:
            one.start()
        for one in loads + tables:
            one.wait()
        for inner in range(pieces):
            row_work(me, inner, first_listed(me, inner), True)

    for step in range(1, half):
        for spot in range(pieces):
            first = step == 1 and spot == 0
            found = None if first else scanned(step, spot)
            for way in range(2):
                copy(way, step - 1, piece_of(way, spot)).wait_recv()
                if step < half - 1 or spot < pieces // 2:
                    one = copy(way, step, piece_of(way, spot))
                    one.start()
                    started.append(one)
            if early and first:
                own_rows()
                found = scanned(step, spot)
            arrived(step, spot, found)
    for spot in range(pieces // 2):
        found = scanned(half, spot)
        for way in range(2):
            copy(way, half - 1, piece_of(way, spot)).wait_recv()
        arrived(half, spot, found)
    for one in started:
        one.wait_send()
    for one in table_copies:
        if early:
            one.wait_send()
        else:
            one.wait()


def gathered(x, near, count, n, early):
    rows, width = x.shape
    pieces = rows // BLK
    vmem = pl.BlockSpec(memory_space=pltpu.VMEM)
    dma = pltpu.SemaphoreType.DMA
    kind = pltpu.VMEM if early else jax.ShapeDtypeStruct
    inputs = [x, near, count] + list(early)
    out_shape = [
        kind((n * rows, width), x.dtype),
        jax.ShapeDtypeStruct((n,) + near.shape, near.dtype),
        jax.ShapeDtypeStruct((n,) + count.shape, count.dtype),
    ]
    scratch = []
    held = [((n + 1, rows, width), x.dtype)]
    if early:
        slot, *stores = early
        kv_here = stores[2].shape[2] // DH
        part_shape = (n * pieces, kv_here, BLK, (H // KVH) * DH)
        out_shape += [kind(part_shape, x.dtype), kind((n * pieces, kv_here, STAT, BLK), jnp.float32)]
        scratch += [pltpu.SMEM(slot.shape, slot.dtype)]
        scratch += [pltpu.SMEM(out_shape[1].shape, near.dtype), pltpu.SMEM(out_shape[2].shape, count.dtype)]
        scratch += [pltpu.VMEM(a.shape, a.dtype) for a in stores]
        scratch += [dma((7,))]
        held += [(part_shape, x.dtype)] + [(a.shape, a.dtype) for a in stores]
    scratch += [
        dma((3,)),
        dma((2, n // 2, pieces)),
        dma((2, n // 2, pieces)),
        dma((2, n)),
        dma((2, n)),
    ]
    return pl.pallas_call(
        functools.partial(gather_kernel, n, pieces, bool(early)),
        in_specs=[pl.BlockSpec(memory_space=pltpu.HBM)] * len(inputs),
        out_specs=[vmem] * len(out_shape),
        out_shape=out_shape,
        scratch_shapes=scratch,
        compiler_params=pltpu.CompilerParams(
            collective_id=0,
            has_side_effects=True,
            vmem_limit_bytes=grant(*held),
        ),
        cost_estimate=long_cost(),
    )(*(pltpu.with_memory_space_constraint(a, pltpu.HBM) for a in inputs))


def merge(lse_a, lse_b):
    top = jnp.maximum(lse_a, lse_b)
    a = jnp.exp2(lse_a - top)
    b = jnp.exp2(lse_b - top)
    total = a + b
    return a / total, b / total, top + jnp.log2(total)


def reduce_kernel(
    n,
    small,
    o_ref,
    lse_ref,
    out_ref,
    got,
    got_lse,
    own,
    own_sem,
    send_sem,
    recv_sem,
    lsend_sem,
    lrecv_sem,
    ready=None,
):
    me = lax.axis_index("seq")
    place = ring_place(me, n)
    groups, width = got.shape[2], got.shape[4]
    wide = width // CUTS
    ways = (1, -1)
    beside = [ring_index(place + way, n) for way in ways]
    if ready is None:
        barrier = pltpu.get_barrier_semaphore()
        for other in beside:
            pl.semaphore_signal(barrier, inc=1, device_id={"seq": other}, device_id_type=MESH)

    def home(way, step):
        return ring_index(place - ways[way] * (1 + step), n)

    def fetch(way, step):
        return pltpu.make_async_copy(
            o_ref.at[home(way, step) * 2 + way], own.at[way, lax.rem(step, 2)], own_sem.at[way, lax.rem(step, 2)]
        )

    def lse_copy(way, step, g, before):
        return pltpu.make_async_remote_copy(
            src_ref=lse_ref.at[home(way, step) * 2 + way, g] if before is None else got_lse.at[way, before, g],
            dst_ref=got_lse.at[way, step, g],
            send_sem=lsend_sem.at[way, step, g],
            recv_sem=lrecv_sem.at[way, step, g],
            device_id={"seq": beside[way]},
            device_id_type=MESH,
        )

    def copy(way, step, g, cut, before):
        part = (g, slice(None), pl.ds(cut * wide, wide))
        return pltpu.make_async_remote_copy(
            src_ref=o_ref.at[(home(way, step) * 2 + way,) + part]
            if before is None
            else got.at[(way, before) + part],
            dst_ref=got.at[(way, step) + part],
            send_sem=send_sem.at[way, step, g * CUTS + cut],
            recv_sem=recv_sem.at[way, step, g * CUTS + cut],
            device_id={"seq": beside[way]},
            device_id_type=MESH,
        )

    def shares_of(way, step, g):
        lse_copy(way, step - 1, g, step - 1).wait_recv()
        if g == 0 and not small:
            fetch(way, step).wait()
        return merge(got_lse[way, step - 1, g], lse_ref[home(way, step) * 2 + way, g])

    def merged(way, step, g, cut, theirs, ours):
        copy(way, step - 1, g, cut, step - 1).wait_recv()
        at = home(way, step) * 2 + way
        columns = []
        for r in range(cut * wide // DH, (cut + 1) * wide // DH):
            cols = slice(r * DH, (r + 1) * DH)
            mine = o_ref[at, g, :, cols] if small else own[way, lax.rem(step, 2), g, :, cols]
            value = (
                got[way, step - 1, g, :, cols].astype(jnp.float32) * theirs[r : r + 1]
                + mine.astype(jnp.float32) * ours[r : r + 1]
            )
            columns.append((r, value))
        return columns

    if not small:
        for way in range(2):
            fetch(way, 1).start()
    if ready is None:
        pl.semaphore_wait(barrier, 2)
    for g in range(groups):
        for way in range(2):
            lse_copy(way, 0, g, None).start()
        for cut in range(CUTS):
            for way in range(2):
                copy(way, 0, g, cut, None).start()

    def one_step(step, carry):
        if not small:
            for way in range(2):
                fetch(way, step + 1).start()
        for g in range(groups):
            shares = []
            for way in range(2):
                theirs, ours, lse = shares_of(way, step, g)
                got_lse[way, step - 1, g] = lse
                lse_copy(way, step, g, step - 1).start()
                shares.append((theirs, ours))
            for cut in range(CUTS):
                for way in range(2):
                    for r, value in merged(way, step, g, cut, *shares[way]):
                        got[way, step - 1, g, :, r * DH : (r + 1) * DH] = value.astype(jnp.bfloat16)
                    copy(way, step, g, cut, step - 1).start()
        return carry

    lax.fori_loop(1, n - 1, one_step, 0)
    for way in range(2):
        for g in range(groups):
            theirs, ours, _ = shares_of(way, n - 1, g)
            for cut in range(CUTS):
                for r, value in merged(way, n - 1, g, cut, theirs, ours):
                    at = g * width + r * DH
                    out_ref[way * BLK : (way + 1) * BLK, at : at + DH] = jnp.transpose(value).astype(jnp.bfloat16)
        if ready is not None:
            ready(way)

    def drain_all():
        def drain(step, before):
            for g in range(groups):
                for way in range(2):
                    lse_copy(way, step, g, before).wait_send()
                    for cut in range(CUTS):
                        copy(way, step, g, cut, before).wait_send()

        drain(0, None)
        lax.fori_loop(1, n - 1, lambda step, carry: (drain(step, step - 1), carry)[1], 0)

    if ready is None:
        drain_all()
    return drain_all


def project_stages(
    n,
    heads,
    x_ref,
    w_hbm,
    out_ref,
    w_ref,
    blocks,
    split,
    got,
    summed,
    landed,
    w_sem,
    wsend,
    wrecv,
    send_sem,
    recv_sem,
    hsend,
    hrecv,
    fsend,
    frecv,
):
    me = lax.axis_index("seq")
    mine = lax.axis_index("head")
    line = n // 2
    at, side = me // 2, lax.rem(me, 2)
    share = x_ref.shape[0] // heads
    columns = w_ref.shape[2]
    ways = (1, -1)
    early = min(2, line - 1)
    weights = pltpu.make_async_copy(w_hbm, w_ref.at[0], w_sem.at[0])
    weights.start()
    barrier = pltpu.get_barrier_semaphore()
    place = ring_place(me, n)
    for way in ways:
        other = ring_index(place + way, n)
        pl.semaphore_signal(barrier, inc=1, device_id={"seq": other}, device_id_type=MESH)
    for k in range(1, heads):
        pl.semaphore_signal(barrier, inc=1, device_id={"head": lax.rem(mine + k, heads)}, device_id_type=MESH)
    for k in range(1, line):
        other = lax.rem(at + k, line) * 2 + side
        pl.semaphore_signal(barrier, inc=1, device_id={"seq": other}, device_id_type=MESH)
    partner = at * 2 + 1 - side
    pl.semaphore_signal(barrier, inc=1, device_id={"seq": partner}, device_id_type=MESH)
    pl.semaphore_wait(barrier, heads + line + 1)

    def inside(spot):
        return jnp.logical_and(spot >= 0, spot < line)

    def copy(way, step, piece, first):
        there = (at - ways[way] * step, pl.ds(pl.multiple_of(piece * share, share), share))
        return pltpu.make_async_remote_copy(
            src_ref=x_ref.at[there[1]] if first else blocks.at[there],
            dst_ref=blocks.at[there],
            send_sem=send_sem.at[way, step, piece],
            recv_sem=recv_sem.at[way, step, piece],
            device_id={"seq": (at + ways[way]) * 2 + side},
            device_id_type=MESH,
        )

    def leaves(way, step):
        return jnp.logical_and(inside(at - ways[way] * step), inside(at + ways[way]))

    def to_head(i, j, source, to):
        return pltpu.make_async_remote_copy(
            src_ref=split.at[i, j, to],
            dst_ref=got.at[i, j, source],
            send_sem=hsend.at[i, j, to],
            recv_sem=hrecv.at[i, j, source],
            device_id={"head": to},
            device_id_type=MESH,
        )

    def to_row(i, j, source):
        owner = source * 2 + (side if j == 0 else 1 - side)
        return pltpu.make_async_remote_copy(
            src_ref=summed.at[i, j],
            dst_ref=landed.at[owner],
            send_sem=fsend.at[i, j],
            recv_sem=frecv.at[source, j],
            device_id={"seq": i * 2 + side},
            device_id_type=MESH,
        )

    def unit(i, c, js, own):
        rows = pl.ds(pl.multiple_of(c * share, share), share)
        value = x_ref[rows] if own else blocks[i, rows]
        for j in js:
            split[i, j, c] = jnp.dot(value, w_ref[j], preferred_element_type=jnp.float32).astype(jnp.bfloat16)

            @pl.when(mine != c)
            def _():
                to_head(i, j, mine, c).start()

    def visit(step, c, js, arriving):
        for way in range(2):
            i = at - ways[way] * step

            @pl.when(inside(i))
            def _():
                if arriving:
                    copy(way, step - 1, c, False).wait_recv()

                    @pl.when(inside(at + ways[way]))
                    def _():
                        copy(way, step, c, False).start()

                unit(i, c, js, False)

    def total_of(i, j):
        total = split[i, j, mine].astype(jnp.float32)
        for k in range(1, heads):
            source = lax.rem(mine + k, heads)
            to_head(i, j, source, mine).wait_recv()
            total = total + got[i, j, source].astype(jnp.float32)
        return total.astype(jnp.bfloat16)

    def settle_own(j):
        landed[at * 2 + (side if j == 0 else 1 - side)] = total_of(at, j)

    def settle(step, js):
        for way in range(2):
            i = at - ways[way] * step

            @pl.when(inside(i))
            def _():
                for j in js:
                    summed[i, j] = total_of(i, j)
                    to_row(i, j, at).start()

    def each(function):
        lax.fori_loop(0, heads, lambda c, carry: (function(c), carry)[1], 0)

    def start_own(c):
        for way in range(2):

            @pl.when(inside(at + ways[way]))
            def _():
                copy(way, 0, c, True).start()

    def run():
        weights.wait()
        exchange = pltpu.make_async_remote_copy(
            src_ref=w_ref.at[0],
            dst_ref=w_ref.at[1],
            send_sem=wsend.at[0],
            recv_sem=wrecv.at[0],
            device_id={"seq": partner},
            device_id_type=MESH,
        )
        exchange.start()
        each(lambda c: unit(at, c, (0,), True))

        def first_steps(step, carry):
            each(lambda c: visit(step, c, (0,), True))

            @pl.when(step == 1)
            def _():
                settle_own(0)

            @pl.when(step > 1)
            def _():
                settle(step - 1, (0,))

            return carry

        lax.fori_loop(1, early + 1, first_steps, 0)
        exchange.wait()
        each(lambda c: unit(at, c, (1,), True))
        lax.fori_loop(1, early + 1, lambda t, carry: (each(lambda c: visit(t, c, (1,), False)), carry)[1], 0)
        settle(early, (0,))

        def late_step(step, carry):
            each(lambda c: visit(step, c, (0, 1), True))

            @pl.when(step == early + 1)
            def _():
                settle_own(1)
                lax.fori_loop(1, early + 1, lambda t, inner: (settle(t, (1,)), inner)[1], 0)

            @pl.when(step > early + 1)
            def _():
                settle(step - 1, (0, 1))

            return carry

        if line - 1 > early:
            lax.fori_loop(early + 1, line, late_step, 0)
            settle(line - 1, (0, 1))
        else:
            settle_own(1)
            lax.fori_loop(1, early + 1, lambda t, inner: (settle(t, (1,)), inner)[1], 0)

        for way in range(2):
            for step in range(2):

                def finish(c):
                    @pl.when(leaves(way, step))
                    def _():
                        copy(way, step, c, step == 0).wait_send()

                if step == 0:
                    each(finish)
                else:

                    def finish_rest(t, carry):
                        def one(c):
                            @pl.when(leaves(way, t))
                            def _():
                                copy(way, t, c, False).wait_send()

                        each(one)
                        return carry

                    lax.fori_loop(1, line, finish_rest, 0)

        def drain(i, carry):
            for j in range(2):
                for k in range(1, heads):
                    to_head(i, j, mine, lax.rem(mine + k, heads)).wait_send()

                @pl.when(i != at)
                def _():
                    to_row(i, j, at).wait_send()
                    to_row(at, j, i).wait_recv()

            return carry

        lax.fori_loop(0, line, drain, 0)
        for i in range(n):
            out_ref[:, i * columns : (i + 1) * columns] = landed[i]

    return start_own, each, run


def project_kernel(n, heads, *refs):
    start_own, each, run = project_stages(n, heads, *refs)
    each(start_own)
    run()


def join_kernel(n, heads, o_ref, lse_ref, w_hbm, out_ref, x_ref, *refs):
    start_own, _, run = project_stages(n, heads, x_ref, w_hbm, out_ref, *refs[8:])
    per_way = BLK * heads // x_ref.shape[0]

    def ready(way):
        for c in range(per_way):
            start_own(way * per_way + c)

    drain = reduce_kernel(n, True, o_ref, lse_ref, x_ref, *refs[:8], ready=ready)
    run()
    drain()


def project_plan(n, heads, rows, width, columns, dtype):
    share = rows // heads
    line = n // 2
    dma = pltpu.SemaphoreType.DMA
    scratch = [
        pltpu.VMEM((2, width, columns), dtype),
        pltpu.VMEM((line, rows, width), dtype),
        pltpu.VMEM((line, 2, heads, share, columns), dtype),
        pltpu.VMEM((line, 2, heads, share, columns), dtype),
        pltpu.VMEM((line, 2, share, columns), dtype),
        pltpu.VMEM((n, share, columns), dtype),
        dma((1,)),
        dma((1,)),
        dma((1,)),
        dma((2, line, heads)),
        dma((2, line, heads)),
        dma((line, 2, heads)),
        dma((line, 2, heads)),
        dma((line, 2)),
        dma((line, 2)),
    ]
    padded = max(columns, BLK)
    held = [
        ((2, width, padded), dtype),
        ((line + 2, rows, width), dtype),
        ((2, n, heads, share, padded), dtype),
        ((3, n, share, padded), dtype),
    ]
    return scratch, held


def reduce_plan(n, small, kv_here, group_width):
    dma = pltpu.SemaphoreType.DMA((2, n - 1, kv_here))
    dma_cuts = pltpu.SemaphoreType.DMA((2, n - 1, kv_here * CUTS))
    scratch = [
        pltpu.VMEM((2, n - 1, kv_here, BLK, group_width), jnp.bfloat16),
        pltpu.VMEM((2, n - 1, kv_here, STAT, BLK), jnp.float32),
        pltpu.VMEM((2, 2, 1 if small else kv_here, BLK, group_width), jnp.bfloat16),
        pltpu.SemaphoreType.DMA((2, 2)),
        dma_cuts,
        dma_cuts,
        dma,
        dma,
    ]
    held = [
        ((2, n + 1, kv_here, BLK, group_width), jnp.bfloat16),
        ((2, 2 * n - 1, kv_here, STAT, BLK), jnp.float32),
    ]
    return scratch, held


def mixed_from(parts, lse, weight, n, heads, rows, width, small):
    _, kv_here, _, group_width = parts.shape
    columns = weight.shape[1]
    vmem = pl.BlockSpec(memory_space=pltpu.VMEM)
    anywhere = pl.BlockSpec(memory_space=pl.ANY)
    reduce_scratch, reduce_held = reduce_plan(n, small, kv_here, group_width)
    project_scratch, project_held = project_plan(n, heads, rows, width, columns, parts.dtype)
    attended = jax.ShapeDtypeStruct((rows, width), parts.dtype)
    out = jax.ShapeDtypeStruct((rows // heads, n * columns), parts.dtype)

    def call(kernel, number, in_specs, out_shape, scratch, held):
        return pl.pallas_call(
            kernel,
            in_specs=in_specs,
            out_specs=vmem,
            out_shape=out_shape,
            scratch_shapes=scratch,
            compiler_params=pltpu.CompilerParams(
                collective_id=number, has_side_effects=True, vmem_limit_bytes=grant(*held)
            ),
            cost_estimate=long_cost(),
        )

    if small:
        scratch = [pltpu.VMEM((rows, width), parts.dtype)] + reduce_scratch + project_scratch
        held = reduce_held + project_held + [(parts.shape, parts.dtype)]
        kernel = functools.partial(join_kernel, n, heads)
        return call(kernel, 1, [vmem, vmem, anywhere], out, scratch, held)(parts, lse, weight)

    def kernel(*refs):
        reduce_kernel(n, small, *refs)

    x = call(kernel, 1, [anywhere, vmem], attended, reduce_scratch, reduce_held)(parts, lse)
    kernel = functools.partial(project_kernel, n, heads)
    return call(kernel, 2, [vmem, anywhere], out, project_scratch, project_held)(x, weight)


def body(
    queries,
    self_keys,
    self_values,
    store_keys,
    store_values,
    kv_slot,
    neighbours,
    counts,
    out_weight,
):
    n = lax.axis_size("seq")
    head_count = lax.axis_size("head")
    local_blocks, degree = neighbours.shape
    local_rows, width = queries.shape
    store_blocks = store_keys.shape[0] // BLK
    all_blocks = local_blocks * n
    kv_here = store_keys.shape[1] // DH
    group_width = (H // KVH) * DH
    rows = (H // KVH) * BLK
    small = queries.size * n * queries.dtype.itemsize <= 8 << 20
    count_row = counts.reshape(1, local_blocks)
    stores = (self_keys, self_values, store_keys, store_values)
    cut = tuple(a.reshape(store_blocks, BLK, -1) for a in stores[2:])
    smem = pl.BlockSpec(memory_space=pltpu.SMEM)
    vmem = pl.BlockSpec(memory_space=pltpu.VMEM)
    params = pltpu.CompilerParams(vmem_limit_bytes=28 << 20)
    cost = pl.CostEstimate(flops=2_000_000_000, bytes_accessed=12 << 20, transcendentals=4_000_000)
    scratch = [
        pltpu.SMEM((degree + 1,), jnp.int32),
        pltpu.VMEM((kv_here, DH, rows), jnp.float32),
        pltpu.VMEM((kv_here, rows), jnp.float32),
        pltpu.VMEM((kv_here, rows), jnp.float32),
    ]
    part_shape = (all_blocks, kv_here, BLK, group_width)
    lse_shape = (all_blocks, kv_here, STAT, BLK)
    if small:
        all_queries, near, count, parts, lse = gathered(queries, neighbours, count_row, n, (kv_slot,) + stores[:2] + cut)
        parts, lse = pl.pallas_call(
            functools.partial(rest_kernel, local_blocks, store_blocks),
            in_specs=[smem] * 3 + [vmem] * 7,
            out_specs=[vmem, vmem],
            out_shape=[pltpu.VMEM(part_shape, jnp.bfloat16), pltpu.VMEM(lse_shape, jnp.float32)],
            scratch_shapes=scratch,
            input_output_aliases={8: 0, 9: 1},
            compiler_params=params,
            cost_estimate=cost,
        )(kv_slot, near, count, all_queries, *stores, parts, lse)
    else:
        all_queries, near, count = gathered(queries, neighbours, count_row, n, ())
        parts, lse = pl.pallas_call(
            functools.partial(part_kernel, local_blocks, store_blocks),
            grid=(all_blocks,),
            in_specs=[smem] * 3 + [pl.BlockSpec((BLK, width), lambda i: (i, 0))] + [vmem] * 4,
            out_specs=[
                pl.BlockSpec((1, kv_here, BLK, group_width), lambda i: (i, 0, 0, 0)),
                pl.BlockSpec((1, kv_here, STAT, BLK), lambda i: (i, 0, 0, 0)),
            ],
            out_shape=[
                jax.ShapeDtypeStruct(part_shape, jnp.bfloat16),
                jax.ShapeDtypeStruct(lse_shape, jnp.float32),
            ],
            scratch_shapes=scratch,
            compiler_params=params,
            cost_estimate=cost,
        )(kv_slot, near, count, all_queries, *stores)
    return mixed_from(parts, lse, out_weight, n, head_count, local_rows, width, small)


def solution(mesh):
    placed = (
        P("seq", "head"),
        P("seq", "head"),
        P("seq", "head"),
        P("seq", "head"),
        P("seq", "head"),
        P(),
        P("seq", None),
        P("seq"),
        P("head", "seq"),
    )
    return jax.shard_map(
        body, mesh=mesh, in_specs=placed, out_specs=P(("seq", "head"), None), check_vma=False
    )
```

```python
import functools

import jax
import jax.numpy as jnp
from jax import lax
from jax.experimental import pallas as pl
from jax.experimental.pallas import tpu as pltpu
from jax.sharding import PartitionSpec as P

H = 32
KVH = 8
DH = 128
BLK = 128
NEG = -1e30
STAT = 8
SCAN = 4
CUTS = 2
LOG2E = 1.4426950408889634
MESH = pl.DeviceIdType.MESH


def asked_rows(q_ref, first_row, g, per_group):
    return jnp.concatenate(
        [
            q_ref[pl.ds(first_row, BLK), (g * per_group + r) * DH : (g * per_group + r + 1) * DH]
            for r in range(per_group)
        ],
        axis=0,
    )


def scores_of(keys, asked):
    scaling = DH ** (-0.5) * LOG2E
    return lax.dot_general(keys, asked, (((1,), (1,)), ((), ())), preferred_element_type=jnp.float32) * scaling


def weighed(values, p):
    return lax.dot_general(
        values, p.astype(jnp.bfloat16), (((0,), (0,)), ((), ())), preferred_element_type=jnp.float32
    )


def causal_mask(rows):
    position = lax.rem(lax.broadcasted_iota(jnp.int32, (BLK, rows), 1), BLK)
    return position >= lax.broadcasted_iota(jnp.int32, (BLK, rows), 0)


def write_part(o_ref, lse_ref, here, g, acc, total, lse):
    per_group = lse.shape[1] // BLK
    o_ref[here, g] = (acc * (1.0 / total)).astype(jnp.bfloat16)
    for r in range(STAT):
        at = (r % per_group) * BLK
        lse_ref[here, g, r : r + 1] = lse[:, at : at + BLK]


def part_row(
    block,
    here,
    first_row,
    done,
    local_blocks,
    store_blocks,
    slot_ref,
    near_ref,
    count_ref,
    q_ref,
    sk_ref,
    sv_ref,
    k_ref,
    v_ref,
    o_ref,
    lse_ref,
    list_ref,
    acc_ref,
    max_ref,
    sum_ref,
):
    owner, inner = lax.div(block, local_blocks), lax.rem(block, local_blocks)
    me = lax.axis_index("seq")
    per_group = H // KVH
    kv_here = k_ref.shape[1] // DH
    rows = per_group * BLK
    listed = count_ref[owner, 0, inner]
    first_slot = me * store_blocks

    def scan_entries(i, found):
        places = [slot_ref[near_ref[owner, inner, i * SCAN + u]] - first_slot for u in range(SCAN)]
        for u, place in enumerate(places):
            list_ref[found] = place
            kept = (place >= 0) & (place < store_blocks) & (i * SCAN + u < listed)
            found = found + kept.astype(jnp.int32)
        return found

    found = lax.fori_loop(0, lax.div(listed + (SCAN - 1), SCAN), scan_entries, jnp.int32(0))
    home = owner == me
    if not done:

        @pl.when(jnp.logical_and(found == 0, jnp.logical_not(home)))
        def _():
            o_ref[here] = jnp.zeros(o_ref.shape[1:], o_ref.dtype)
            lse_ref[here] = jnp.full(lse_ref.shape[1:], NEG, lse_ref.dtype)

    @pl.when(found > done if done else jnp.logical_or(found > 0, home))
    def _():
        if done:
            for g in range(kv_here):
                max_ref[g : g + 1] = jnp.concatenate(
                    [lse_ref[here, g, r : r + 1] for r in range(per_group)], axis=1
                )
                sum_ref[g : g + 1] = jnp.ones((1, rows), jnp.float32)
                acc_ref[g] = o_ref[here, g].astype(jnp.float32)
        else:

            @pl.when(home)
            def _():
                start = pl.multiple_of(inner * BLK, BLK)
                for g in range(kv_here):
                    cols = slice(g * DH, (g + 1) * DH)
                    asked = asked_rows(q_ref, first_row, g, per_group)
                    s = jnp.where(causal_mask(rows), scores_of(sk_ref[pl.ds(start, BLK), cols], asked), NEG)
                    m = jnp.max(s, axis=0, keepdims=True)
                    p = jnp.exp2(s - m)
                    max_ref[g : g + 1] = m
                    sum_ref[g : g + 1] = jnp.sum(p, axis=0, keepdims=True)
                    acc_ref[g] = weighed(sv_ref[pl.ds(start, BLK), cols], p)

            @pl.when(jnp.logical_not(home))
            def _():
                max_ref[...] = jnp.full_like(max_ref, NEG)
                sum_ref[...] = jnp.zeros_like(sum_ref)
                acc_ref[...] = jnp.zeros_like(acc_ref)

        def take(*places):
            starts = [pl.multiple_of(place * BLK, BLK) for place in places]

            def rows_of(ref, cols):
                return jnp.concatenate([ref[pl.ds(start, BLK), cols] for start in starts], axis=0)

            for g in range(kv_here):
                cols = slice(g * DH, (g + 1) * DH)
                s = scores_of(rows_of(k_ref, cols), asked_rows(q_ref, first_row, g, per_group))
                old = max_ref[g : g + 1]
                new = jnp.maximum(old, jnp.max(s, axis=0, keepdims=True))
                p = jnp.exp2(s - new)
                shrink = jnp.exp2(old - new)
                max_ref[g : g + 1] = new
                sum_ref[g : g + 1] = sum_ref[g : g + 1] * shrink + jnp.sum(p, axis=0, keepdims=True)
                acc_ref[g] = acc_ref[g] * shrink + weighed(rows_of(v_ref, cols), p)

        left = found - done

        @pl.loop(0, lax.div(left, 2))
        def _(i):
            take(list_ref[done + 2 * i], list_ref[done + 2 * i + 1])

        @pl.when(lax.rem(left, 2) == 1)
        def _():
            take(list_ref[found - 1])

        for g in range(kv_here):
            total = sum_ref[g : g + 1]
            write_part(o_ref, lse_ref, here, g, acc_ref[g], total, max_ref[g : g + 1] + jnp.log2(total))


def part_kernel(local_blocks, store_blocks, *refs):
    block = pl.program_id(0)
    part_row(block, 0, 0, 0, local_blocks, store_blocks, *refs)


def rest_kernel(local_blocks, store_blocks, *refs):
    def row(block, carry):
        first_row = pl.multiple_of(block * BLK, BLK)
        part_row(block, block, first_row, 1, local_blocks, store_blocks, *refs[:8], *refs[10:])
        return carry

    lax.fori_loop(0, refs[10].shape[0], row, 0)


def grant(*arrays):
    size = 0
    for shape, dtype in arrays:
        cells = 1
        for d in shape:
            cells = cells * d
        size += cells * jnp.dtype(dtype).itemsize
    return min(size + (4 << 20), 60 << 20)


def long_cost():
    return pl.CostEstimate(flops=200_000_000_000, bytes_accessed=1 << 20, transcendentals=0)


def ring_place(index, n):
    odd = lax.rem(index, 2)
    half = index // 2
    return (1 - odd) * half + odd * (n - 1 - half)


def ring_index(place, n):
    place = lax.rem(place + 2 * n, n)
    far = place // (n // 2)
    return (1 - far) * (2 * place) + far * (2 * (n - 1 - place) + 1)


def gather_kernel(n, pieces, early, *refs):
    refs = list(refs)

    def some(count):
        return [refs.pop(0) for _ in range(count)]

    x_ref, near_ref, count_ref = some(3)
    if early:
        slot_hbm, *store_hbm = some(5)
    out_ref, nears_ref, counts_ref = some(3)
    if early:
        o_ref, lse_ref, slot_ref, near_smem, count_smem, sk_ref, sv_ref, k_ref, v_ref, load_sem = some(10)
    own_sem, send_sem, recv_sem, tsend_sem, trecv_sem = refs
    me = lax.axis_index("seq")
    place = ring_place(me, n)
    rows = x_ref.shape[0]
    sub = rows // pieces
    half = n // 2
    ways = (1, -1)
    beside = [ring_index(place + way, n) for way in ways]
    own = [
        pltpu.make_async_copy(source, target, own_sem.at[i])
        for i, (source, target) in enumerate(
            (
                (x_ref, out_ref.at[pl.ds(pl.multiple_of(me * rows, rows), rows)]),
                (near_ref, nears_ref.at[me]),
                (count_ref, counts_ref.at[me]),
            )
        )
    ]
    for one in own:
        one.start()
    loads = []
    if early:
        sources = [slot_hbm] + store_hbm
        for i, (source, target) in enumerate(zip(sources, (slot_ref, sk_ref, sv_ref, k_ref, v_ref))):
            loads.append(pltpu.make_async_copy(source, target, load_sem.at[i]))
    for one in loads:
        one.start()
    barrier = pltpu.get_barrier_semaphore()
    for k in range(1, n):
        pl.semaphore_signal(barrier, inc=1, device_id={"seq": lax.rem(me + k, n)}, device_id_type=MESH)
    for one in own:
        one.wait()
    pl.semaphore_wait(barrier, n - 1)

    def copy(way, step, piece):
        owner = ring_index(place - ways[way] * step, n)
        there = pl.ds(pl.multiple_of(owner * rows + piece * sub, sub), sub)
        return pltpu.make_async_remote_copy(
            src_ref=out_ref.at[there],
            dst_ref=out_ref.at[there],
            send_sem=send_sem.at[way, step, piece],
            recv_sem=recv_sem.at[way, step, piece],
            device_id={"seq": beside[way]},
            device_id_type=MESH,
        )

    def piece_of(way, spot):
        return spot if way == 0 else pieces - 1 - spot

    table_copies = []
    for t, target in enumerate((nears_ref, counts_ref)):
        for k in range(1, n):
            table_copies.append(
                pltpu.make_async_remote_copy(
                    src_ref=target.at[me],
                    dst_ref=target.at[me],
                    send_sem=tsend_sem.at[t, k],
                    recv_sem=trecv_sem.at[t, k],
                    device_id={"seq": lax.rem(me + k, n)},
                    device_id_type=MESH,
                )
            )
    for one in table_copies:
        one.start()
    started = []
    for spot in range(pieces):
        for way in range(2):
            one = copy(way, 0, piece_of(way, spot))
            one.start()
            started.append(one)

    def first_listed(owner, inner):
        degree = near_ref.shape[1]
        store_blocks = k_ref.shape[0]
        listed = count_smem[owner, 0, inner]

        def look(i, best):
            e = degree - SCAN * (i + 1)
            for u in range(SCAN - 1, -1, -1):
                spot = slot_ref[near_smem[owner, inner, e + u]] - me * store_blocks
                kept = ((spot >= 0) & (spot < store_blocks) & (e + u < listed)).astype(jnp.int32)
                best = best + kept * (spot - best)
            return best

        return lax.fori_loop(0, degree // SCAN, look, jnp.int32(-1))

    def row_work(owner, inner, spot, mine):
        per_group = H // KVH
        taken = jnp.maximum(spot, 0)
        missing = jnp.minimum(spot, 0).astype(jnp.float32) * -NEG
        first_row = pl.multiple_of(owner * rows + inner * BLK, BLK)
        for g in range(k_ref.shape[2] // DH):
            cols = slice(g * DH, (g + 1) * DH)
            asked = asked_rows(out_ref, first_row, g, per_group)
            keys, values = k_ref[taken, :, cols], v_ref[taken, :, cols]
            if mine:
                near = pl.ds(pl.multiple_of(inner * BLK, BLK), BLK)
                keys = jnp.concatenate([sk_ref[near, cols], keys], axis=0)
                values = jnp.concatenate([sv_ref[near, cols], values], axis=0)
            s = scores_of(keys, asked)
            if mine:
                inside = jnp.where(causal_mask(s.shape[1]), s[:BLK], NEG)
                s = jnp.concatenate([inside, s[BLK:] + missing], axis=0)
            m = jnp.max(s, axis=0, keepdims=True)
            p = jnp.exp2(s - m)
            total = jnp.sum(p, axis=0, keepdims=True)
            lse = m + jnp.log2(total)
            if not mine:
                lse = lse + missing
            write_part(o_ref, lse_ref, owner * pieces + inner, g, weighed(values, p), total, lse)

    def row_at(way, step, spot):
        return ring_index(place - ways[way] * step, n), piece_of(way, spot)

    def scanned(step, spot):
        return [first_listed(*row_at(way, step, spot)) for way in range(2)] if early else None

    def arrived(step, spot, found):
        if early:
            for way in range(2):
                row_work(*row_at(way, step, spot), found[way], False)

    def own_rows():
        for one in table_copies:
            one.wait_recv()
        tables = [
            pltpu.make_async_copy(source, target, load_sem.at[5 + i])
            for i, (source, target) in enumerate(((nears_ref, near_smem), (counts_ref, count_smem)))
        ]
        for one in tables:
            one.start()
        for one in loads + tables:
            one.wait()
        for inner in range(pieces):
            row_work(me, inner, first_listed(me, inner), True)

    for step in range(1, half):
        for spot in range(pieces):
            first = step == 1 and spot == 0
            found = None if first else scanned(step, spot)
            for way in range(2):
                copy(way, step - 1, piece_of(way, spot)).wait_recv()
                if step < half - 1 or spot < pieces // 2:
                    one = copy(way, step, piece_of(way, spot))
                    one.start()
                    started.append(one)
            if early and first:
                own_rows()
                found = scanned(step, spot)
            arrived(step, spot, found)
    for spot in range(pieces // 2):
        found = scanned(half, spot)
        for way in range(2):
            copy(way, half - 1, piece_of(way, spot)).wait_recv()
        arrived(half, spot, found)
    for one in started:
        one.wait_send()
    for one in table_copies:
        if early:
            one.wait_send()
        else:
            one.wait()


def gathered(x, near, count, n, early):
    rows, width = x.shape
    pieces = rows // BLK
    vmem = pl.BlockSpec(memory_space=pltpu.VMEM)
    dma = pltpu.SemaphoreType.DMA
    kind = pltpu.VMEM if early else jax.ShapeDtypeStruct
    inputs = [x, near, count] + list(early)
    out_shape = [
        kind((n * rows, width), x.dtype),
        jax.ShapeDtypeStruct((n,) + near.shape, near.dtype),
        jax.ShapeDtypeStruct((n,) + count.shape, count.dtype),
    ]
    scratch = []
    held = [((n + 1, rows, width), x.dtype)]
    if early:
        slot, *stores = early
        kv_here = stores[2].shape[2] // DH
        part_shape = (n * pieces, kv_here, BLK, (H // KVH) * DH)
        out_shape += [kind(part_shape, x.dtype), kind((n * pieces, kv_here, STAT, BLK), jnp.float32)]
        scratch += [pltpu.SMEM(slot.shape, slot.dtype)]
        scratch += [pltpu.SMEM(out_shape[1].shape, near.dtype), pltpu.SMEM(out_shape[2].shape, count.dtype)]
        scratch += [pltpu.VMEM(a.shape, a.dtype) for a in stores]
        scratch += [dma((7,))]
        held += [(part_shape, x.dtype)] + [(a.shape, a.dtype) for a in stores]
    scratch += [
        dma((3,)),
        dma((2, n // 2, pieces)),
        dma((2, n // 2, pieces)),
        dma((2, n)),
        dma((2, n)),
    ]
    return pl.pallas_call(
        functools.partial(gather_kernel, n, pieces, bool(early)),
        in_specs=[pl.BlockSpec(memory_space=pltpu.HBM)] * len(inputs),
        out_specs=[vmem] * len(out_shape),
        out_shape=out_shape,
        scratch_shapes=scratch,
        compiler_params=pltpu.CompilerParams(
            collective_id=0,
            has_side_effects=True,
            vmem_limit_bytes=grant(*held),
        ),
        cost_estimate=long_cost(),
    )(*(pltpu.with_memory_space_constraint(a, pltpu.HBM) for a in inputs))


def merge(lse_a, lse_b):
    top = jnp.maximum(lse_a, lse_b)
    a = jnp.exp2(lse_a - top)
    b = jnp.exp2(lse_b - top)
    total = a + b
    return a / total, b / total, top + jnp.log2(total)


def reduce_kernel(
    n,
    small,
    o_ref,
    lse_ref,
    out_ref,
    got,
    got_lse,
    own,
    own_sem,
    send_sem,
    recv_sem,
    lsend_sem,
    lrecv_sem,
    ready=None,
):
    me = lax.axis_index("seq")
    place = ring_place(me, n)
    groups, width = got.shape[2], got.shape[4]
    wide = width // CUTS
    ways = (1, -1)
    beside = [ring_index(place + way, n) for way in ways]
    if ready is None:
        barrier = pltpu.get_barrier_semaphore()
        for other in beside:
            pl.semaphore_signal(barrier, inc=1, device_id={"seq": other}, device_id_type=MESH)

    def home(way, step):
        return ring_index(place - ways[way] * (1 + step), n)

    def fetch(way, step):
        return pltpu.make_async_copy(
            o_ref.at[home(way, step) * 2 + way], own.at[way, lax.rem(step, 2)], own_sem.at[way, lax.rem(step, 2)]
        )

    def lse_copy(way, step, g, before):
        return pltpu.make_async_remote_copy(
            src_ref=lse_ref.at[home(way, step) * 2 + way, g] if before is None else got_lse.at[way, before, g],
            dst_ref=got_lse.at[way, step, g],
            send_sem=lsend_sem.at[way, step, g],
            recv_sem=lrecv_sem.at[way, step, g],
            device_id={"seq": beside[way]},
            device_id_type=MESH,
        )

    def copy(way, step, g, cut, before):
        part = (g, slice(None), pl.ds(cut * wide, wide))
        return pltpu.make_async_remote_copy(
            src_ref=o_ref.at[(home(way, step) * 2 + way,) + part]
            if before is None
            else got.at[(way, before) + part],
            dst_ref=got.at[(way, step) + part],
            send_sem=send_sem.at[way, step, g * CUTS + cut],
            recv_sem=recv_sem.at[way, step, g * CUTS + cut],
            device_id={"seq": beside[way]},
            device_id_type=MESH,
        )

    def shares_of(way, step, g):
        lse_copy(way, step - 1, g, step - 1).wait_recv()
        if g == 0 and not small:
            fetch(way, step).wait()
        return merge(got_lse[way, step - 1, g], lse_ref[home(way, step) * 2 + way, g])

    def merged(way, step, g, cut, theirs, ours):
        copy(way, step - 1, g, cut, step - 1).wait_recv()
        at = home(way, step) * 2 + way
        columns = []
        for r in range(cut * wide // DH, (cut + 1) * wide // DH):
            cols = slice(r * DH, (r + 1) * DH)
            mine = o_ref[at, g, :, cols] if small else own[way, lax.rem(step, 2), g, :, cols]
            value = (
                got[way, step - 1, g, :, cols].astype(jnp.float32) * theirs[r : r + 1]
                + mine.astype(jnp.float32) * ours[r : r + 1]
            )
            columns.append((r, value))
        return columns

    if not small:
        for way in range(2):
            fetch(way, 1).start()
    if ready is None:
        pl.semaphore_wait(barrier, 2)
    for g in range(groups):
        for way in range(2):
            lse_copy(way, 0, g, None).start()
        for cut in range(CUTS):
            for way in range(2):
                copy(way, 0, g, cut, None).start()

    def one_step(step, carry):
        if not small:
            for way in range(2):
                fetch(way, step + 1).start()
        for g in range(groups):
            shares = []
            for way in range(2):
                theirs, ours, lse = shares_of(way, step, g)
                got_lse[way, step - 1, g] = lse
                lse_copy(way, step, g, step - 1).start()
                shares.append((theirs, ours))
            for cut in range(CUTS):
                for way in range(2):
                    for r, value in merged(way, step, g, cut, *shares[way]):
                        got[way, step - 1, g, :, r * DH : (r + 1) * DH] = value.astype(jnp.bfloat16)
                    copy(way, step, g, cut, step - 1).start()
        return carry

    lax.fori_loop(1, n - 1, one_step, 0)
    for way in range(2):
        for g in range(groups):
            theirs, ours, _ = shares_of(way, n - 1, g)
            for cut in range(CUTS):
                for r, value in merged(way, n - 1, g, cut, theirs, ours):
                    at = g * width + r * DH
                    out_ref[way * BLK : (way + 1) * BLK, at : at + DH] = jnp.transpose(value).astype(jnp.bfloat16)
        if ready is not None:
            ready(way)

    def drain_all():
        def drain(step, before):
            for g in range(groups):
                for way in range(2):
                    lse_copy(way, step, g, before).wait_send()
                    for cut in range(CUTS):
                        copy(way, step, g, cut, before).wait_send()

        drain(0, None)
        lax.fori_loop(1, n - 1, lambda step, carry: (drain(step, step - 1), carry)[1], 0)

    if ready is None:
        drain_all()
    return drain_all


def project_stages(
    n,
    heads,
    joined,
    x_ref,
    w_hbm,
    out_ref,
    w_ref,
    blocks,
    split,
    got,
    summed,
    landed,
    w_sem,
    wsend,
    wrecv,
    send_sem,
    recv_sem,
    hsend,
    hrecv,
    fsend,
    frecv,
):
    me = lax.axis_index("seq")
    mine = lax.axis_index("head")
    line = n // 2
    at, side = me // 2, lax.rem(me, 2)
    share = x_ref.shape[0] // heads
    columns = w_ref.shape[2]
    ways = (1, -1)
    early = min(2, line - 1)
    weights = pltpu.make_async_copy(w_hbm, w_ref.at[0], w_sem.at[0])
    weights.start()
    barrier = pltpu.get_barrier_semaphore()
    place = ring_place(me, n)
    for way in ways:
        other = ring_index(place + way, n)
        pl.semaphore_signal(barrier, inc=1, device_id={"seq": other}, device_id_type=MESH)
    for k in range(1, heads):
        pl.semaphore_signal(barrier, inc=1, device_id={"head": lax.rem(mine + k, heads)}, device_id_type=MESH)
    partner = at * 2 + 1 - side
    if not joined:
        for k in range(1, line):
            other = lax.rem(at + k, line) * 2 + side
            pl.semaphore_signal(barrier, inc=1, device_id={"seq": other}, device_id_type=MESH)
        pl.semaphore_signal(barrier, inc=1, device_id={"seq": partner}, device_id_type=MESH)
    pl.semaphore_wait(barrier, heads + 1 if joined else heads + line + 1)

    def inside(spot):
        return jnp.logical_and(spot >= 0, spot < line)

    def copy(way, step, piece, first):
        there = (at - ways[way] * step, pl.ds(pl.multiple_of(piece * share, share), share))
        return pltpu.make_async_remote_copy(
            src_ref=x_ref.at[there[1]] if first else blocks.at[there],
            dst_ref=blocks.at[there],
            send_sem=send_sem.at[way, step, piece],
            recv_sem=recv_sem.at[way, step, piece],
            device_id={"seq": (at + ways[way]) * 2 + side},
            device_id_type=MESH,
        )

    def leaves(way, step):
        return jnp.logical_and(inside(at - ways[way] * step), inside(at + ways[way]))

    def to_head(i, j, source, to):
        return pltpu.make_async_remote_copy(
            src_ref=split.at[i, j, to],
            dst_ref=got.at[i, j, source],
            send_sem=hsend.at[i, j, to],
            recv_sem=hrecv.at[i, j, source],
            device_id={"head": to},
            device_id_type=MESH,
        )

    def to_row(i, j, source):
        owner = source * 2 + (side if j == 0 else 1 - side)
        return pltpu.make_async_remote_copy(
            src_ref=summed.at[i, j],
            dst_ref=landed.at[owner],
            send_sem=fsend.at[i, j],
            recv_sem=frecv.at[source, j],
            device_id={"seq": i * 2 + side},
            device_id_type=MESH,
        )

    def unit(i, c, js, own):
        rows = pl.ds(pl.multiple_of(c * share, share), share)
        value = x_ref[rows] if own else blocks[i, rows]
        for j in js:
            split[i, j, c] = jnp.dot(value, w_ref[j], preferred_element_type=jnp.float32).astype(jnp.bfloat16)

            @pl.when(mine != c)
            def _():
                to_head(i, j, mine, c).start()

    def visit(step, c, js, arriving):
        for way in range(2):
            i = at - ways[way] * step

            @pl.when(inside(i))
            def _():
                if arriving:
                    copy(way, step - 1, c, False).wait_recv()

                    @pl.when(inside(at + ways[way]))
                    def _():
                        copy(way, step, c, False).start()

                unit(i, c, js, False)

    def total_of(i, j):
        total = split[i, j, mine].astype(jnp.float32)
        for k in range(1, heads):
            source = lax.rem(mine + k, heads)
            to_head(i, j, source, mine).wait_recv()
            total = total + got[i, j, source].astype(jnp.float32)
        return total.astype(jnp.bfloat16)

    def settle_own(j):
        landed[at * 2 + (side if j == 0 else 1 - side)] = total_of(at, j)

    def settle(step, js):
        for way in range(2):
            i = at - ways[way] * step

            @pl.when(inside(i))
            def _():
                for j in js:
                    summed[i, j] = total_of(i, j)
                    to_row(i, j, at).start()

    def each(function):
        lax.fori_loop(0, heads, lambda c, carry: (function(c), carry)[1], 0)

    def start_own(c):
        for way in range(2):

            @pl.when(inside(at + ways[way]))
            def _():
                copy(way, 0, c, True).start()

    def run():
        weights.wait()
        exchange = pltpu.make_async_remote_copy(
            src_ref=w_ref.at[0],
            dst_ref=w_ref.at[1],
            send_sem=wsend.at[0],
            recv_sem=wrecv.at[0],
            device_id={"seq": partner},
            device_id_type=MESH,
        )
        exchange.start()
        each(lambda c: unit(at, c, (0,), True))

        def first_steps(step, carry):
            each(lambda c: visit(step, c, (0,), True))

            @pl.when(step == 1)
            def _():
                settle_own(0)

            @pl.when(step > 1)
            def _():
                settle(step - 1, (0,))

            return carry

        lax.fori_loop(1, early + 1, first_steps, 0)
        exchange.wait()
        each(lambda c: unit(at, c, (1,), True))
        lax.fori_loop(1, early + 1, lambda t, carry: (each(lambda c: visit(t, c, (1,), False)), carry)[1], 0)
        settle(early, (0,))

        def settle_early():
            settle_own(1)
            lax.fori_loop(1, early + 1, lambda t, carry: (settle(t, (1,)), carry)[1], 0)

        def late_step(step, carry):
            def late_visit(c):
                visit(step, c, (0, 1), True)

                @pl.when(jnp.logical_and(c == 0, step == early + 1))
                def _():
                    settle_early()

                @pl.when(jnp.logical_and(c == 0, step > early + 1))
                def _():
                    settle(step - 1, (0, 1))

                @pl.when(jnp.logical_and(mine == c - 1, step == line - 1))
                def _():
                    settle(step, (0, 1))

            each(late_visit)
            return carry

        if line - 1 > early:
            lax.fori_loop(early + 1, line, late_step, 0)

            @pl.when(mine == heads - 1)
            def _():
                settle(line - 1, (0, 1))

        else:
            settle_early()

        for way in range(2):
            for step in range(2):

                def finish(c):
                    @pl.when(leaves(way, step))
                    def _():
                        copy(way, step, c, step == 0).wait_send()

                if step == 0:
                    each(finish)
                else:

                    def finish_rest(t, carry):
                        def one(c):
                            @pl.when(leaves(way, t))
                            def _():
                                copy(way, t, c, False).wait_send()

                        each(one)
                        return carry

                    lax.fori_loop(1, line, finish_rest, 0)

        def drain(i, carry):
            for j in range(2):
                for k in range(1, heads):
                    to_head(i, j, mine, lax.rem(mine + k, heads)).wait_send()

                @pl.when(i != at)
                def _():
                    to_row(i, j, at).wait_send()
                    to_row(at, j, i).wait_recv()

            return carry

        lax.fori_loop(0, line, drain, 0)
        for i in range(n):
            out_ref[:, i * columns : (i + 1) * columns] = landed[i]

    return start_own, each, run


def project_kernel(n, heads, *refs):
    start_own, each, run = project_stages(n, heads, False, *refs)
    each(start_own)
    run()


def join_kernel(n, heads, o_ref, lse_ref, w_hbm, out_ref, x_ref, *refs):
    start_own, _, run = project_stages(n, heads, True, x_ref, w_hbm, out_ref, *refs[8:])
    per_way = BLK * heads // x_ref.shape[0]

    def ready(way):
        for c in range(per_way):
            start_own(way * per_way + c)

    drain = reduce_kernel(n, True, o_ref, lse_ref, x_ref, *refs[:8], ready=ready)
    run()
    drain()


def project_plan(n, heads, rows, width, columns, dtype):
    share = rows // heads
    line = n // 2
    dma = pltpu.SemaphoreType.DMA
    scratch = [
        pltpu.VMEM((2, width, columns), dtype),
        pltpu.VMEM((line, rows, width), dtype),
        pltpu.VMEM((line, 2, heads, share, columns), dtype),
        pltpu.VMEM((line, 2, heads, share, columns), dtype),
        pltpu.VMEM((line, 2, share, columns), dtype),
        pltpu.VMEM((n, share, columns), dtype),
        dma((1,)),
        dma((1,)),
        dma((1,)),
        dma((2, line, heads)),
        dma((2, line, heads)),
        dma((line, 2, heads)),
        dma((line, 2, heads)),
        dma((line, 2)),
        dma((line, 2)),
    ]
    padded = max(columns, BLK)
    held = [
        ((2, width, padded), dtype),
        ((line + 2, rows, width), dtype),
        ((2, n, heads, share, padded), dtype),
        ((3, n, share, padded), dtype),
    ]
    return scratch, held


def reduce_plan(n, small, kv_here, group_width):
    dma = pltpu.SemaphoreType.DMA((2, n - 1, kv_here))
    dma_cuts = pltpu.SemaphoreType.DMA((2, n - 1, kv_here * CUTS))
    scratch = [
        pltpu.VMEM((2, n - 1, kv_here, BLK, group_width), jnp.bfloat16),
        pltpu.VMEM((2, n - 1, kv_here, STAT, BLK), jnp.float32),
        pltpu.VMEM((2, 2, 1 if small else kv_here, BLK, group_width), jnp.bfloat16),
        pltpu.SemaphoreType.DMA((2, 2)),
        dma_cuts,
        dma_cuts,
        dma,
        dma,
    ]
    held = [
        ((2, n + 1, kv_here, BLK, group_width), jnp.bfloat16),
        ((2, 2 * n - 1, kv_here, STAT, BLK), jnp.float32),
    ]
    return scratch, held


def mixed_from(parts, lse, weight, n, heads, rows, width, small):
    _, kv_here, _, group_width = parts.shape
    columns = weight.shape[1]
    vmem = pl.BlockSpec(memory_space=pltpu.VMEM)
    anywhere = pl.BlockSpec(memory_space=pl.ANY)
    reduce_scratch, reduce_held = reduce_plan(n, small, kv_here, group_width)
    project_scratch, project_held = project_plan(n, heads, rows, width, columns, parts.dtype)
    attended = jax.ShapeDtypeStruct((rows, width), parts.dtype)
    out = jax.ShapeDtypeStruct((rows // heads, n * columns), parts.dtype)

    def call(kernel, number, in_specs, out_shape, scratch, held):
        return pl.pallas_call(
            kernel,
            in_specs=in_specs,
            out_specs=vmem,
            out_shape=out_shape,
            scratch_shapes=scratch,
            compiler_params=pltpu.CompilerParams(
                collective_id=number, has_side_effects=True, vmem_limit_bytes=grant(*held)
            ),
            cost_estimate=long_cost(),
        )

    if small:
        scratch = [pltpu.VMEM((rows, width), parts.dtype)] + reduce_scratch + project_scratch
        held = reduce_held + project_held + [(parts.shape, parts.dtype)]
        kernel = functools.partial(join_kernel, n, heads)
        return call(kernel, 1, [vmem, vmem, anywhere], out, scratch, held)(parts, lse, weight)

    def kernel(*refs):
        reduce_kernel(n, small, *refs)

    x = call(kernel, 1, [anywhere, vmem], attended, reduce_scratch, reduce_held)(parts, lse)
    kernel = functools.partial(project_kernel, n, heads)
    return call(kernel, 2, [vmem, anywhere], out, project_scratch, project_held)(x, weight)


def body(
    queries,
    self_keys,
    self_values,
    store_keys,
    store_values,
    kv_slot,
    neighbours,
    counts,
    out_weight,
):
    n = lax.axis_size("seq")
    head_count = lax.axis_size("head")
    local_blocks, degree = neighbours.shape
    local_rows, width = queries.shape
    store_blocks = store_keys.shape[0] // BLK
    all_blocks = local_blocks * n
    kv_here = store_keys.shape[1] // DH
    group_width = (H // KVH) * DH
    rows = (H // KVH) * BLK
    small = queries.size * n * queries.dtype.itemsize <= 8 << 20
    count_row = counts.reshape(1, local_blocks)
    stores = (self_keys, self_values, store_keys, store_values)
    cut = tuple(a.reshape(store_blocks, BLK, -1) for a in stores[2:])
    smem = pl.BlockSpec(memory_space=pltpu.SMEM)
    vmem = pl.BlockSpec(memory_space=pltpu.VMEM)
    params = pltpu.CompilerParams(vmem_limit_bytes=28 << 20)
    cost = pl.CostEstimate(flops=2_000_000_000, bytes_accessed=12 << 20, transcendentals=4_000_000)
    scratch = [
        pltpu.SMEM((degree + 1,), jnp.int32),
        pltpu.VMEM((kv_here, DH, rows), jnp.float32),
        pltpu.VMEM((kv_here, rows), jnp.float32),
        pltpu.VMEM((kv_here, rows), jnp.float32),
    ]
    part_shape = (all_blocks, kv_here, BLK, group_width)
    lse_shape = (all_blocks, kv_here, STAT, BLK)
    if small:
        all_queries, near, count, parts, lse = gathered(queries, neighbours, count_row, n, (kv_slot,) + stores[:2] + cut)
        parts, lse = pl.pallas_call(
            functools.partial(rest_kernel, local_blocks, store_blocks),
            in_specs=[smem] * 3 + [vmem] * 7,
            out_specs=[vmem, vmem],
            out_shape=[pltpu.VMEM(part_shape, jnp.bfloat16), pltpu.VMEM(lse_shape, jnp.float32)],
            scratch_shapes=scratch,
            input_output_aliases={8: 0, 9: 1},
            compiler_params=params,
            cost_estimate=cost,
        )(kv_slot, near, count, all_queries, *stores, parts, lse)
    else:
        all_queries, near, count = gathered(queries, neighbours, count_row, n, ())
        parts, lse = pl.pallas_call(
            functools.partial(part_kernel, local_blocks, store_blocks),
            grid=(all_blocks,),
            in_specs=[smem] * 3 + [pl.BlockSpec((BLK, width), lambda i: (i, 0))] + [vmem] * 4,
            out_specs=[
                pl.BlockSpec((1, kv_here, BLK, group_width), lambda i: (i, 0, 0, 0)),
                pl.BlockSpec((1, kv_here, STAT, BLK), lambda i: (i, 0, 0, 0)),
            ],
            out_shape=[
                jax.ShapeDtypeStruct(part_shape, jnp.bfloat16),
                jax.ShapeDtypeStruct(lse_shape, jnp.float32),
            ],
            scratch_shapes=scratch,
            compiler_params=params,
            cost_estimate=cost,
        )(kv_slot, near, count, all_queries, *stores)
    return mixed_from(parts, lse, out_weight, n, head_count, local_rows, width, small)


def solution(mesh):
    placed = (
        P("seq", "head"),
        P("seq", "head"),
        P("seq", "head"),
        P("seq", "head"),
        P("seq", "head"),
        P(),
        P("seq", None),
        P("seq"),
        P("head", "seq"),
    )
    return jax.shard_map(
        body, mesh=mesh, in_specs=placed, out_specs=P(("seq", "head"), None), check_vma=False
    )
```

```python
import functools

import jax
import jax.numpy as jnp
from jax import lax
from jax.experimental import pallas as pl
from jax.experimental.pallas import tpu as pltpu
from jax.sharding import PartitionSpec as P

H = 32
KVH = 8
DH = 128
BLK = 128
NEG = -1e30
SCAN = 4
CUTS = 1
LOG2E = 1.4426950408889634
MESH = pl.DeviceIdType.MESH


def asked_rows(q_ref, first_row, g, per_group):
    return jnp.concatenate(
        [
            q_ref[pl.ds(first_row, BLK), (g * per_group + r) * DH : (g * per_group + r + 1) * DH]
            for r in range(per_group)
        ],
        axis=0,
    )


def scores_of(keys, asked):
    scaling = DH ** (-0.5) * LOG2E
    return lax.dot_general(keys, asked, (((1,), (1,)), ((), ())), preferred_element_type=jnp.float32) * scaling


def weighed(values, p):
    return lax.dot_general(
        values, p.astype(jnp.bfloat16), (((0,), (0,)), ((), ())), preferred_element_type=jnp.float32
    )


def causal_mask(rows):
    position = lax.rem(lax.broadcasted_iota(jnp.int32, (BLK, rows), 1), BLK)
    return position >= lax.broadcasted_iota(jnp.int32, (BLK, rows), 0)


def write_part(o_ref, lse_ref, here, g, acc, total, lse):
    per_group = lse.shape[1] // BLK
    o_ref[here, g] = (acc * (1.0 / total)).astype(jnp.bfloat16)
    for r in range(per_group):
        head = g * per_group + r
        lse_ref[here, head : head + 1] = lse[:, r * BLK : (r + 1) * BLK]


def part_row(
    block,
    here,
    first_row,
    done,
    local_blocks,
    store_blocks,
    slot_ref,
    near_ref,
    count_ref,
    q_ref,
    sk_ref,
    sv_ref,
    k_ref,
    v_ref,
    o_ref,
    lse_ref,
    list_ref,
    acc_ref,
    max_ref,
    sum_ref,
):
    owner, inner = lax.div(block, local_blocks), lax.rem(block, local_blocks)
    me = lax.axis_index("seq")
    per_group = H // KVH
    kv_here = k_ref.shape[1] // DH
    rows = per_group * BLK
    listed = count_ref[owner, 0, inner]
    first_slot = me * store_blocks

    def scan_entries(i, found):
        places = [slot_ref[near_ref[owner, inner, i * SCAN + u]] - first_slot for u in range(SCAN)]
        for u, place in enumerate(places):
            list_ref[found] = place
            kept = (place >= 0) & (place < store_blocks) & (i * SCAN + u < listed)
            found = found + kept.astype(jnp.int32)
        return found

    found = lax.fori_loop(0, lax.div(listed + (SCAN - 1), SCAN), scan_entries, jnp.int32(0))
    home = owner == me
    if not done:

        @pl.when(jnp.logical_and(found == 0, jnp.logical_not(home)))
        def _():
            o_ref[here] = jnp.zeros(o_ref.shape[1:], o_ref.dtype)
            lse_ref[here] = jnp.full(lse_ref.shape[1:], NEG, lse_ref.dtype)

    @pl.when(found > done if done else jnp.logical_or(found > 0, home))
    def _():
        if done:
            for g in range(kv_here):
                max_ref[g : g + 1] = jnp.concatenate(
                    [
                        lse_ref[here, head : head + 1]
                        for head in range(g * per_group, (g + 1) * per_group)
                    ],
                    axis=1,
                )
                sum_ref[g : g + 1] = jnp.ones((1, rows), jnp.float32)
                acc_ref[g] = o_ref[here, g].astype(jnp.float32)
        else:

            @pl.when(home)
            def _():
                start = pl.multiple_of(inner * BLK, BLK)
                for g in range(kv_here):
                    cols = slice(g * DH, (g + 1) * DH)
                    asked = asked_rows(q_ref, first_row, g, per_group)
                    s = jnp.where(causal_mask(rows), scores_of(sk_ref[pl.ds(start, BLK), cols], asked), NEG)
                    m = jnp.max(s, axis=0, keepdims=True)
                    p = jnp.exp2(s - m)
                    max_ref[g : g + 1] = m
                    sum_ref[g : g + 1] = jnp.sum(p, axis=0, keepdims=True)
                    acc_ref[g] = weighed(sv_ref[pl.ds(start, BLK), cols], p)

            @pl.when(jnp.logical_not(home))
            def _():
                max_ref[...] = jnp.full_like(max_ref, NEG)
                sum_ref[...] = jnp.zeros_like(sum_ref)
                acc_ref[...] = jnp.zeros_like(acc_ref)

        def take(*places):
            starts = [pl.multiple_of(place * BLK, BLK) for place in places]

            def rows_of(ref, cols):
                return jnp.concatenate([ref[pl.ds(start, BLK), cols] for start in starts], axis=0)

            for g in range(kv_here):
                cols = slice(g * DH, (g + 1) * DH)
                s = scores_of(rows_of(k_ref, cols), asked_rows(q_ref, first_row, g, per_group))
                old = max_ref[g : g + 1]
                new = jnp.maximum(old, jnp.max(s, axis=0, keepdims=True))
                p = jnp.exp2(s - new)
                shrink = jnp.exp2(old - new)
                max_ref[g : g + 1] = new
                sum_ref[g : g + 1] = sum_ref[g : g + 1] * shrink + jnp.sum(p, axis=0, keepdims=True)
                acc_ref[g] = acc_ref[g] * shrink + weighed(rows_of(v_ref, cols), p)

        left = found - done

        @pl.loop(0, lax.div(left, 2))
        def _(i):
            take(list_ref[done + 2 * i], list_ref[done + 2 * i + 1])

        @pl.when(lax.rem(left, 2) == 1)
        def _():
            take(list_ref[found - 1])

        for g in range(kv_here):
            total = sum_ref[g : g + 1]
            write_part(o_ref, lse_ref, here, g, acc_ref[g], total, max_ref[g : g + 1] + jnp.log2(total))


def part_kernel(local_blocks, store_blocks, *refs):
    block = pl.program_id(0)
    part_row(block, 0, 0, 0, local_blocks, store_blocks, *refs)


def rest_kernel(local_blocks, store_blocks, *refs):
    def row(block, carry):
        first_row = pl.multiple_of(block * BLK, BLK)
        part_row(block, block, first_row, 1, local_blocks, store_blocks, *refs[:8], *refs[10:])
        return carry

    lax.fori_loop(0, refs[10].shape[0], row, 0)


def grant(*arrays):
    size = 0
    for shape, dtype in arrays:
        cells = 1
        for d in shape:
            cells = cells * d
        size += cells * jnp.dtype(dtype).itemsize
    return min(size + (4 << 20), 60 << 20)


def long_cost():
    return pl.CostEstimate(flops=200_000_000_000, bytes_accessed=1 << 20, transcendentals=0)


def ring_place(index, n):
    odd = lax.rem(index, 2)
    half = index // 2
    return (1 - odd) * half + odd * (n - 1 - half)


def ring_index(place, n):
    place = lax.rem(place + 2 * n, n)
    far = place // (n // 2)
    return (1 - far) * (2 * place) + far * (2 * (n - 1 - place) + 1)


def gather_kernel(n, pieces, early, *refs):
    refs = list(refs)

    def some(count):
        return [refs.pop(0) for _ in range(count)]

    x_ref, near_ref, count_ref = some(3)
    if early:
        slot_hbm, *store_hbm = some(5)
    out_ref, nears_ref, counts_ref = some(3)
    if early:
        o_ref, lse_ref, slot_ref, near_smem, count_smem, sk_ref, sv_ref, k_ref, v_ref, load_sem = some(10)
    own_sem, send_sem, recv_sem, tsend_sem, trecv_sem = refs
    me = lax.axis_index("seq")
    place = ring_place(me, n)
    rows = x_ref.shape[0]
    sub = rows // pieces
    half = n // 2
    ways = (1, -1)
    beside = [ring_index(place + way, n) for way in ways]
    own = [
        pltpu.make_async_copy(source, target, own_sem.at[i])
        for i, (source, target) in enumerate(
            (
                (x_ref, out_ref.at[pl.ds(pl.multiple_of(me * rows, rows), rows)]),
                (near_ref, nears_ref.at[me]),
                (count_ref, counts_ref.at[me]),
            )
        )
    ]
    for one in own:
        one.start()
    loads = []
    if early:
        sources = [slot_hbm] + store_hbm
        for i, (source, target) in enumerate(zip(sources, (slot_ref, sk_ref, sv_ref, k_ref, v_ref))):
            loads.append(pltpu.make_async_copy(source, target, load_sem.at[i]))
    for one in loads:
        one.start()
    barrier = pltpu.get_barrier_semaphore()
    for k in range(1, n):
        pl.semaphore_signal(barrier, inc=1, device_id={"seq": lax.rem(me + k, n)}, device_id_type=MESH)
    for one in own:
        one.wait()
    pl.semaphore_wait(barrier, n - 1)

    def copy(way, step, piece):
        owner = ring_index(place - ways[way] * step, n)
        there = pl.ds(pl.multiple_of(owner * rows + piece * sub, sub), sub)
        return pltpu.make_async_remote_copy(
            src_ref=out_ref.at[there],
            dst_ref=out_ref.at[there],
            send_sem=send_sem.at[way, step, piece],
            recv_sem=recv_sem.at[way, step, piece],
            device_id={"seq": beside[way]},
            device_id_type=MESH,
        )

    def piece_of(way, spot):
        return spot if way == 0 else pieces - 1 - spot

    table_copies = []
    for t, target in enumerate((nears_ref, counts_ref)):
        for k in range(1, n):
            table_copies.append(
                pltpu.make_async_remote_copy(
                    src_ref=target.at[me],
                    dst_ref=target.at[me],
                    send_sem=tsend_sem.at[t, k],
                    recv_sem=trecv_sem.at[t, k],
                    device_id={"seq": lax.rem(me + k, n)},
                    device_id_type=MESH,
                )
            )
    for one in table_copies:
        one.start()
    started = []
    for spot in range(pieces):
        for way in range(2):
            one = copy(way, 0, piece_of(way, spot))
            one.start()
            started.append(one)

    def first_listed(owner, inner):
        degree = near_ref.shape[1]
        store_blocks = k_ref.shape[0]
        listed = count_smem[owner, 0, inner]

        def look(i, best):
            e = degree - SCAN * (i + 1)
            for u in range(SCAN - 1, -1, -1):
                spot = slot_ref[near_smem[owner, inner, e + u]] - me * store_blocks
                kept = ((spot >= 0) & (spot < store_blocks) & (e + u < listed)).astype(jnp.int32)
                best = best + kept * (spot - best)
            return best

        return lax.fori_loop(0, degree // SCAN, look, jnp.int32(-1))

    def row_work(owner, inner, spot, mine):
        per_group = H // KVH
        taken = jnp.maximum(spot, 0)
        missing = jnp.minimum(spot, 0).astype(jnp.float32) * -NEG
        first_row = pl.multiple_of(owner * rows + inner * BLK, BLK)
        for g in range(k_ref.shape[2] // DH):
            cols = slice(g * DH, (g + 1) * DH)
            asked = asked_rows(out_ref, first_row, g, per_group)
            keys, values = k_ref[taken, :, cols], v_ref[taken, :, cols]
            if mine:
                near = pl.ds(pl.multiple_of(inner * BLK, BLK), BLK)
                keys = jnp.concatenate([sk_ref[near, cols], keys], axis=0)
                values = jnp.concatenate([sv_ref[near, cols], values], axis=0)
            s = scores_of(keys, asked)
            if mine:
                inside = jnp.where(causal_mask(s.shape[1]), s[:BLK], NEG)
                s = jnp.concatenate([inside, s[BLK:] + missing], axis=0)
            m = jnp.max(s, axis=0, keepdims=True)
            p = jnp.exp2(s - m)
            total = jnp.sum(p, axis=0, keepdims=True)
            lse = m + jnp.log2(total)
            if not mine:
                lse = lse + missing
            write_part(o_ref, lse_ref, owner * pieces + inner, g, weighed(values, p), total, lse)

    def row_at(way, step, spot):
        return ring_index(place - ways[way] * step, n), piece_of(way, spot)

    def scanned(step, spot):
        return [first_listed(*row_at(way, step, spot)) for way in range(2)] if early else None

    def arrived(step, spot, found):
        if early:
            for way in range(2):
                row_work(*row_at(way, step, spot), found[way], False)

    def own_rows():
        for one in table_copies:
            one.wait_recv()
        tables = [
            pltpu.make_async_copy(source, target, load_sem.at[5 + i])
            for i, (source, target) in enumerate(((nears_ref, near_smem), (counts_ref, count_smem)))
        ]
        for one in tables:
            one.start()
        for one in loads + tables:
            one.wait()
        for inner in range(pieces):
            row_work(me, inner, first_listed(me, inner), True)

    for step in range(1, half):
        for spot in range(pieces):
            first = step == 1 and spot == 0
            found = None if first else scanned(step, spot)
            for way in range(2):
                copy(way, step - 1, piece_of(way, spot)).wait_recv()
                if step < half - 1 or spot < pieces // 2:
                    one = copy(way, step, piece_of(way, spot))
                    one.start()
                    started.append(one)
            if early and first:
                own_rows()
                found = scanned(step, spot)
            arrived(step, spot, found)
    for spot in range(pieces // 2):
        found = scanned(half, spot)
        for way in range(2):
            copy(way, half - 1, piece_of(way, spot)).wait_recv()
        arrived(half, spot, found)
    for one in started:
        one.wait_send()
    for one in table_copies:
        if early:
            one.wait_send()
        else:
            one.wait()


def gathered(x, near, count, n, early):
    rows, width = x.shape
    pieces = rows // BLK
    vmem = pl.BlockSpec(memory_space=pltpu.VMEM)
    dma = pltpu.SemaphoreType.DMA
    kind = pltpu.VMEM if early else jax.ShapeDtypeStruct
    inputs = [x, near, count] + list(early)
    out_shape = [
        kind((n * rows, width), x.dtype),
        jax.ShapeDtypeStruct((n,) + near.shape, near.dtype),
        jax.ShapeDtypeStruct((n,) + count.shape, count.dtype),
    ]
    scratch = []
    held = [((n + 1, rows, width), x.dtype)]
    if early:
        slot, *stores = early
        kv_here = stores[2].shape[2] // DH
        part_shape = (n * pieces, kv_here, BLK, (H // KVH) * DH)
        out_shape += [kind(part_shape, x.dtype), kind((n * pieces, kv_here * (H // KVH), BLK), jnp.float32)]
        scratch += [pltpu.SMEM(slot.shape, slot.dtype)]
        scratch += [pltpu.SMEM(out_shape[1].shape, near.dtype), pltpu.SMEM(out_shape[2].shape, count.dtype)]
        scratch += [pltpu.VMEM(a.shape, a.dtype) for a in stores]
        scratch += [dma((7,))]
        held += [(part_shape, x.dtype)] + [(a.shape, a.dtype) for a in stores]
    scratch += [
        dma((3,)),
        dma((2, n // 2, pieces)),
        dma((2, n // 2, pieces)),
        dma((2, n)),
        dma((2, n)),
    ]
    return pl.pallas_call(
        functools.partial(gather_kernel, n, pieces, bool(early)),
        in_specs=[pl.BlockSpec(memory_space=pltpu.HBM)] * len(inputs),
        out_specs=[vmem] * len(out_shape),
        out_shape=out_shape,
        scratch_shapes=scratch,
        compiler_params=pltpu.CompilerParams(
            collective_id=0,
            has_side_effects=True,
            vmem_limit_bytes=grant(*held),
        ),
        cost_estimate=long_cost(),
    )(*(pltpu.with_memory_space_constraint(a, pltpu.HBM) for a in inputs))


def merge(lse_a, lse_b):
    top = jnp.maximum(lse_a, lse_b)
    a = jnp.exp2(lse_a - top)
    b = jnp.exp2(lse_b - top)
    total = a + b
    return a / total, b / total, top + jnp.log2(total)


def reduce_kernel(
    n,
    small,
    o_ref,
    lse_ref,
    out_ref,
    got,
    got_lse,
    own,
    own_sem,
    send_sem,
    recv_sem,
    lsend_sem,
    lrecv_sem,
    ready=None,
):
    me = lax.axis_index("seq")
    place = ring_place(me, n)
    groups, width = got.shape[2], got.shape[4]
    wide = width // CUTS
    ways = (1, -1)
    beside = [ring_index(place + way, n) for way in ways]
    if ready is None:
        barrier = pltpu.get_barrier_semaphore()
        for other in beside:
            pl.semaphore_signal(barrier, inc=1, device_id={"seq": other}, device_id_type=MESH)

    def home(way, step):
        return ring_index(place - ways[way] * (1 + step), n)

    def fetch(way, step):
        return pltpu.make_async_copy(
            o_ref.at[home(way, step) * 2 + way], own.at[way, lax.rem(step, 2)], own_sem.at[way, lax.rem(step, 2)]
        )

    def lse_copy(way, step, before):
        return pltpu.make_async_remote_copy(
            src_ref=lse_ref.at[home(way, step) * 2 + way] if before is None else got_lse.at[way, before],
            dst_ref=got_lse.at[way, step],
            send_sem=lsend_sem.at[way, step],
            recv_sem=lrecv_sem.at[way, step],
            device_id={"seq": beside[way]},
            device_id_type=MESH,
        )

    def copy(way, step, g, cut, before):
        part = (g, slice(None), pl.ds(cut * wide, wide))
        return pltpu.make_async_remote_copy(
            src_ref=o_ref.at[(home(way, step) * 2 + way,) + part]
            if before is None
            else got.at[(way, before) + part],
            dst_ref=got.at[(way, step) + part],
            send_sem=send_sem.at[way, step, g * CUTS + cut],
            recv_sem=recv_sem.at[way, step, g * CUTS + cut],
            device_id={"seq": beside[way]},
            device_id_type=MESH,
        )

    def shares_of(way, step):
        lse_copy(way, step - 1, step - 1).wait_recv()
        if not small:
            fetch(way, step).wait()
        return merge(got_lse[way, step - 1], lse_ref[home(way, step) * 2 + way])

    def merged(way, step, g, cut, theirs, ours):
        copy(way, step - 1, g, cut, step - 1).wait_recv()
        at = home(way, step) * 2 + way
        columns = []
        for r in range(cut * wide // DH, (cut + 1) * wide // DH):
            cols = slice(r * DH, (r + 1) * DH)
            head = g * (width // DH) + r
            mine = o_ref[at, g, :, cols] if small else own[way, lax.rem(step, 2), g, :, cols]
            value = (
                got[way, step - 1, g, :, cols].astype(jnp.float32) * theirs[head : head + 1]
                + mine.astype(jnp.float32) * ours[head : head + 1]
            )
            columns.append((r, value))
        return columns

    if not small:
        for way in range(2):
            fetch(way, 1).start()
    if ready is None:
        pl.semaphore_wait(barrier, 2)
    for way in range(2):
        lse_copy(way, 0, None).start()
    for g in range(groups):
        for cut in range(CUTS):
            for way in range(2):
                copy(way, 0, g, cut, None).start()

    def one_step(step, carry):
        if not small:
            for way in range(2):
                fetch(way, step + 1).start()
        shares = []
        for way in range(2):
            theirs, ours, lse = shares_of(way, step)
            got_lse[way, step - 1] = lse
            lse_copy(way, step, step - 1).start()
            shares.append((theirs, ours))
        for g in range(groups):
            for cut in range(CUTS):
                for way in range(2):
                    for r, value in merged(way, step, g, cut, *shares[way]):
                        got[way, step - 1, g, :, r * DH : (r + 1) * DH] = value.astype(jnp.bfloat16)
                    copy(way, step, g, cut, step - 1).start()
        return carry

    lax.fori_loop(1, n - 1, one_step, 0)
    for way in range(2):
        theirs, ours, _ = shares_of(way, n - 1)
        for g in range(groups):
            for cut in range(CUTS):
                for r, value in merged(way, n - 1, g, cut, theirs, ours):
                    at = g * width + r * DH
                    out_ref[way * BLK : (way + 1) * BLK, at : at + DH] = jnp.transpose(value).astype(jnp.bfloat16)
        if ready is not None:
            ready(way)

    def drain_all():
        def drain(step, before):
            for way in range(2):
                lse_copy(way, step, before).wait_send()
                for g in range(groups):
                    for cut in range(CUTS):
                        copy(way, step, g, cut, before).wait_send()

        drain(0, None)
        lax.fori_loop(1, n - 1, lambda step, carry: (drain(step, step - 1), carry)[1], 0)

    if ready is None:
        drain_all()
    return drain_all


def project_stages(
    n,
    heads,
    joined,
    x_ref,
    w_hbm,
    out_ref,
    w_ref,
    blocks,
    split,
    got,
    summed,
    landed,
    w_sem,
    wsend,
    wrecv,
    send_sem,
    recv_sem,
    hsend,
    hrecv,
    fsend,
    frecv,
):
    me = lax.axis_index("seq")
    mine = lax.axis_index("head")
    line = n // 2
    at, side = me // 2, lax.rem(me, 2)
    share = x_ref.shape[0] // heads
    columns = w_ref.shape[2]
    ways = (1, -1)
    early = min(2, line - 1)
    weights = pltpu.make_async_copy(w_hbm, w_ref.at[0], w_sem.at[0])
    weights.start()
    barrier = pltpu.get_barrier_semaphore()
    place = ring_place(me, n)
    for way in ways:
        other = ring_index(place + way, n)
        pl.semaphore_signal(barrier, inc=1, device_id={"seq": other}, device_id_type=MESH)
    for k in range(1, heads):
        pl.semaphore_signal(barrier, inc=1, device_id={"head": lax.rem(mine + k, heads)}, device_id_type=MESH)
    partner = at * 2 + 1 - side
    if not joined:
        for k in range(1, line):
            other = lax.rem(at + k, line) * 2 + side
            pl.semaphore_signal(barrier, inc=1, device_id={"seq": other}, device_id_type=MESH)
        pl.semaphore_signal(barrier, inc=1, device_id={"seq": partner}, device_id_type=MESH)
    pl.semaphore_wait(barrier, heads + 1 if joined else heads + line + 1)

    def inside(spot):
        return jnp.logical_and(spot >= 0, spot < line)

    def copy(way, step, piece, first):
        there = (at - ways[way] * step, pl.ds(pl.multiple_of(piece * share, share), share))
        return pltpu.make_async_remote_copy(
            src_ref=x_ref.at[there[1]] if first else blocks.at[there],
            dst_ref=blocks.at[there],
            send_sem=send_sem.at[way, step, piece],
            recv_sem=recv_sem.at[way, step, piece],
            device_id={"seq": (at + ways[way]) * 2 + side},
            device_id_type=MESH,
        )

    def leaves(way, step):
        return jnp.logical_and(inside(at - ways[way] * step), inside(at + ways[way]))

    def to_head(i, j, source, to):
        return pltpu.make_async_remote_copy(
            src_ref=split.at[i, j, to],
            dst_ref=got.at[i, j, source],
            send_sem=hsend.at[i, j, to],
            recv_sem=hrecv.at[i, j, source],
            device_id={"head": to},
            device_id_type=MESH,
        )

    def to_row(i, j, source):
        owner = source * 2 + (side if j == 0 else 1 - side)
        return pltpu.make_async_remote_copy(
            src_ref=summed.at[i, j],
            dst_ref=landed.at[owner],
            send_sem=fsend.at[i, j],
            recv_sem=frecv.at[source, j],
            device_id={"seq": i * 2 + side},
            device_id_type=MESH,
        )

    def unit(i, c, js, own):
        rows = pl.ds(pl.multiple_of(c * share, share), share)
        value = x_ref[rows] if own else blocks[i, rows]
        for j in js:
            split[i, j, c] = jnp.dot(value, w_ref[j], preferred_element_type=jnp.float32).astype(jnp.bfloat16)

            @pl.when(mine != c)
            def _():
                to_head(i, j, mine, c).start()

    def visit(step, c, js, arriving):
        for way in range(2):
            i = at - ways[way] * step

            @pl.when(inside(i))
            def _():
                if arriving:
                    copy(way, step - 1, c, False).wait_recv()

                    @pl.when(inside(at + ways[way]))
                    def _():
                        copy(way, step, c, False).start()

                unit(i, c, js, False)

    def total_of(i, j):
        total = split[i, j, mine].astype(jnp.float32)
        for k in range(1, heads):
            source = lax.rem(mine + k, heads)
            to_head(i, j, source, mine).wait_recv()
            total = total + got[i, j, source].astype(jnp.float32)
        return total.astype(jnp.bfloat16)

    def settle_own(j):
        landed[at * 2 + (side if j == 0 else 1 - side)] = total_of(at, j)

    def settle(step, js):
        for way in range(2):
            i = at - ways[way] * step

            @pl.when(inside(i))
            def _():
                for j in js:
                    summed[i, j] = total_of(i, j)
                    to_row(i, j, at).start()

    def each(function):
        lax.fori_loop(0, heads, lambda c, carry: (function(c), carry)[1], 0)

    def start_own(c):
        for way in range(2):

            @pl.when(inside(at + ways[way]))
            def _():
                copy(way, 0, c, True).start()

    def run():
        weights.wait()
        exchange = pltpu.make_async_remote_copy(
            src_ref=w_ref.at[0],
            dst_ref=w_ref.at[1],
            send_sem=wsend.at[0],
            recv_sem=wrecv.at[0],
            device_id={"seq": partner},
            device_id_type=MESH,
        )
        exchange.start()
        each(lambda c: unit(at, c, (0,), True))

        def first_steps(step, carry):
            each(lambda c: visit(step, c, (0,), True))

            @pl.when(step == 1)
            def _():
                settle_own(0)

            @pl.when(step > 1)
            def _():
                settle(step - 1, (0,))

            return carry

        lax.fori_loop(1, early + 1, first_steps, 0)
        exchange.wait()
        each(lambda c: unit(at, c, (1,), True))
        lax.fori_loop(1, early + 1, lambda t, carry: (each(lambda c: visit(t, c, (1,), False)), carry)[1], 0)
        settle(early, (0,))

        def settle_early():
            settle_own(1)
            lax.fori_loop(1, early + 1, lambda t, carry: (settle(t, (1,)), carry)[1], 0)

        def late_step(step, carry):
            def late_visit(c):
                visit(step, c, (0, 1), True)

                @pl.when(jnp.logical_and(c == 0, step == early + 1))
                def _():
                    settle_early()

                @pl.when(jnp.logical_and(c == 0, step > early + 1))
                def _():
                    settle(step - 1, (0, 1))

                @pl.when(jnp.logical_and(mine == c - 1, step == line - 1))
                def _():
                    settle(step, (0, 1))

            each(late_visit)
            return carry

        if line - 1 > early:
            lax.fori_loop(early + 1, line, late_step, 0)

            @pl.when(mine == heads - 1)
            def _():
                settle(line - 1, (0, 1))

        else:
            settle_early()

        for way in range(2):
            for step in range(2):

                def finish(c):
                    @pl.when(leaves(way, step))
                    def _():
                        copy(way, step, c, step == 0).wait_send()

                if step == 0:
                    each(finish)
                else:

                    def finish_rest(t, carry):
                        def one(c):
                            @pl.when(leaves(way, t))
                            def _():
                                copy(way, t, c, False).wait_send()

                        each(one)
                        return carry

                    lax.fori_loop(1, line, finish_rest, 0)

        def drain(i, carry):
            for j in range(2):
                for k in range(1, heads):
                    to_head(i, j, mine, lax.rem(mine + k, heads)).wait_send()

                @pl.when(i != at)
                def _():
                    to_row(i, j, at).wait_send()
                    to_row(at, j, i).wait_recv()

            return carry

        lax.fori_loop(0, line, drain, 0)
        for i in range(n):
            out_ref[:, i * columns : (i + 1) * columns] = landed[i]

    return start_own, each, run


def project_kernel(n, heads, *refs):
    start_own, each, run = project_stages(n, heads, False, *refs)
    each(start_own)
    run()


def join_kernel(n, heads, o_ref, lse_ref, w_hbm, out_ref, x_ref, *refs):
    start_own, _, run = project_stages(n, heads, True, x_ref, w_hbm, out_ref, *refs[8:])
    per_way = BLK * heads // x_ref.shape[0]

    def ready(way):
        for c in range(per_way):
            start_own(way * per_way + c)

    drain = reduce_kernel(n, True, o_ref, lse_ref, x_ref, *refs[:8], ready=ready)
    run()
    drain()


def project_plan(n, heads, rows, width, columns, dtype):
    share = rows // heads
    line = n // 2
    dma = pltpu.SemaphoreType.DMA
    scratch = [
        pltpu.VMEM((2, width, columns), dtype),
        pltpu.VMEM((line, rows, width), dtype),
        pltpu.VMEM((line, 2, heads, share, columns), dtype),
        pltpu.VMEM((line, 2, heads, share, columns), dtype),
        pltpu.VMEM((line, 2, share, columns), dtype),
        pltpu.VMEM((n, share, columns), dtype),
        dma((1,)),
        dma((1,)),
        dma((1,)),
        dma((2, line, heads)),
        dma((2, line, heads)),
        dma((line, 2, heads)),
        dma((line, 2, heads)),
        dma((line, 2)),
        dma((line, 2)),
    ]
    padded = max(columns, BLK)
    held = [
        ((2, width, padded), dtype),
        ((line + 2, rows, width), dtype),
        ((2, n, heads, share, padded), dtype),
        ((3, n, share, padded), dtype),
    ]
    return scratch, held


def reduce_plan(n, small, kv_here, group_width):
    heads_here = kv_here * (H // KVH)
    dma = pltpu.SemaphoreType.DMA((2, n - 1))
    dma_cuts = pltpu.SemaphoreType.DMA((2, n - 1, kv_here * CUTS))
    scratch = [
        pltpu.VMEM((2, n - 1, kv_here, BLK, group_width), jnp.bfloat16),
        pltpu.VMEM((2, n - 1, heads_here, BLK), jnp.float32),
        pltpu.VMEM((2, 2, 1 if small else kv_here, BLK, group_width), jnp.bfloat16),
        pltpu.SemaphoreType.DMA((2, 2)),
        dma_cuts,
        dma_cuts,
        dma,
        dma,
    ]
    held = [
        ((2, n + 1, kv_here, BLK, group_width), jnp.bfloat16),
        ((2, 2 * n - 1, heads_here, BLK), jnp.float32),
    ]
    return scratch, held


def mixed_from(parts, lse, weight, n, heads, rows, width, small):
    _, kv_here, _, group_width = parts.shape
    columns = weight.shape[1]
    vmem = pl.BlockSpec(memory_space=pltpu.VMEM)
    anywhere = pl.BlockSpec(memory_space=pl.ANY)
    reduce_scratch, reduce_held = reduce_plan(n, small, kv_here, group_width)
    project_scratch, project_held = project_plan(n, heads, rows, width, columns, parts.dtype)
    attended = jax.ShapeDtypeStruct((rows, width), parts.dtype)
    out = jax.ShapeDtypeStruct((rows // heads, n * columns), parts.dtype)

    def call(kernel, number, in_specs, out_shape, scratch, held):
        return pl.pallas_call(
            kernel,
            in_specs=in_specs,
            out_specs=vmem,
            out_shape=out_shape,
            scratch_shapes=scratch,
            compiler_params=pltpu.CompilerParams(
                collective_id=number, has_side_effects=True, vmem_limit_bytes=grant(*held)
            ),
            cost_estimate=long_cost(),
        )

    if small:
        scratch = [pltpu.VMEM((rows, width), parts.dtype)] + reduce_scratch + project_scratch
        held = reduce_held + project_held + [(parts.shape, parts.dtype)]
        kernel = functools.partial(join_kernel, n, heads)
        return call(kernel, 1, [vmem, vmem, anywhere], out, scratch, held)(parts, lse, weight)

    def kernel(*refs):
        reduce_kernel(n, small, *refs)

    x = call(kernel, 1, [anywhere, vmem], attended, reduce_scratch, reduce_held)(parts, lse)
    kernel = functools.partial(project_kernel, n, heads)
    return call(kernel, 2, [vmem, anywhere], out, project_scratch, project_held)(x, weight)


def body(
    queries,
    self_keys,
    self_values,
    store_keys,
    store_values,
    kv_slot,
    neighbours,
    counts,
    out_weight,
):
    n = lax.axis_size("seq")
    head_count = lax.axis_size("head")
    local_blocks, degree = neighbours.shape
    local_rows, width = queries.shape
    store_blocks = store_keys.shape[0] // BLK
    all_blocks = local_blocks * n
    kv_here = store_keys.shape[1] // DH
    group_width = (H // KVH) * DH
    rows = (H // KVH) * BLK
    small = queries.size * n * queries.dtype.itemsize <= 8 << 20
    count_row = counts.reshape(1, local_blocks)
    stores = (self_keys, self_values, store_keys, store_values)
    cut = tuple(a.reshape(store_blocks, BLK, -1) for a in stores[2:])
    smem = pl.BlockSpec(memory_space=pltpu.SMEM)
    vmem = pl.BlockSpec(memory_space=pltpu.VMEM)
    params = pltpu.CompilerParams(vmem_limit_bytes=28 << 20)
    cost = pl.CostEstimate(flops=2_000_000_000, bytes_accessed=12 << 20, transcendentals=4_000_000)
    scratch = [
        pltpu.SMEM((degree + 1,), jnp.int32),
        pltpu.VMEM((kv_here, DH, rows), jnp.float32),
        pltpu.VMEM((kv_here, rows), jnp.float32),
        pltpu.VMEM((kv_here, rows), jnp.float32),
    ]
    part_shape = (all_blocks, kv_here, BLK, group_width)
    lse_shape = (all_blocks, kv_here * (H // KVH), BLK)
    if small:
        all_queries, near, count, parts, lse = gathered(queries, neighbours, count_row, n, (kv_slot,) + stores[:2] + cut)
        parts, lse = pl.pallas_call(
            functools.partial(rest_kernel, local_blocks, store_blocks),
            in_specs=[smem] * 3 + [vmem] * 7,
            out_specs=[vmem, vmem],
            out_shape=[pltpu.VMEM(part_shape, jnp.bfloat16), pltpu.VMEM(lse_shape, jnp.float32)],
            scratch_shapes=scratch,
            input_output_aliases={8: 0, 9: 1},
            compiler_params=params,
            cost_estimate=cost,
        )(kv_slot, near, count, all_queries, *stores, parts, lse)
    else:
        all_queries, near, count = gathered(queries, neighbours, count_row, n, ())
        parts, lse = pl.pallas_call(
            functools.partial(part_kernel, local_blocks, store_blocks),
            grid=(all_blocks,),
            in_specs=[smem] * 3 + [pl.BlockSpec((BLK, width), lambda i: (i, 0))] + [vmem] * 4,
            out_specs=[
                pl.BlockSpec((1, kv_here, BLK, group_width), lambda i: (i, 0, 0, 0)),
                pl.BlockSpec((1, kv_here * (H // KVH), BLK), lambda i: (i, 0, 0)),
            ],
            out_shape=[
                jax.ShapeDtypeStruct(part_shape, jnp.bfloat16),
                jax.ShapeDtypeStruct(lse_shape, jnp.float32),
            ],
            scratch_shapes=scratch,
            compiler_params=params,
            cost_estimate=cost,
        )(kv_slot, near, count, all_queries, *stores)
    return mixed_from(parts, lse, out_weight, n, head_count, local_rows, width, small)


def solution(mesh):
    placed = (
        P("seq", "head"),
        P("seq", "head"),
        P("seq", "head"),
        P("seq", "head"),
        P("seq", "head"),
        P(),
        P("seq", None),
        P("seq"),
        P("head", "seq"),
    )
    return jax.shard_map(
        body, mesh=mesh, in_specs=placed, out_specs=P(("seq", "head"), None), check_vma=False
    )
```

```python
import functools

import jax
import jax.numpy as jnp
from jax import lax
from jax.experimental import pallas as pl
from jax.experimental.pallas import tpu as pltpu
from jax.sharding import PartitionSpec as P

H = 32
KVH = 8
DH = 128
BLK = 128
NEG = -1e30
SCAN = 4
AHEAD = 2
CUTS = 1
LOG2E = 1.4426950408889634
MESH = pl.DeviceIdType.MESH


def asked_rows(q_ref, first_row, g, per_group):
    return jnp.concatenate(
        [
            q_ref[pl.ds(first_row, BLK), (g * per_group + r) * DH : (g * per_group + r + 1) * DH]
            for r in range(per_group)
        ],
        axis=0,
    )


def scores_of(keys, asked):
    scaling = DH ** (-0.5) * LOG2E
    return lax.dot_general(keys, asked, (((1,), (1,)), ((), ())), preferred_element_type=jnp.float32) * scaling


def weighed(values, p):
    return lax.dot_general(
        values, p.astype(jnp.bfloat16), (((0,), (0,)), ((), ())), preferred_element_type=jnp.float32
    )


def causal_mask(rows):
    position = lax.rem(lax.broadcasted_iota(jnp.int32, (BLK, rows), 1), BLK)
    return position >= lax.broadcasted_iota(jnp.int32, (BLK, rows), 0)


def write_part(o_ref, lse_ref, here, g, acc, total, lse):
    per_group = lse.shape[1] // BLK
    o_ref[here, g] = (acc * (1.0 / total)).astype(jnp.bfloat16)
    for r in range(per_group):
        head = g * per_group + r
        lse_ref[here, head : head + 1] = lse[:, r * BLK : (r + 1) * BLK]


def part_row(
    block,
    here,
    first_row,
    done,
    local_blocks,
    store_blocks,
    slot_ref,
    near_ref,
    count_ref,
    q_ref,
    sk_ref,
    sv_ref,
    k_ref,
    v_ref,
    o_ref,
    lse_ref,
    list_ref,
    acc_ref,
    max_ref,
    sum_ref,
):
    owner, inner = lax.div(block, local_blocks), lax.rem(block, local_blocks)
    me = lax.axis_index("seq")
    per_group = H // KVH
    kv_here = k_ref.shape[1] // DH
    rows = per_group * BLK
    listed = count_ref[owner, 0, inner]
    first_slot = me * store_blocks

    def scan_entries(i, found):
        places = [slot_ref[near_ref[owner, inner, i * SCAN + u]] - first_slot for u in range(SCAN)]
        for u, place in enumerate(places):
            list_ref[found] = place
            kept = (place >= 0) & (place < store_blocks) & (i * SCAN + u < listed)
            found = found + kept.astype(jnp.int32)
        return found

    found = lax.fori_loop(0, lax.div(listed + (SCAN - 1), SCAN), scan_entries, jnp.int32(0))
    home = owner == me
    if not done:

        @pl.when(jnp.logical_and(found == 0, jnp.logical_not(home)))
        def _():
            o_ref[here] = jnp.zeros(o_ref.shape[1:], o_ref.dtype)
            lse_ref[here] = jnp.full(lse_ref.shape[1:], NEG, lse_ref.dtype)

    @pl.when(found > done if done else jnp.logical_or(found > 0, home))
    def _():
        if done:
            for g in range(kv_here):
                max_ref[g : g + 1] = jnp.concatenate(
                    [
                        lse_ref[here, head : head + 1]
                        for head in range(g * per_group, (g + 1) * per_group)
                    ],
                    axis=1,
                )
                sum_ref[g : g + 1] = jnp.ones((1, rows), jnp.float32)
                acc_ref[g] = o_ref[here, g].astype(jnp.float32)
        else:

            @pl.when(home)
            def _():
                start = pl.multiple_of(inner * BLK, BLK)
                for g in range(kv_here):
                    cols = slice(g * DH, (g + 1) * DH)
                    asked = asked_rows(q_ref, first_row, g, per_group)
                    s = jnp.where(causal_mask(rows), scores_of(sk_ref[pl.ds(start, BLK), cols], asked), NEG)
                    m = jnp.max(s, axis=0, keepdims=True)
                    p = jnp.exp2(s - m)
                    max_ref[g : g + 1] = m
                    sum_ref[g : g + 1] = jnp.sum(p, axis=0, keepdims=True)
                    acc_ref[g] = weighed(sv_ref[pl.ds(start, BLK), cols], p)

            @pl.when(jnp.logical_not(home))
            def _():
                max_ref[...] = jnp.full_like(max_ref, NEG)
                sum_ref[...] = jnp.zeros_like(sum_ref)
                acc_ref[...] = jnp.zeros_like(acc_ref)

        def take(*places):
            starts = [pl.multiple_of(place * BLK, BLK) for place in places]

            def rows_of(ref, cols):
                return jnp.concatenate([ref[pl.ds(start, BLK), cols] for start in starts], axis=0)

            for g in range(kv_here):
                cols = slice(g * DH, (g + 1) * DH)
                s = scores_of(rows_of(k_ref, cols), asked_rows(q_ref, first_row, g, per_group))
                old = max_ref[g : g + 1]
                new = jnp.maximum(old, jnp.max(s, axis=0, keepdims=True))
                p = jnp.exp2(s - new)
                shrink = jnp.exp2(old - new)
                max_ref[g : g + 1] = new
                sum_ref[g : g + 1] = sum_ref[g : g + 1] * shrink + jnp.sum(p, axis=0, keepdims=True)
                acc_ref[g] = acc_ref[g] * shrink + weighed(rows_of(v_ref, cols), p)

        left = found - done

        @pl.loop(0, lax.div(left, 2))
        def _(i):
            take(list_ref[done + 2 * i], list_ref[done + 2 * i + 1])

        @pl.when(lax.rem(left, 2) == 1)
        def _():
            take(list_ref[found - 1])

        for g in range(kv_here):
            total = sum_ref[g : g + 1]
            write_part(o_ref, lse_ref, here, g, acc_ref[g], total, max_ref[g : g + 1] + jnp.log2(total))


def part_kernel(local_blocks, store_blocks, *refs):
    block = pl.program_id(0)
    part_row(block, 0, 0, 0, local_blocks, store_blocks, *refs)


def rest_kernel(local_blocks, store_blocks, *refs):
    def row(block, carry):
        first_row = pl.multiple_of(block * BLK, BLK)
        part_row(block, block, first_row, AHEAD, local_blocks, store_blocks, *refs[:8], *refs[10:])
        return carry

    lax.fori_loop(0, refs[10].shape[0], row, 0)


def grant(*arrays):
    size = 0
    for shape, dtype in arrays:
        cells = 1
        for d in shape:
            cells = cells * d
        size += cells * jnp.dtype(dtype).itemsize
    return min(size + (4 << 20), 60 << 20)


def long_cost():
    return pl.CostEstimate(flops=200_000_000_000, bytes_accessed=1 << 20, transcendentals=0)


def ring_place(index, n):
    odd = lax.rem(index, 2)
    half = index // 2
    return (1 - odd) * half + odd * (n - 1 - half)


def ring_index(place, n):
    place = lax.rem(place + 2 * n, n)
    far = place // (n // 2)
    return (1 - far) * (2 * place) + far * (2 * (n - 1 - place) + 1)


def gather_kernel(n, pieces, early, *refs):
    refs = list(refs)

    def some(count):
        return [refs.pop(0) for _ in range(count)]

    x_ref, near_ref, count_ref = some(3)
    if early:
        slot_hbm, *store_hbm = some(5)
    out_ref, nears_ref, counts_ref = some(3)
    if early:
        o_ref, lse_ref, slot_ref, near_smem, count_smem, sk_ref, sv_ref, k_ref, v_ref, load_sem = some(10)
    own_sem, send_sem, recv_sem, tsend_sem, trecv_sem = refs
    me = lax.axis_index("seq")
    place = ring_place(me, n)
    rows = x_ref.shape[0]
    sub = rows // pieces
    half = n // 2
    ways = (1, -1)
    beside = [ring_index(place + way, n) for way in ways]
    own = [
        pltpu.make_async_copy(source, target, own_sem.at[i])
        for i, (source, target) in enumerate(
            (
                (x_ref, out_ref.at[pl.ds(pl.multiple_of(me * rows, rows), rows)]),
                (near_ref, nears_ref.at[me]),
                (count_ref, counts_ref.at[me]),
            )
        )
    ]
    for one in own:
        one.start()
    loads = []
    if early:
        sources = [slot_hbm] + store_hbm
        for i, (source, target) in enumerate(zip(sources, (slot_ref, sk_ref, sv_ref, k_ref, v_ref))):
            loads.append(pltpu.make_async_copy(source, target, load_sem.at[i]))
    for one in loads:
        one.start()
    barrier = pltpu.get_barrier_semaphore()
    for k in range(1, n):
        pl.semaphore_signal(barrier, inc=1, device_id={"seq": lax.rem(me + k, n)}, device_id_type=MESH)
    for one in own:
        one.wait()
    pl.semaphore_wait(barrier, n - 1)

    def copy(way, step, piece):
        owner = ring_index(place - ways[way] * step, n)
        there = pl.ds(pl.multiple_of(owner * rows + piece * sub, sub), sub)
        return pltpu.make_async_remote_copy(
            src_ref=out_ref.at[there],
            dst_ref=out_ref.at[there],
            send_sem=send_sem.at[way, step, piece],
            recv_sem=recv_sem.at[way, step, piece],
            device_id={"seq": beside[way]},
            device_id_type=MESH,
        )

    def piece_of(way, spot):
        return spot if way == 0 else pieces - 1 - spot

    table_copies = []
    for t, target in enumerate((nears_ref, counts_ref)):
        for k in range(1, n):
            table_copies.append(
                pltpu.make_async_remote_copy(
                    src_ref=target.at[me],
                    dst_ref=target.at[me],
                    send_sem=tsend_sem.at[t, k],
                    recv_sem=trecv_sem.at[t, k],
                    device_id={"seq": lax.rem(me + k, n)},
                    device_id_type=MESH,
                )
            )
    for one in table_copies:
        one.start()
    started = []
    for spot in range(pieces):
        for way in range(2):
            one = copy(way, 0, piece_of(way, spot))
            one.start()
            started.append(one)

    def first_listed(owner, inner):
        degree = near_ref.shape[1]
        store_blocks = k_ref.shape[0]
        listed = count_smem[owner, 0, inner]

        def look_past(before):
            def look(i, best):
                e = degree - SCAN * (i + 1)
                for u in range(SCAN - 1, -1, -1):
                    spot = slot_ref[near_smem[owner, inner, e + u]] - me * store_blocks
                    kept = (spot >= 0) & (spot < store_blocks) & (e + u < listed)
                    for other in before:
                        kept = kept & (spot != other)
                    best = best + kept.astype(jnp.int32) * (spot - best)
                return best

            return lax.fori_loop(0, degree // SCAN, look, jnp.int32(-1))

        found = []
        for _ in range(AHEAD):
            found.append(look_past(found))
        return found

    def row_work(owner, inner, spots, mine):
        per_group = H // KVH
        taken = [jnp.maximum(spot, 0) for spot in spots]
        missing = [jnp.minimum(spot, 0).astype(jnp.float32) * -NEG for spot in spots]
        first_row = pl.multiple_of(owner * rows + inner * BLK, BLK)
        for g in range(k_ref.shape[2] // DH):
            cols = slice(g * DH, (g + 1) * DH)
            asked = asked_rows(out_ref, first_row, g, per_group)
            keys = [k_ref[i, :, cols] for i in taken]
            values = [v_ref[i, :, cols] for i in taken]
            if mine:
                near = pl.ds(pl.multiple_of(inner * BLK, BLK), BLK)
                keys = [sk_ref[near, cols]] + keys
                values = [sv_ref[near, cols]] + values
            s = scores_of(jnp.concatenate(keys, axis=0), asked)
            cuts = [s[i * BLK : (i + 1) * BLK] for i in range(len(keys))]
            for i, lack in enumerate(missing):
                if mine or i > 0:
                    at = i + 1 if mine else i
                    cuts[at] = cuts[at] + lack
            if mine:
                cuts[0] = jnp.where(causal_mask(s.shape[1]), cuts[0], NEG)
            s = jnp.concatenate(cuts, axis=0)
            m = jnp.max(s, axis=0, keepdims=True)
            p = jnp.exp2(s - m)
            total = jnp.sum(p, axis=0, keepdims=True)
            lse = m + jnp.log2(total)
            if not mine:
                lse = lse + missing[0]
            write_part(
                o_ref, lse_ref, owner * pieces + inner, g, weighed(jnp.concatenate(values, axis=0), p), total, lse
            )

    def row_at(way, step, spot):
        return ring_index(place - ways[way] * step, n), piece_of(way, spot)

    def scanned(step, spot):
        return [first_listed(*row_at(way, step, spot)) for way in range(2)] if early else None

    def arrived(step, spot, found):
        if early:
            for way in range(2):
                row_work(*row_at(way, step, spot), found[way], False)

    def own_rows():
        for one in table_copies:
            one.wait_recv()
        tables = [
            pltpu.make_async_copy(source, target, load_sem.at[5 + i])
            for i, (source, target) in enumerate(((nears_ref, near_smem), (counts_ref, count_smem)))
        ]
        for one in tables:
            one.start()
        for one in loads + tables:
            one.wait()
        for inner in range(pieces):
            row_work(me, inner, first_listed(me, inner), True)

    for step in range(1, half):
        for spot in range(pieces):
            first = step == 1 and spot == 0
            found = None if first else scanned(step, spot)
            for way in range(2):
                copy(way, step - 1, piece_of(way, spot)).wait_recv()
                if step < half - 1 or spot < pieces // 2:
                    one = copy(way, step, piece_of(way, spot))
                    one.start()
                    started.append(one)
            if early and first:
                own_rows()
                found = scanned(step, spot)
            arrived(step, spot, found)
    for spot in range(pieces // 2):
        found = scanned(half, spot)
        for way in range(2):
            copy(way, half - 1, piece_of(way, spot)).wait_recv()
        arrived(half, spot, found)
    for one in started:
        one.wait_send()
    for one in table_copies:
        if early:
            one.wait_send()
        else:
            one.wait()


def gathered(x, near, count, n, early):
    rows, width = x.shape
    pieces = rows // BLK
    vmem = pl.BlockSpec(memory_space=pltpu.VMEM)
    dma = pltpu.SemaphoreType.DMA
    kind = pltpu.VMEM if early else jax.ShapeDtypeStruct
    inputs = [x, near, count] + list(early)
    out_shape = [
        kind((n * rows, width), x.dtype),
        jax.ShapeDtypeStruct((n,) + near.shape, near.dtype),
        jax.ShapeDtypeStruct((n,) + count.shape, count.dtype),
    ]
    scratch = []
    held = [((n + 1, rows, width), x.dtype)]
    if early:
        slot, *stores = early
        kv_here = stores[2].shape[2] // DH
        part_shape = (n * pieces, kv_here, BLK, (H // KVH) * DH)
        out_shape += [kind(part_shape, x.dtype), kind((n * pieces, kv_here * (H // KVH), BLK), jnp.float32)]
        scratch += [pltpu.SMEM(slot.shape, slot.dtype)]
        scratch += [pltpu.SMEM(out_shape[1].shape, near.dtype), pltpu.SMEM(out_shape[2].shape, count.dtype)]
        scratch += [pltpu.VMEM(a.shape, a.dtype) for a in stores]
        scratch += [dma((7,))]
        held += [(part_shape, x.dtype)] + [(a.shape, a.dtype) for a in stores]
    scratch += [
        dma((3,)),
        dma((2, n // 2, pieces)),
        dma((2, n // 2, pieces)),
        dma((2, n)),
        dma((2, n)),
    ]
    return pl.pallas_call(
        functools.partial(gather_kernel, n, pieces, bool(early)),
        in_specs=[pl.BlockSpec(memory_space=pltpu.HBM)] * len(inputs),
        out_specs=[vmem] * len(out_shape),
        out_shape=out_shape,
        scratch_shapes=scratch,
        compiler_params=pltpu.CompilerParams(
            collective_id=0,
            has_side_effects=True,
            vmem_limit_bytes=grant(*held),
        ),
        cost_estimate=long_cost(),
    )(*(pltpu.with_memory_space_constraint(a, pltpu.HBM) for a in inputs))


def merge(lse_a, lse_b):
    top = jnp.maximum(lse_a, lse_b)
    a = jnp.exp2(lse_a - top)
    b = jnp.exp2(lse_b - top)
    total = a + b
    return a / total, b / total, top + jnp.log2(total)


def reduce_kernel(
    n,
    small,
    o_ref,
    lse_ref,
    out_ref,
    got,
    got_lse,
    own,
    own_sem,
    send_sem,
    recv_sem,
    lsend_sem,
    lrecv_sem,
    ready=None,
):
    me = lax.axis_index("seq")
    place = ring_place(me, n)
    groups, width = got.shape[2], got.shape[4]
    wide = width // CUTS
    ways = (1, -1)
    beside = [ring_index(place + way, n) for way in ways]
    if ready is None:
        barrier = pltpu.get_barrier_semaphore()
        for other in beside:
            pl.semaphore_signal(barrier, inc=1, device_id={"seq": other}, device_id_type=MESH)

    def home(way, step):
        return ring_index(place - ways[way] * (1 + step), n)

    def fetch(way, step):
        return pltpu.make_async_copy(
            o_ref.at[home(way, step) * 2 + way], own.at[way, lax.rem(step, 2)], own_sem.at[way, lax.rem(step, 2)]
        )

    def lse_copy(way, step, before):
        return pltpu.make_async_remote_copy(
            src_ref=lse_ref.at[home(way, step) * 2 + way] if before is None else got_lse.at[way, before],
            dst_ref=got_lse.at[way, step],
            send_sem=lsend_sem.at[way, step],
            recv_sem=lrecv_sem.at[way, step],
            device_id={"seq": beside[way]},
            device_id_type=MESH,
        )

    def copy(way, step, g, cut, before):
        part = (g, slice(None), pl.ds(cut * wide, wide))
        return pltpu.make_async_remote_copy(
            src_ref=o_ref.at[(home(way, step) * 2 + way,) + part]
            if before is None
            else got.at[(way, before) + part],
            dst_ref=got.at[(way, step) + part],
            send_sem=send_sem.at[way, step, g * CUTS + cut],
            recv_sem=recv_sem.at[way, step, g * CUTS + cut],
            device_id={"seq": beside[way]},
            device_id_type=MESH,
        )

    def shares_of(way, step):
        lse_copy(way, step - 1, step - 1).wait_recv()
        if not small:
            fetch(way, step).wait()
        return merge(got_lse[way, step - 1], lse_ref[home(way, step) * 2 + way])

    def merged(way, step, g, cut, theirs, ours):
        copy(way, step - 1, g, cut, step - 1).wait_recv()
        at = home(way, step) * 2 + way
        columns = []
        for r in range(cut * wide // DH, (cut + 1) * wide // DH):
            cols = slice(r * DH, (r + 1) * DH)
            head = g * (width // DH) + r
            mine = o_ref[at, g, :, cols] if small else own[way, lax.rem(step, 2), g, :, cols]
            value = (
                got[way, step - 1, g, :, cols].astype(jnp.float32) * theirs[head : head + 1]
                + mine.astype(jnp.float32) * ours[head : head + 1]
            )
            columns.append((r, value))
        return columns

    if not small:
        for way in range(2):
            fetch(way, 1).start()
    if ready is None:
        pl.semaphore_wait(barrier, 2)
    for way in range(2):
        lse_copy(way, 0, None).start()
    for g in range(groups):
        for cut in range(CUTS):
            for way in range(2):
                copy(way, 0, g, cut, None).start()

    def one_step(step, carry):
        if not small:
            for way in range(2):
                fetch(way, step + 1).start()
        shares = []
        for way in range(2):
            theirs, ours, lse = shares_of(way, step)
            got_lse[way, step - 1] = lse
            lse_copy(way, step, step - 1).start()
            shares.append((theirs, ours))
        for g in range(groups):
            for cut in range(CUTS):
                for way in range(2):
                    for r, value in merged(way, step, g, cut, *shares[way]):
                        got[way, step - 1, g, :, r * DH : (r + 1) * DH] = value.astype(jnp.bfloat16)
                    copy(way, step, g, cut, step - 1).start()
        return carry

    lax.fori_loop(1, n - 1, one_step, 0)
    for way in range(2):
        theirs, ours, _ = shares_of(way, n - 1)
        for g in range(groups):
            for cut in range(CUTS):
                for r, value in merged(way, n - 1, g, cut, theirs, ours):
                    at = g * width + r * DH
                    out_ref[way * BLK : (way + 1) * BLK, at : at + DH] = jnp.transpose(value).astype(jnp.bfloat16)
        if ready is not None:
            ready(way)

    def drain_all():
        def drain(step, before):
            for way in range(2):
                lse_copy(way, step, before).wait_send()
                for g in range(groups):
                    for cut in range(CUTS):
                        copy(way, step, g, cut, before).wait_send()

        drain(0, None)
        lax.fori_loop(1, n - 1, lambda step, carry: (drain(step, step - 1), carry)[1], 0)

    if ready is None:
        drain_all()
    return drain_all


def project_stages(
    n,
    heads,
    joined,
    x_ref,
    w_hbm,
    out_ref,
    w_ref,
    blocks,
    split,
    got,
    summed,
    landed,
    w_sem,
    wsend,
    wrecv,
    send_sem,
    recv_sem,
    hsend,
    hrecv,
    fsend,
    frecv,
):
    me = lax.axis_index("seq")
    mine = lax.axis_index("head")
    line = n // 2
    at, side = me // 2, lax.rem(me, 2)
    share = x_ref.shape[0] // heads
    columns = w_ref.shape[2]
    ways = (1, -1)
    early = min(2, line - 1)
    weights = pltpu.make_async_copy(w_hbm, w_ref.at[0], w_sem.at[0])
    weights.start()
    barrier = pltpu.get_barrier_semaphore()
    place = ring_place(me, n)
    for way in ways:
        other = ring_index(place + way, n)
        pl.semaphore_signal(barrier, inc=1, device_id={"seq": other}, device_id_type=MESH)
    for k in range(1, heads):
        pl.semaphore_signal(barrier, inc=1, device_id={"head": lax.rem(mine + k, heads)}, device_id_type=MESH)
    partner = at * 2 + 1 - side
    if not joined:
        for k in range(1, line):
            other = lax.rem(at + k, line) * 2 + side
            pl.semaphore_signal(barrier, inc=1, device_id={"seq": other}, device_id_type=MESH)
        pl.semaphore_signal(barrier, inc=1, device_id={"seq": partner}, device_id_type=MESH)
    pl.semaphore_wait(barrier, heads + 1 if joined else heads + line + 1)

    def inside(spot):
        return jnp.logical_and(spot >= 0, spot < line)

    def copy(way, step, piece, first):
        there = (at - ways[way] * step, pl.ds(pl.multiple_of(piece * share, share), share))
        return pltpu.make_async_remote_copy(
            src_ref=x_ref.at[there[1]] if first else blocks.at[there],
            dst_ref=blocks.at[there],
            send_sem=send_sem.at[way, step, piece],
            recv_sem=recv_sem.at[way, step, piece],
            device_id={"seq": (at + ways[way]) * 2 + side},
            device_id_type=MESH,
        )

    def leaves(way, step):
        return jnp.logical_and(inside(at - ways[way] * step), inside(at + ways[way]))

    def to_head(i, j, source, to):
        return pltpu.make_async_remote_copy(
            src_ref=split.at[i, j, to],
            dst_ref=got.at[i, j, source],
            send_sem=hsend.at[i, j, to],
            recv_sem=hrecv.at[i, j, source],
            device_id={"head": to},
            device_id_type=MESH,
        )

    def to_row(i, j, source):
        owner = source * 2 + (side if j == 0 else 1 - side)
        return pltpu.make_async_remote_copy(
            src_ref=summed.at[i, j],
            dst_ref=landed.at[owner],
            send_sem=fsend.at[i, j],
            recv_sem=frecv.at[source, j],
            device_id={"seq": i * 2 + side},
            device_id_type=MESH,
        )

    def unit(i, c, js, own):
        rows = pl.ds(pl.multiple_of(c * share, share), share)
        value = x_ref[rows] if own else blocks[i, rows]
        for j in js:
            split[i, j, c] = jnp.dot(value, w_ref[j], preferred_element_type=jnp.float32).astype(jnp.bfloat16)

            @pl.when(mine != c)
            def _():
                to_head(i, j, mine, c).start()

    def visit(step, c, js, arriving):
        for way in range(2):
            i = at - ways[way] * step

            @pl.when(inside(i))
            def _():
                if arriving:
                    copy(way, step - 1, c, False).wait_recv()

                    @pl.when(inside(at + ways[way]))
                    def _():
                        copy(way, step, c, False).start()

                unit(i, c, js, False)

    def total_of(i, j):
        total = split[i, j, mine].astype(jnp.float32)
        for k in range(1, heads):
            source = lax.rem(mine + k, heads)
            to_head(i, j, source, mine).wait_recv()
            total = total + got[i, j, source].astype(jnp.float32)
        return total.astype(jnp.bfloat16)

    def settle_own(j):
        landed[at * 2 + (side if j == 0 else 1 - side)] = total_of(at, j)

    def settle(step, js):
        for way in range(2):
            i = at - ways[way] * step

            @pl.when(inside(i))
            def _():
                for j in js:
                    summed[i, j] = total_of(i, j)
                    to_row(i, j, at).start()

    def each(function):
        lax.fori_loop(0, heads, lambda c, carry: (function(c), carry)[1], 0)

    def start_own(c):
        for way in range(2):

            @pl.when(inside(at + ways[way]))
            def _():
                copy(way, 0, c, True).start()

    def run():
        weights.wait()
        exchange = pltpu.make_async_remote_copy(
            src_ref=w_ref.at[0],
            dst_ref=w_ref.at[1],
            send_sem=wsend.at[0],
            recv_sem=wrecv.at[0],
            device_id={"seq": partner},
            device_id_type=MESH,
        )
        exchange.start()
        each(lambda c: unit(at, c, (0,), True))

        def first_steps(step, carry):
            each(lambda c: visit(step, c, (0,), True))

            @pl.when(step == 1)
            def _():
                settle_own(0)

            @pl.when(step > 1)
            def _():
                settle(step - 1, (0,))

            return carry

        lax.fori_loop(1, early + 1, first_steps, 0)
        exchange.wait()
        each(lambda c: unit(at, c, (1,), True))
        lax.fori_loop(1, early + 1, lambda t, carry: (each(lambda c: visit(t, c, (1,), False)), carry)[1], 0)
        settle(early, (0,))

        def settle_early():
            settle_own(1)
            lax.fori_loop(1, early + 1, lambda t, carry: (settle(t, (1,)), carry)[1], 0)

        def late_step(step, carry):
            def late_visit(c):
                visit(step, c, (0, 1), True)

                @pl.when(jnp.logical_and(c == 0, step == early + 1))
                def _():
                    settle_early()

                @pl.when(jnp.logical_and(c == 0, step > early + 1))
                def _():
                    settle(step - 1, (0, 1))

                @pl.when(jnp.logical_and(mine == c - 1, step == line - 1))
                def _():
                    settle(step, (0, 1))

            each(late_visit)
            return carry

        if line - 1 > early:
            lax.fori_loop(early + 1, line, late_step, 0)

            @pl.when(mine == heads - 1)
            def _():
                settle(line - 1, (0, 1))

        else:
            settle_early()

        for way in range(2):
            for step in range(2):

                def finish(c):
                    @pl.when(leaves(way, step))
                    def _():
                        copy(way, step, c, step == 0).wait_send()

                if step == 0:
                    each(finish)
                else:

                    def finish_rest(t, carry):
                        def one(c):
                            @pl.when(leaves(way, t))
                            def _():
                                copy(way, t, c, False).wait_send()

                        each(one)
                        return carry

                    lax.fori_loop(1, line, finish_rest, 0)

        def drain(i, carry):
            for j in range(2):
                for k in range(1, heads):
                    to_head(i, j, mine, lax.rem(mine + k, heads)).wait_send()

                @pl.when(i != at)
                def _():
                    to_row(i, j, at).wait_send()
                    to_row(at, j, i).wait_recv()

            return carry

        lax.fori_loop(0, line, drain, 0)
        for i in range(n):
            out_ref[:, i * columns : (i + 1) * columns] = landed[i]

    return start_own, each, run


def project_kernel(n, heads, *refs):
    start_own, each, run = project_stages(n, heads, False, *refs)
    each(start_own)
    run()


def join_kernel(n, heads, o_ref, lse_ref, w_hbm, out_ref, x_ref, *refs):
    start_own, _, run = project_stages(n, heads, True, x_ref, w_hbm, out_ref, *refs[8:])
    per_way = BLK * heads // x_ref.shape[0]

    def ready(way):
        for c in range(per_way):
            start_own(way * per_way + c)

    drain = reduce_kernel(n, True, o_ref, lse_ref, x_ref, *refs[:8], ready=ready)
    run()
    drain()


def project_plan(n, heads, rows, width, columns, dtype):
    share = rows // heads
    line = n // 2
    dma = pltpu.SemaphoreType.DMA
    scratch = [
        pltpu.VMEM((2, width, columns), dtype),
        pltpu.VMEM((line, rows, width), dtype),
        pltpu.VMEM((line, 2, heads, share, columns), dtype),
        pltpu.VMEM((line, 2, heads, share, columns), dtype),
        pltpu.VMEM((line, 2, share, columns), dtype),
        pltpu.VMEM((n, share, columns), dtype),
        dma((1,)),
        dma((1,)),
        dma((1,)),
        dma((2, line, heads)),
        dma((2, line, heads)),
        dma((line, 2, heads)),
        dma((line, 2, heads)),
        dma((line, 2)),
        dma((line, 2)),
    ]
    padded = max(columns, BLK)
    held = [
        ((2, width, padded), dtype),
        ((line + 2, rows, width), dtype),
        ((2, n, heads, share, padded), dtype),
        ((3, n, share, padded), dtype),
    ]
    return scratch, held


def reduce_plan(n, small, kv_here, group_width):
    heads_here = kv_here * (H // KVH)
    dma = pltpu.SemaphoreType.DMA((2, n - 1))
    dma_cuts = pltpu.SemaphoreType.DMA((2, n - 1, kv_here * CUTS))
    scratch = [
        pltpu.VMEM((2, n - 1, kv_here, BLK, group_width), jnp.bfloat16),
        pltpu.VMEM((2, n - 1, heads_here, BLK), jnp.float32),
        pltpu.VMEM((2, 2, 1 if small else kv_here, BLK, group_width), jnp.bfloat16),
        pltpu.SemaphoreType.DMA((2, 2)),
        dma_cuts,
        dma_cuts,
        dma,
        dma,
    ]
    held = [
        ((2, n + 1, kv_here, BLK, group_width), jnp.bfloat16),
        ((2, 2 * n - 1, heads_here, BLK), jnp.float32),
    ]
    return scratch, held


def mixed_from(parts, lse, weight, n, heads, rows, width, small):
    _, kv_here, _, group_width = parts.shape
    columns = weight.shape[1]
    vmem = pl.BlockSpec(memory_space=pltpu.VMEM)
    anywhere = pl.BlockSpec(memory_space=pl.ANY)
    reduce_scratch, reduce_held = reduce_plan(n, small, kv_here, group_width)
    project_scratch, project_held = project_plan(n, heads, rows, width, columns, parts.dtype)
    attended = jax.ShapeDtypeStruct((rows, width), parts.dtype)
    out = jax.ShapeDtypeStruct((rows // heads, n * columns), parts.dtype)

    def call(kernel, number, in_specs, out_shape, scratch, held):
        return pl.pallas_call(
            kernel,
            in_specs=in_specs,
            out_specs=vmem,
            out_shape=out_shape,
            scratch_shapes=scratch,
            compiler_params=pltpu.CompilerParams(
                collective_id=number, has_side_effects=True, vmem_limit_bytes=grant(*held)
            ),
            cost_estimate=long_cost(),
        )

    if small:
        scratch = [pltpu.VMEM((rows, width), parts.dtype)] + reduce_scratch + project_scratch
        held = reduce_held + project_held + [(parts.shape, parts.dtype)]
        kernel = functools.partial(join_kernel, n, heads)
        return call(kernel, 1, [vmem, vmem, anywhere], out, scratch, held)(parts, lse, weight)

    def kernel(*refs):
        reduce_kernel(n, small, *refs)

    x = call(kernel, 1, [anywhere, vmem], attended, reduce_scratch, reduce_held)(parts, lse)
    kernel = functools.partial(project_kernel, n, heads)
    return call(kernel, 2, [vmem, anywhere], out, project_scratch, project_held)(x, weight)


def body(
    queries,
    self_keys,
    self_values,
    store_keys,
    store_values,
    kv_slot,
    neighbours,
    counts,
    out_weight,
):
    n = lax.axis_size("seq")
    head_count = lax.axis_size("head")
    local_blocks, degree = neighbours.shape
    local_rows, width = queries.shape
    store_blocks = store_keys.shape[0] // BLK
    all_blocks = local_blocks * n
    kv_here = store_keys.shape[1] // DH
    group_width = (H // KVH) * DH
    rows = (H // KVH) * BLK
    small = queries.size * n * queries.dtype.itemsize <= 8 << 20
    count_row = counts.reshape(1, local_blocks)
    stores = (self_keys, self_values, store_keys, store_values)
    cut = tuple(a.reshape(store_blocks, BLK, -1) for a in stores[2:])
    smem = pl.BlockSpec(memory_space=pltpu.SMEM)
    vmem = pl.BlockSpec(memory_space=pltpu.VMEM)
    params = pltpu.CompilerParams(vmem_limit_bytes=28 << 20)
    cost = pl.CostEstimate(flops=2_000_000_000, bytes_accessed=12 << 20, transcendentals=4_000_000)
    scratch = [
        pltpu.SMEM((degree + 1,), jnp.int32),
        pltpu.VMEM((kv_here, DH, rows), jnp.float32),
        pltpu.VMEM((kv_here, rows), jnp.float32),
        pltpu.VMEM((kv_here, rows), jnp.float32),
    ]
    part_shape = (all_blocks, kv_here, BLK, group_width)
    lse_shape = (all_blocks, kv_here * (H // KVH), BLK)
    if small:
        all_queries, near, count, parts, lse = gathered(queries, neighbours, count_row, n, (kv_slot,) + stores[:2] + cut)
        parts, lse = pl.pallas_call(
            functools.partial(rest_kernel, local_blocks, store_blocks),
            in_specs=[smem] * 3 + [vmem] * 7,
            out_specs=[vmem, vmem],
            out_shape=[pltpu.VMEM(part_shape, jnp.bfloat16), pltpu.VMEM(lse_shape, jnp.float32)],
            scratch_shapes=scratch,
            input_output_aliases={8: 0, 9: 1},
            compiler_params=params,
            cost_estimate=cost,
        )(kv_slot, near, count, all_queries, *stores, parts, lse)
    else:
        all_queries, near, count = gathered(queries, neighbours, count_row, n, ())
        parts, lse = pl.pallas_call(
            functools.partial(part_kernel, local_blocks, store_blocks),
            grid=(all_blocks,),
            in_specs=[smem] * 3 + [pl.BlockSpec((BLK, width), lambda i: (i, 0))] + [vmem] * 4,
            out_specs=[
                pl.BlockSpec((1, kv_here, BLK, group_width), lambda i: (i, 0, 0, 0)),
                pl.BlockSpec((1, kv_here * (H // KVH), BLK), lambda i: (i, 0, 0)),
            ],
            out_shape=[
                jax.ShapeDtypeStruct(part_shape, jnp.bfloat16),
                jax.ShapeDtypeStruct(lse_shape, jnp.float32),
            ],
            scratch_shapes=scratch,
            compiler_params=params,
            cost_estimate=cost,
        )(kv_slot, near, count, all_queries, *stores)
    return mixed_from(parts, lse, out_weight, n, head_count, local_rows, width, small)


def solution(mesh):
    placed = (
        P("seq", "head"),
        P("seq", "head"),
        P("seq", "head"),
        P("seq", "head"),
        P("seq", "head"),
        P(),
        P("seq", None),
        P("seq"),
        P("head", "seq"),
    )
    return jax.shard_map(
        body, mesh=mesh, in_specs=placed, out_specs=P(("seq", "head"), None), check_vma=False
    )
```

```python
import functools

import jax
import jax.numpy as jnp
from jax import lax
from jax.experimental import pallas as pl
from jax.experimental.pallas import tpu as pltpu
from jax.sharding import PartitionSpec as P

H = 32
KVH = 8
DH = 128
BLK = 128
NEG = -1e30
SCAN = 4
AHEAD = 2
CUTS = 1
LOG2E = 1.4426950408889634
MESH = pl.DeviceIdType.MESH


def asked_rows(q_ref, first_row, g, per_group):
    return jnp.concatenate(
        [
            q_ref[pl.ds(first_row, BLK), (g * per_group + r) * DH : (g * per_group + r + 1) * DH]
            for r in range(per_group)
        ],
        axis=0,
    )


def scores_of(keys, asked):
    scaling = DH ** (-0.5) * LOG2E
    return lax.dot_general(keys, asked, (((1,), (1,)), ((), ())), preferred_element_type=jnp.float32) * scaling


def weighed(values, p):
    return lax.dot_general(
        values, p.astype(jnp.bfloat16), (((0,), (0,)), ((), ())), preferred_element_type=jnp.float32
    )


def causal_mask(rows):
    position = lax.rem(lax.broadcasted_iota(jnp.int32, (BLK, rows), 1), BLK)
    return position >= lax.broadcasted_iota(jnp.int32, (BLK, rows), 0)


def write_part(o_ref, lse_ref, here, g, acc, total, lse):
    per_group = lse.shape[1] // BLK
    o_ref[here, g] = (acc * (1.0 / total)).astype(jnp.bfloat16)
    for r in range(per_group):
        head = g * per_group + r
        lse_ref[here, head : head + 1] = lse[:, r * BLK : (r + 1) * BLK]


def part_row(
    block,
    here,
    first_row,
    done,
    local_blocks,
    store_blocks,
    slot_ref,
    near_ref,
    count_ref,
    q_ref,
    sk_ref,
    sv_ref,
    k_ref,
    v_ref,
    o_ref,
    lse_ref,
    list_ref,
    acc_ref,
    max_ref,
    sum_ref,
):
    owner, inner = lax.div(block, local_blocks), lax.rem(block, local_blocks)
    me = lax.axis_index("seq")
    per_group = H // KVH
    kv_here = k_ref.shape[1] // DH
    rows = per_group * BLK
    listed = count_ref[owner, 0, inner]
    first_slot = me * store_blocks

    def scan_entries(i, found):
        places = [slot_ref[near_ref[owner, inner, i * SCAN + u]] - first_slot for u in range(SCAN)]
        for u, place in enumerate(places):
            list_ref[found] = place
            kept = (place >= 0) & (place < store_blocks) & (i * SCAN + u < listed)
            found = found + kept.astype(jnp.int32)
        return found

    found = lax.fori_loop(0, lax.div(listed + (SCAN - 1), SCAN), scan_entries, jnp.int32(0))
    home = owner == me
    if not done:

        @pl.when(jnp.logical_and(found == 0, jnp.logical_not(home)))
        def _():
            o_ref[here] = jnp.zeros(o_ref.shape[1:], o_ref.dtype)
            lse_ref[here] = jnp.full(lse_ref.shape[1:], NEG, lse_ref.dtype)

    @pl.when(found > done if done else jnp.logical_or(found > 0, home))
    def _():
        if done:
            for g in range(kv_here):
                max_ref[g : g + 1] = jnp.concatenate(
                    [
                        lse_ref[here, head : head + 1]
                        for head in range(g * per_group, (g + 1) * per_group)
                    ],
                    axis=1,
                )
                sum_ref[g : g + 1] = jnp.ones((1, rows), jnp.float32)
                acc_ref[g] = o_ref[here, g].astype(jnp.float32)
        else:

            @pl.when(home)
            def _():
                start = pl.multiple_of(inner * BLK, BLK)
                for g in range(kv_here):
                    cols = slice(g * DH, (g + 1) * DH)
                    asked = asked_rows(q_ref, first_row, g, per_group)
                    s = jnp.where(causal_mask(rows), scores_of(sk_ref[pl.ds(start, BLK), cols], asked), NEG)
                    m = jnp.max(s, axis=0, keepdims=True)
                    p = jnp.exp2(s - m)
                    max_ref[g : g + 1] = m
                    sum_ref[g : g + 1] = jnp.sum(p, axis=0, keepdims=True)
                    acc_ref[g] = weighed(sv_ref[pl.ds(start, BLK), cols], p)

            @pl.when(jnp.logical_not(home))
            def _():
                max_ref[...] = jnp.full_like(max_ref, NEG)
                sum_ref[...] = jnp.zeros_like(sum_ref)
                acc_ref[...] = jnp.zeros_like(acc_ref)

        def take(*places):
            starts = [pl.multiple_of(place * BLK, BLK) for place in places]

            def rows_of(ref, cols):
                return jnp.concatenate([ref[pl.ds(start, BLK), cols] for start in starts], axis=0)

            for g in range(kv_here):
                cols = slice(g * DH, (g + 1) * DH)
                s = scores_of(rows_of(k_ref, cols), asked_rows(q_ref, first_row, g, per_group))
                old = max_ref[g : g + 1]
                new = jnp.maximum(old, jnp.max(s, axis=0, keepdims=True))
                p = jnp.exp2(s - new)
                shrink = jnp.exp2(old - new)
                max_ref[g : g + 1] = new
                sum_ref[g : g + 1] = sum_ref[g : g + 1] * shrink + jnp.sum(p, axis=0, keepdims=True)
                acc_ref[g] = acc_ref[g] * shrink + weighed(rows_of(v_ref, cols), p)

        left = found - done

        @pl.loop(0, lax.div(left, 2))
        def _(i):
            take(list_ref[done + 2 * i], list_ref[done + 2 * i + 1])

        @pl.when(lax.rem(left, 2) == 1)
        def _():
            take(list_ref[found - 1])

        for g in range(kv_here):
            total = sum_ref[g : g + 1]
            write_part(o_ref, lse_ref, here, g, acc_ref[g], total, max_ref[g : g + 1] + jnp.log2(total))


def part_kernel(local_blocks, store_blocks, *refs):
    block = pl.program_id(0)
    part_row(block, 0, 0, 0, local_blocks, store_blocks, *refs)


def rest_kernel(local_blocks, store_blocks, *refs):
    def row(block, carry):
        first_row = pl.multiple_of(block * BLK, BLK)
        listed = refs[2][lax.div(block, local_blocks), 0, lax.rem(block, local_blocks)]

        @pl.when(listed > AHEAD)
        def _():
            part_row(block, block, first_row, AHEAD, local_blocks, store_blocks, *refs[:8], *refs[10:])

        return carry

    lax.fori_loop(0, refs[10].shape[0], row, 0)


def grant(*arrays):
    size = 0
    for shape, dtype in arrays:
        cells = 1
        for d in shape:
            cells = cells * d
        size += cells * jnp.dtype(dtype).itemsize
    return min(size + (4 << 20), 60 << 20)


def long_cost():
    return pl.CostEstimate(flops=200_000_000_000, bytes_accessed=1 << 20, transcendentals=0)


def ring_place(index, n):
    odd = lax.rem(index, 2)
    half = index // 2
    return (1 - odd) * half + odd * (n - 1 - half)


def ring_index(place, n):
    place = lax.rem(place + 2 * n, n)
    far = place // (n // 2)
    return (1 - far) * (2 * place) + far * (2 * (n - 1 - place) + 1)


def gather_kernel(n, pieces, early, *refs):
    refs = list(refs)

    def some(count):
        return [refs.pop(0) for _ in range(count)]

    x_ref, near_ref, count_ref = some(3)
    if early:
        slot_hbm, *store_hbm = some(5)
    out_ref, nears_ref, counts_ref = some(3)
    if early:
        o_ref, lse_ref, slot_ref, near_smem, count_smem, sk_ref, sv_ref, k_ref, v_ref, load_sem = some(10)
    own_sem, send_sem, recv_sem, tsend_sem, trecv_sem = refs
    me = lax.axis_index("seq")
    place = ring_place(me, n)
    rows = x_ref.shape[0]
    sub = rows // pieces
    half = n // 2
    ways = (1, -1)
    beside = [ring_index(place + way, n) for way in ways]
    own = [
        pltpu.make_async_copy(source, target, own_sem.at[i])
        for i, (source, target) in enumerate(
            (
                (x_ref, out_ref.at[pl.ds(pl.multiple_of(me * rows, rows), rows)]),
                (near_ref, nears_ref.at[me]),
                (count_ref, counts_ref.at[me]),
            )
        )
    ]
    for one in own:
        one.start()
    loads = []
    if early:
        sources = [slot_hbm] + store_hbm
        for i, (source, target) in enumerate(zip(sources, (slot_ref, sk_ref, sv_ref, k_ref, v_ref))):
            loads.append(pltpu.make_async_copy(source, target, load_sem.at[i]))
    for one in loads:
        one.start()
    barrier = pltpu.get_barrier_semaphore()
    for k in range(1, n):
        pl.semaphore_signal(barrier, inc=1, device_id={"seq": lax.rem(me + k, n)}, device_id_type=MESH)
    for one in own:
        one.wait()
    pl.semaphore_wait(barrier, n - 1)

    def copy(way, step, piece):
        owner = ring_index(place - ways[way] * step, n)
        there = pl.ds(pl.multiple_of(owner * rows + piece * sub, sub), sub)
        return pltpu.make_async_remote_copy(
            src_ref=out_ref.at[there],
            dst_ref=out_ref.at[there],
            send_sem=send_sem.at[way, step, piece],
            recv_sem=recv_sem.at[way, step, piece],
            device_id={"seq": beside[way]},
            device_id_type=MESH,
        )

    def piece_of(way, spot):
        return spot if way == 0 else pieces - 1 - spot

    table_copies = []
    for t, target in enumerate((nears_ref, counts_ref)):
        for k in range(1, n):
            table_copies.append(
                pltpu.make_async_remote_copy(
                    src_ref=target.at[me],
                    dst_ref=target.at[me],
                    send_sem=tsend_sem.at[t, k],
                    recv_sem=trecv_sem.at[t, k],
                    device_id={"seq": lax.rem(me + k, n)},
                    device_id_type=MESH,
                )
            )
    for one in table_copies:
        one.start()
    started = []
    for spot in range(pieces):
        for way in range(2):
            one = copy(way, 0, piece_of(way, spot))
            one.start()
            started.append(one)

    def first_listed(owner, inner):
        degree = near_ref.shape[1]
        store_blocks = k_ref.shape[0]
        listed = count_smem[owner, 0, inner]

        def look_past(before):
            def look(i, best):
                e = degree - SCAN * (i + 1)
                for u in range(SCAN - 1, -1, -1):
                    spot = slot_ref[near_smem[owner, inner, e + u]] - me * store_blocks
                    kept = (spot >= 0) & (spot < store_blocks) & (e + u < listed)
                    for other in before:
                        kept = kept & (spot != other)
                    best = best + kept.astype(jnp.int32) * (spot - best)
                return best

            return lax.fori_loop(0, degree // SCAN, look, jnp.int32(-1))

        found = []
        for _ in range(AHEAD):
            found.append(look_past(found))
        return found

    def row_work(owner, inner, spots, mine):
        per_group = H // KVH
        taken = [jnp.maximum(spot, 0) for spot in spots]
        missing = [jnp.minimum(spot, 0).astype(jnp.float32) * -NEG for spot in spots]
        first_row = pl.multiple_of(owner * rows + inner * BLK, BLK)
        for g in range(k_ref.shape[2] // DH):
            cols = slice(g * DH, (g + 1) * DH)
            asked = asked_rows(out_ref, first_row, g, per_group)
            keys = [k_ref[i, :, cols] for i in taken]
            values = [v_ref[i, :, cols] for i in taken]
            if mine:
                near = pl.ds(pl.multiple_of(inner * BLK, BLK), BLK)
                keys = [sk_ref[near, cols]] + keys
                values = [sv_ref[near, cols]] + values
            s = scores_of(jnp.concatenate(keys, axis=0), asked)
            cuts = [s[i * BLK : (i + 1) * BLK] for i in range(len(keys))]
            for i, lack in enumerate(missing):
                if mine or i > 0:
                    at = i + 1 if mine else i
                    cuts[at] = cuts[at] + lack
            if mine:
                cuts[0] = jnp.where(causal_mask(s.shape[1]), cuts[0], NEG)
            s = jnp.concatenate(cuts, axis=0)
            m = jnp.max(s, axis=0, keepdims=True)
            p = jnp.exp2(s - m)
            total = jnp.sum(p, axis=0, keepdims=True)
            lse = m + jnp.log2(total)
            if not mine:
                lse = lse + missing[0]
            write_part(
                o_ref, lse_ref, owner * pieces + inner, g, weighed(jnp.concatenate(values, axis=0), p), total, lse
            )

    def row_at(way, step, spot):
        return ring_index(place - ways[way] * step, n), piece_of(way, spot)

    def scanned(step, spot):
        return [first_listed(*row_at(way, step, spot)) for way in range(2)] if early else None

    def arrived(step, spot, found):
        if early:
            for way in range(2):
                row_work(*row_at(way, step, spot), found[way], False)

    def own_rows():
        for one in table_copies:
            one.wait_recv()
        tables = [
            pltpu.make_async_copy(source, target, load_sem.at[5 + i])
            for i, (source, target) in enumerate(((nears_ref, near_smem), (counts_ref, count_smem)))
        ]
        for one in tables:
            one.start()
        for one in loads + tables:
            one.wait()
        for inner in range(pieces):
            row_work(me, inner, first_listed(me, inner), True)

    for step in range(1, half):
        for spot in range(pieces):
            first = step == 1 and spot == 0
            found = None if first else scanned(step, spot)
            for way in range(2):
                copy(way, step - 1, piece_of(way, spot)).wait_recv()
                if step < half - 1 or spot < pieces // 2:
                    one = copy(way, step, piece_of(way, spot))
                    one.start()
                    started.append(one)
            if early and first:
                own_rows()
                found = scanned(step, spot)
            arrived(step, spot, found)
    for spot in range(pieces // 2):
        found = scanned(half, spot)
        for way in range(2):
            copy(way, half - 1, piece_of(way, spot)).wait_recv()
        arrived(half, spot, found)
    for one in started:
        one.wait_send()
    for one in table_copies:
        if early:
            one.wait_send()
        else:
            one.wait()


def gathered(x, near, count, n, early):
    rows, width = x.shape
    pieces = rows // BLK
    vmem = pl.BlockSpec(memory_space=pltpu.VMEM)
    dma = pltpu.SemaphoreType.DMA
    kind = pltpu.VMEM if early else jax.ShapeDtypeStruct
    inputs = [x, near, count] + list(early)
    out_shape = [
        kind((n * rows, width), x.dtype),
        jax.ShapeDtypeStruct((n,) + near.shape, near.dtype),
        jax.ShapeDtypeStruct((n,) + count.shape, count.dtype),
    ]
    scratch = []
    held = [((n + 1, rows, width), x.dtype)]
    if early:
        slot, *stores = early
        kv_here = stores[2].shape[2] // DH
        part_shape = (n * pieces, kv_here, BLK, (H // KVH) * DH)
        out_shape += [kind(part_shape, x.dtype), kind((n * pieces, kv_here * (H // KVH), BLK), jnp.float32)]
        scratch += [pltpu.SMEM(slot.shape, slot.dtype)]
        scratch += [pltpu.SMEM(out_shape[1].shape, near.dtype), pltpu.SMEM(out_shape[2].shape, count.dtype)]
        scratch += [pltpu.VMEM(a.shape, a.dtype) for a in stores]
        scratch += [dma((7,))]
        held += [(part_shape, x.dtype)] + [(a.shape, a.dtype) for a in stores]
    scratch += [
        dma((3,)),
        dma((2, n // 2, pieces)),
        dma((2, n // 2, pieces)),
        dma((2, n)),
        dma((2, n)),
    ]
    return pl.pallas_call(
        functools.partial(gather_kernel, n, pieces, bool(early)),
        in_specs=[pl.BlockSpec(memory_space=pltpu.HBM)] * len(inputs),
        out_specs=[vmem] * len(out_shape),
        out_shape=out_shape,
        scratch_shapes=scratch,
        compiler_params=pltpu.CompilerParams(
            collective_id=0,
            has_side_effects=True,
            vmem_limit_bytes=grant(*held),
        ),
        cost_estimate=long_cost(),
    )(*(pltpu.with_memory_space_constraint(a, pltpu.HBM) for a in inputs))


def merge(lse_a, lse_b):
    top = jnp.maximum(lse_a, lse_b)
    a = jnp.exp2(lse_a - top)
    b = jnp.exp2(lse_b - top)
    total = a + b
    return a / total, b / total, top + jnp.log2(total)


def reduce_kernel(
    n,
    small,
    o_ref,
    lse_ref,
    out_ref,
    got,
    got_lse,
    own,
    own_sem,
    send_sem,
    recv_sem,
    lsend_sem,
    lrecv_sem,
    ready=None,
):
    me = lax.axis_index("seq")
    place = ring_place(me, n)
    groups, width = got.shape[2], got.shape[4]
    wide = width // CUTS
    ways = (1, -1)
    beside = [ring_index(place + way, n) for way in ways]
    if ready is None:
        barrier = pltpu.get_barrier_semaphore()
        for other in beside:
            pl.semaphore_signal(barrier, inc=1, device_id={"seq": other}, device_id_type=MESH)

    def home(way, step):
        return ring_index(place - ways[way] * (1 + step), n)

    def fetch(way, step):
        return pltpu.make_async_copy(
            o_ref.at[home(way, step) * 2 + way], own.at[way, lax.rem(step, 2)], own_sem.at[way, lax.rem(step, 2)]
        )

    def lse_copy(way, step, before):
        return pltpu.make_async_remote_copy(
            src_ref=lse_ref.at[home(way, step) * 2 + way] if before is None else got_lse.at[way, before],
            dst_ref=got_lse.at[way, step],
            send_sem=lsend_sem.at[way, step],
            recv_sem=lrecv_sem.at[way, step],
            device_id={"seq": beside[way]},
            device_id_type=MESH,
        )

    def copy(way, step, g, cut, before):
        part = (g, slice(None), pl.ds(cut * wide, wide))
        return pltpu.make_async_remote_copy(
            src_ref=o_ref.at[(home(way, step) * 2 + way,) + part]
            if before is None
            else got.at[(way, before) + part],
            dst_ref=got.at[(way, step) + part],
            send_sem=send_sem.at[way, step, g * CUTS + cut],
            recv_sem=recv_sem.at[way, step, g * CUTS + cut],
            device_id={"seq": beside[way]},
            device_id_type=MESH,
        )

    def shares_of(way, step):
        lse_copy(way, step - 1, step - 1).wait_recv()
        if not small:
            fetch(way, step).wait()
        return merge(got_lse[way, step - 1], lse_ref[home(way, step) * 2 + way])

    def merged(way, step, g, cut, theirs, ours):
        copy(way, step - 1, g, cut, step - 1).wait_recv()
        at = home(way, step) * 2 + way
        columns = []
        for r in range(cut * wide // DH, (cut + 1) * wide // DH):
            cols = slice(r * DH, (r + 1) * DH)
            head = g * (width // DH) + r
            mine = o_ref[at, g, :, cols] if small else own[way, lax.rem(step, 2), g, :, cols]
            value = (
                got[way, step - 1, g, :, cols].astype(jnp.float32) * theirs[head : head + 1]
                + mine.astype(jnp.float32) * ours[head : head + 1]
            )
            columns.append((r, value))
        return columns

    if not small:
        for way in range(2):
            fetch(way, 1).start()
    if ready is None:
        pl.semaphore_wait(barrier, 2)
    for way in range(2):
        lse_copy(way, 0, None).start()
    for g in range(groups):
        for cut in range(CUTS):
            for way in range(2):
                copy(way, 0, g, cut, None).start()

    def one_step(step, carry):
        if not small:
            for way in range(2):
                fetch(way, step + 1).start()
        shares = []
        for way in range(2):
            theirs, ours, lse = shares_of(way, step)
            got_lse[way, step - 1] = lse
            lse_copy(way, step, step - 1).start()
            shares.append((theirs, ours))
        for g in range(groups):
            for cut in range(CUTS):
                for way in range(2):
                    for r, value in merged(way, step, g, cut, *shares[way]):
                        got[way, step - 1, g, :, r * DH : (r + 1) * DH] = value.astype(jnp.bfloat16)
                    copy(way, step, g, cut, step - 1).start()
        return carry

    lax.fori_loop(1, n - 1, one_step, 0)
    for way in range(2):
        theirs, ours, _ = shares_of(way, n - 1)
        for g in range(groups):
            for cut in range(CUTS):
                for r, value in merged(way, n - 1, g, cut, theirs, ours):
                    at = g * width + r * DH
                    out_ref[way * BLK : (way + 1) * BLK, at : at + DH] = jnp.transpose(value).astype(jnp.bfloat16)
        if ready is not None:
            ready(way)

    def drain_all():
        def drain(step, before):
            for way in range(2):
                lse_copy(way, step, before).wait_send()
                for g in range(groups):
                    for cut in range(CUTS):
                        copy(way, step, g, cut, before).wait_send()

        drain(0, None)
        lax.fori_loop(1, n - 1, lambda step, carry: (drain(step, step - 1), carry)[1], 0)

    if ready is None:
        drain_all()
    return drain_all


def project_stages(
    n,
    heads,
    joined,
    x_ref,
    w_hbm,
    out_ref,
    w_ref,
    blocks,
    split,
    got,
    summed,
    landed,
    w_sem,
    wsend,
    wrecv,
    send_sem,
    recv_sem,
    hsend,
    hrecv,
    fsend,
    frecv,
):
    me = lax.axis_index("seq")
    mine = lax.axis_index("head")
    line = n // 2
    at, side = me // 2, lax.rem(me, 2)
    share = x_ref.shape[0] // heads
    columns = w_ref.shape[2]
    ways = (1, -1)
    early = min(2, line - 1)
    weights = pltpu.make_async_copy(w_hbm, w_ref.at[0], w_sem.at[0])
    weights.start()
    barrier = pltpu.get_barrier_semaphore()
    place = ring_place(me, n)
    for way in ways:
        other = ring_index(place + way, n)
        pl.semaphore_signal(barrier, inc=1, device_id={"seq": other}, device_id_type=MESH)
    for k in range(1, heads):
        pl.semaphore_signal(barrier, inc=1, device_id={"head": lax.rem(mine + k, heads)}, device_id_type=MESH)
    partner = at * 2 + 1 - side
    if not joined:
        for k in range(1, line):
            other = lax.rem(at + k, line) * 2 + side
            pl.semaphore_signal(barrier, inc=1, device_id={"seq": other}, device_id_type=MESH)
        pl.semaphore_signal(barrier, inc=1, device_id={"seq": partner}, device_id_type=MESH)
    pl.semaphore_wait(barrier, heads + 1 if joined else heads + line + 1)

    def inside(spot):
        return jnp.logical_and(spot >= 0, spot < line)

    def copy(way, step, piece, first):
        there = (at - ways[way] * step, pl.ds(pl.multiple_of(piece * share, share), share))
        return pltpu.make_async_remote_copy(
            src_ref=x_ref.at[there[1]] if first else blocks.at[there],
            dst_ref=blocks.at[there],
            send_sem=send_sem.at[way, step, piece],
            recv_sem=recv_sem.at[way, step, piece],
            device_id={"seq": (at + ways[way]) * 2 + side},
            device_id_type=MESH,
        )

    def leaves(way, step):
        return jnp.logical_and(inside(at - ways[way] * step), inside(at + ways[way]))

    def to_head(i, j, source, to):
        return pltpu.make_async_remote_copy(
            src_ref=split.at[i, j, to],
            dst_ref=got.at[i, j, source],
            send_sem=hsend.at[i, j, to],
            recv_sem=hrecv.at[i, j, source],
            device_id={"head": to},
            device_id_type=MESH,
        )

    def to_row(i, j, source):
        owner = source * 2 + (side if j == 0 else 1 - side)
        return pltpu.make_async_remote_copy(
            src_ref=summed.at[i, j],
            dst_ref=landed.at[owner],
            send_sem=fsend.at[i, j],
            recv_sem=frecv.at[source, j],
            device_id={"seq": i * 2 + side},
            device_id_type=MESH,
        )

    def unit(i, c, js, own):
        rows = pl.ds(pl.multiple_of(c * share, share), share)
        value = x_ref[rows] if own else blocks[i, rows]
        for j in js:
            split[i, j, c] = jnp.dot(value, w_ref[j], preferred_element_type=jnp.float32).astype(jnp.bfloat16)

            @pl.when(mine != c)
            def _():
                to_head(i, j, mine, c).start()

    def visit(step, c, js, arriving):
        for way in range(2):
            i = at - ways[way] * step

            @pl.when(inside(i))
            def _():
                if arriving:
                    copy(way, step - 1, c, False).wait_recv()

                    @pl.when(inside(at + ways[way]))
                    def _():
                        copy(way, step, c, False).start()

                unit(i, c, js, False)

    def total_of(i, j):
        total = split[i, j, mine].astype(jnp.float32)
        for k in range(1, heads):
            source = lax.rem(mine + k, heads)
            to_head(i, j, source, mine).wait_recv()
            total = total + got[i, j, source].astype(jnp.float32)
        return total.astype(jnp.bfloat16)

    def settle_own(j):
        landed[at * 2 + (side if j == 0 else 1 - side)] = total_of(at, j)

    def settle(step, js):
        for way in range(2):
            i = at - ways[way] * step

            @pl.when(inside(i))
            def _():
                for j in js:
                    summed[i, j] = total_of(i, j)
                    to_row(i, j, at).start()

    def each(function):
        lax.fori_loop(0, heads, lambda c, carry: (function(c), carry)[1], 0)

    def start_own(c):
        for way in range(2):

            @pl.when(inside(at + ways[way]))
            def _():
                copy(way, 0, c, True).start()

    def run():
        weights.wait()
        exchange = pltpu.make_async_remote_copy(
            src_ref=w_ref.at[0],
            dst_ref=w_ref.at[1],
            send_sem=wsend.at[0],
            recv_sem=wrecv.at[0],
            device_id={"seq": partner},
            device_id_type=MESH,
        )
        exchange.start()
        each(lambda c: unit(at, c, (0,), True))

        def first_steps(step, carry):
            each(lambda c: visit(step, c, (0,), True))

            @pl.when(step == 1)
            def _():
                settle_own(0)

            @pl.when(step > 1)
            def _():
                settle(step - 1, (0,))

            return carry

        lax.fori_loop(1, early + 1, first_steps, 0)
        exchange.wait()
        each(lambda c: unit(at, c, (1,), True))
        lax.fori_loop(1, early + 1, lambda t, carry: (each(lambda c: visit(t, c, (1,), False)), carry)[1], 0)
        settle(early, (0,))

        def settle_early():
            settle_own(1)
            lax.fori_loop(1, early + 1, lambda t, carry: (settle(t, (1,)), carry)[1], 0)

        def late_step(step, carry):
            def late_visit(c):
                visit(step, c, (0, 1), True)

                @pl.when(jnp.logical_and(c == 0, step == early + 1))
                def _():
                    settle_early()

                @pl.when(jnp.logical_and(c == 0, step > early + 1))
                def _():
                    settle(step - 1, (0, 1))

                @pl.when(jnp.logical_and(mine == c - 1, step == line - 1))
                def _():
                    settle(step, (0, 1))

            each(late_visit)
            return carry

        if line - 1 > early:
            lax.fori_loop(early + 1, line, late_step, 0)

            @pl.when(mine == heads - 1)
            def _():
                settle(line - 1, (0, 1))

        else:
            settle_early()

        for way in range(2):
            for step in range(2):

                def finish(c):
                    @pl.when(leaves(way, step))
                    def _():
                        copy(way, step, c, step == 0).wait_send()

                if step == 0:
                    each(finish)
                else:

                    def finish_rest(t, carry):
                        def one(c):
                            @pl.when(leaves(way, t))
                            def _():
                                copy(way, t, c, False).wait_send()

                        each(one)
                        return carry

                    lax.fori_loop(1, line, finish_rest, 0)

        def drain(i, carry):
            for j in range(2):
                for k in range(1, heads):
                    to_head(i, j, mine, lax.rem(mine + k, heads)).wait_send()

                @pl.when(i != at)
                def _():
                    to_row(i, j, at).wait_send()
                    to_row(at, j, i).wait_recv()

            return carry

        lax.fori_loop(0, line, drain, 0)
        for i in range(n):
            out_ref[:, i * columns : (i + 1) * columns] = landed[i]

    return start_own, each, run


def project_kernel(n, heads, *refs):
    start_own, each, run = project_stages(n, heads, False, *refs)
    each(start_own)
    run()


def join_kernel(n, heads, o_ref, lse_ref, w_hbm, out_ref, x_ref, *refs):
    start_own, _, run = project_stages(n, heads, True, x_ref, w_hbm, out_ref, *refs[8:])
    per_way = BLK * heads // x_ref.shape[0]

    def ready(way):
        for c in range(per_way):
            start_own(way * per_way + c)

    drain = reduce_kernel(n, True, o_ref, lse_ref, x_ref, *refs[:8], ready=ready)
    run()
    drain()


def project_plan(n, heads, rows, width, columns, dtype):
    share = rows // heads
    line = n // 2
    dma = pltpu.SemaphoreType.DMA
    scratch = [
        pltpu.VMEM((2, width, columns), dtype),
        pltpu.VMEM((line, rows, width), dtype),
        pltpu.VMEM((line, 2, heads, share, columns), dtype),
        pltpu.VMEM((line, 2, heads, share, columns), dtype),
        pltpu.VMEM((line, 2, share, columns), dtype),
        pltpu.VMEM((n, share, columns), dtype),
        dma((1,)),
        dma((1,)),
        dma((1,)),
        dma((2, line, heads)),
        dma((2, line, heads)),
        dma((line, 2, heads)),
        dma((line, 2, heads)),
        dma((line, 2)),
        dma((line, 2)),
    ]
    padded = max(columns, BLK)
    held = [
        ((2, width, padded), dtype),
        ((line + 2, rows, width), dtype),
        ((2, n, heads, share, padded), dtype),
        ((3, n, share, padded), dtype),
    ]
    return scratch, held


def reduce_plan(n, small, kv_here, group_width):
    heads_here = kv_here * (H // KVH)
    dma = pltpu.SemaphoreType.DMA((2, n - 1))
    dma_cuts = pltpu.SemaphoreType.DMA((2, n - 1, kv_here * CUTS))
    scratch = [
        pltpu.VMEM((2, n - 1, kv_here, BLK, group_width), jnp.bfloat16),
        pltpu.VMEM((2, n - 1, heads_here, BLK), jnp.float32),
        pltpu.VMEM((2, 2, 1 if small else kv_here, BLK, group_width), jnp.bfloat16),
        pltpu.SemaphoreType.DMA((2, 2)),
        dma_cuts,
        dma_cuts,
        dma,
        dma,
    ]
    held = [
        ((2, n + 1, kv_here, BLK, group_width), jnp.bfloat16),
        ((2, 2 * n - 1, heads_here, BLK), jnp.float32),
    ]
    return scratch, held


def mixed_from(parts, lse, weight, n, heads, rows, width, small):
    _, kv_here, _, group_width = parts.shape
    columns = weight.shape[1]
    vmem = pl.BlockSpec(memory_space=pltpu.VMEM)
    anywhere = pl.BlockSpec(memory_space=pl.ANY)
    reduce_scratch, reduce_held = reduce_plan(n, small, kv_here, group_width)
    project_scratch, project_held = project_plan(n, heads, rows, width, columns, parts.dtype)
    attended = jax.ShapeDtypeStruct((rows, width), parts.dtype)
    out = jax.ShapeDtypeStruct((rows // heads, n * columns), parts.dtype)

    def call(kernel, number, in_specs, out_shape, scratch, held):
        return pl.pallas_call(
            kernel,
            in_specs=in_specs,
            out_specs=vmem,
            out_shape=out_shape,
            scratch_shapes=scratch,
            compiler_params=pltpu.CompilerParams(
                collective_id=number, has_side_effects=True, vmem_limit_bytes=grant(*held)
            ),
            cost_estimate=long_cost(),
        )

    if small:
        scratch = [pltpu.VMEM((rows, width), parts.dtype)] + reduce_scratch + project_scratch
        held = reduce_held + project_held + [(parts.shape, parts.dtype)]
        kernel = functools.partial(join_kernel, n, heads)
        return call(kernel, 1, [vmem, vmem, anywhere], out, scratch, held)(parts, lse, weight)

    def kernel(*refs):
        reduce_kernel(n, small, *refs)

    x = call(kernel, 1, [anywhere, vmem], attended, reduce_scratch, reduce_held)(parts, lse)
    kernel = functools.partial(project_kernel, n, heads)
    return call(kernel, 2, [vmem, anywhere], out, project_scratch, project_held)(x, weight)


def body(
    queries,
    self_keys,
    self_values,
    store_keys,
    store_values,
    kv_slot,
    neighbours,
    counts,
    out_weight,
):
    n = lax.axis_size("seq")
    head_count = lax.axis_size("head")
    local_blocks, degree = neighbours.shape
    local_rows, width = queries.shape
    store_blocks = store_keys.shape[0] // BLK
    all_blocks = local_blocks * n
    kv_here = store_keys.shape[1] // DH
    group_width = (H // KVH) * DH
    rows = (H // KVH) * BLK
    small = queries.size * n * queries.dtype.itemsize <= 8 << 20
    count_row = counts.reshape(1, local_blocks)
    stores = (self_keys, self_values, store_keys, store_values)
    cut = tuple(a.reshape(store_blocks, BLK, -1) for a in stores[2:])
    smem = pl.BlockSpec(memory_space=pltpu.SMEM)
    vmem = pl.BlockSpec(memory_space=pltpu.VMEM)
    params = pltpu.CompilerParams(vmem_limit_bytes=28 << 20)
    cost = pl.CostEstimate(flops=2_000_000_000, bytes_accessed=12 << 20, transcendentals=4_000_000)
    scratch = [
        pltpu.SMEM((degree + 1,), jnp.int32),
        pltpu.VMEM((kv_here, DH, rows), jnp.float32),
        pltpu.VMEM((kv_here, rows), jnp.float32),
        pltpu.VMEM((kv_here, rows), jnp.float32),
    ]
    part_shape = (all_blocks, kv_here, BLK, group_width)
    lse_shape = (all_blocks, kv_here * (H // KVH), BLK)
    if small:
        all_queries, near, count, parts, lse = gathered(queries, neighbours, count_row, n, (kv_slot,) + stores[:2] + cut)
        parts, lse = pl.pallas_call(
            functools.partial(rest_kernel, local_blocks, store_blocks),
            in_specs=[smem] * 3 + [vmem] * 7,
            out_specs=[vmem, vmem],
            out_shape=[pltpu.VMEM(part_shape, jnp.bfloat16), pltpu.VMEM(lse_shape, jnp.float32)],
            scratch_shapes=scratch,
            input_output_aliases={8: 0, 9: 1},
            compiler_params=params,
            cost_estimate=cost,
        )(kv_slot, near, count, all_queries, *stores, parts, lse)
    else:
        all_queries, near, count = gathered(queries, neighbours, count_row, n, ())
        parts, lse = pl.pallas_call(
            functools.partial(part_kernel, local_blocks, store_blocks),
            grid=(all_blocks,),
            in_specs=[smem] * 3 + [pl.BlockSpec((BLK, width), lambda i: (i, 0))] + [vmem] * 4,
            out_specs=[
                pl.BlockSpec((1, kv_here, BLK, group_width), lambda i: (i, 0, 0, 0)),
                pl.BlockSpec((1, kv_here * (H // KVH), BLK), lambda i: (i, 0, 0)),
            ],
            out_shape=[
                jax.ShapeDtypeStruct(part_shape, jnp.bfloat16),
                jax.ShapeDtypeStruct(lse_shape, jnp.float32),
            ],
            scratch_shapes=scratch,
            compiler_params=params,
            cost_estimate=cost,
        )(kv_slot, near, count, all_queries, *stores)
    return mixed_from(parts, lse, out_weight, n, head_count, local_rows, width, small)


def solution(mesh):
    placed = (
        P("seq", "head"),
        P("seq", "head"),
        P("seq", "head"),
        P("seq", "head"),
        P("seq", "head"),
        P(),
        P("seq", None),
        P("seq"),
        P("head", "seq"),
    )
    return jax.shard_map(
        body, mesh=mesh, in_specs=placed, out_specs=P(("seq", "head"), None), check_vma=False
    )
```

```python
import functools

import jax
import jax.numpy as jnp
from jax import lax
from jax.experimental import pallas as pl
from jax.experimental.pallas import tpu as pltpu
from jax.sharding import PartitionSpec as P

H = 32
KVH = 8
DH = 128
BLK = 128
NEG = -1e30
SCAN = 4
AHEAD = 2
CUTS = 1
LOG2E = 1.4426950408889634
MESH = pl.DeviceIdType.MESH


def asked_rows(q_ref, first_row, g, per_group):
    return jnp.concatenate(
        [
            q_ref[pl.ds(first_row, BLK), (g * per_group + r) * DH : (g * per_group + r + 1) * DH]
            for r in range(per_group)
        ],
        axis=0,
    )


def scores_of(keys, asked):
    scaling = DH ** (-0.5) * LOG2E
    return lax.dot_general(keys, asked, (((1,), (1,)), ((), ())), preferred_element_type=jnp.float32) * scaling


def weighed(values, p):
    return lax.dot_general(
        values, p.astype(jnp.bfloat16), (((0,), (0,)), ((), ())), preferred_element_type=jnp.float32
    )


def causal_mask(rows):
    position = lax.rem(lax.broadcasted_iota(jnp.int32, (BLK, rows), 1), BLK)
    return position >= lax.broadcasted_iota(jnp.int32, (BLK, rows), 0)


def write_part(o_ref, lse_ref, here, g, acc, total, lse):
    per_group = lse.shape[1] // BLK
    o_ref[here, g] = (acc * (1.0 / total)).astype(jnp.bfloat16)
    for r in range(per_group):
        head = g * per_group + r
        lse_ref[here, head : head + 1] = lse[:, r * BLK : (r + 1) * BLK]


def part_row(
    block,
    here,
    first_row,
    done,
    local_blocks,
    store_blocks,
    slot_ref,
    near_ref,
    count_ref,
    q_ref,
    sk_ref,
    sv_ref,
    k_ref,
    v_ref,
    o_ref,
    lse_ref,
    list_ref,
    acc_ref,
    max_ref,
    sum_ref,
):
    owner, inner = lax.div(block, local_blocks), lax.rem(block, local_blocks)
    me = lax.axis_index("seq")
    per_group = H // KVH
    kv_here = k_ref.shape[1] // DH
    rows = per_group * BLK
    listed = count_ref[owner, 0, inner]
    first_slot = me * store_blocks

    def scan_entries(i, found):
        places = [slot_ref[near_ref[owner, inner, i * SCAN + u]] - first_slot for u in range(SCAN)]
        for u, place in enumerate(places):
            list_ref[found] = place
            kept = (place >= 0) & (place < store_blocks) & (i * SCAN + u < listed)
            found = found + kept.astype(jnp.int32)
        return found

    found = lax.fori_loop(0, lax.div(listed + (SCAN - 1), SCAN), scan_entries, jnp.int32(0))
    home = owner == me
    if not done:

        @pl.when(jnp.logical_and(found == 0, jnp.logical_not(home)))
        def _():
            o_ref[here] = jnp.zeros(o_ref.shape[1:], o_ref.dtype)
            lse_ref[here] = jnp.full(lse_ref.shape[1:], NEG, lse_ref.dtype)

    @pl.when(found > done if done else jnp.logical_or(found > 0, home))
    def _():
        if done:
            for g in range(kv_here):
                max_ref[g : g + 1] = jnp.concatenate(
                    [
                        lse_ref[here, head : head + 1]
                        for head in range(g * per_group, (g + 1) * per_group)
                    ],
                    axis=1,
                )
                sum_ref[g : g + 1] = jnp.ones((1, rows), jnp.float32)
                acc_ref[g] = o_ref[here, g].astype(jnp.float32)
        else:

            @pl.when(home)
            def _():
                start = pl.multiple_of(inner * BLK, BLK)
                for g in range(kv_here):
                    cols = slice(g * DH, (g + 1) * DH)
                    asked = asked_rows(q_ref, first_row, g, per_group)
                    s = jnp.where(causal_mask(rows), scores_of(sk_ref[pl.ds(start, BLK), cols], asked), NEG)
                    m = jnp.max(s, axis=0, keepdims=True)
                    p = jnp.exp2(s - m)
                    max_ref[g : g + 1] = m
                    sum_ref[g : g + 1] = jnp.sum(p, axis=0, keepdims=True)
                    acc_ref[g] = weighed(sv_ref[pl.ds(start, BLK), cols], p)

            @pl.when(jnp.logical_not(home))
            def _():
                max_ref[...] = jnp.full_like(max_ref, NEG)
                sum_ref[...] = jnp.zeros_like(sum_ref)
                acc_ref[...] = jnp.zeros_like(acc_ref)

        def take(*places):
            starts = [pl.multiple_of(place * BLK, BLK) for place in places]

            def rows_of(ref, cols):
                return jnp.concatenate([ref[pl.ds(start, BLK), cols] for start in starts], axis=0)

            for g in range(kv_here):
                cols = slice(g * DH, (g + 1) * DH)
                s = scores_of(rows_of(k_ref, cols), asked_rows(q_ref, first_row, g, per_group))
                old = max_ref[g : g + 1]
                new = jnp.maximum(old, jnp.max(s, axis=0, keepdims=True))
                p = jnp.exp2(s - new)
                shrink = jnp.exp2(old - new)
                max_ref[g : g + 1] = new
                sum_ref[g : g + 1] = sum_ref[g : g + 1] * shrink + jnp.sum(p, axis=0, keepdims=True)
                acc_ref[g] = acc_ref[g] * shrink + weighed(rows_of(v_ref, cols), p)

        left = found - done

        @pl.loop(0, lax.div(left, 2))
        def _(i):
            take(list_ref[done + 2 * i], list_ref[done + 2 * i + 1])

        @pl.when(lax.rem(left, 2) == 1)
        def _():
            take(list_ref[found - 1])

        for g in range(kv_here):
            total = sum_ref[g : g + 1]
            write_part(o_ref, lse_ref, here, g, acc_ref[g], total, max_ref[g : g + 1] + jnp.log2(total))


def part_kernel(local_blocks, store_blocks, *refs):
    block = pl.program_id(0)
    part_row(block, 0, 0, 0, local_blocks, store_blocks, *refs)


def rest_kernel(local_blocks, store_blocks, *refs):
    def row(block, carry):
        first_row = pl.multiple_of(block * BLK, BLK)
        listed = refs[2][lax.div(block, local_blocks), 0, lax.rem(block, local_blocks)]

        @pl.when(listed > AHEAD)
        def _():
            part_row(block, block, first_row, AHEAD, local_blocks, store_blocks, *refs[:8], *refs[10:])

        return carry

    lax.fori_loop(0, refs[10].shape[0], row, 0)


def grant(*arrays):
    size = 0
    for shape, dtype in arrays:
        cells = 1
        for d in shape:
            cells = cells * d
        size += cells * jnp.dtype(dtype).itemsize
    return min(size + (4 << 20), 60 << 20)


def long_cost():
    return pl.CostEstimate(flops=200_000_000_000, bytes_accessed=1 << 20, transcendentals=0)


def ring_place(index, n):
    odd = lax.rem(index, 2)
    half = index // 2
    return (1 - odd) * half + odd * (n - 1 - half)


def ring_index(place, n):
    place = lax.rem(place + 2 * n, n)
    far = place // (n // 2)
    return (1 - far) * (2 * place) + far * (2 * (n - 1 - place) + 1)


def gather_kernel(n, pieces, early, *refs):
    refs = list(refs)

    def some(count):
        return [refs.pop(0) for _ in range(count)]

    x_ref, near_ref, count_ref = some(3)
    if early:
        slot_hbm, *store_hbm = some(5)
    out_ref, nears_ref, counts_ref = some(3)
    if early:
        o_ref, lse_ref, slot_ref, near_smem, count_smem, sk_ref, sv_ref, k_ref, v_ref, load_sem = some(10)
    own_sem, send_sem, recv_sem, tsend_sem, trecv_sem = refs
    me = lax.axis_index("seq")
    place = ring_place(me, n)
    rows = x_ref.shape[0]
    sub = rows // pieces
    half = n // 2
    ways = (1, -1)
    beside = [ring_index(place + way, n) for way in ways]
    own = [
        pltpu.make_async_copy(source, target, own_sem.at[i])
        for i, (source, target) in enumerate(
            (
                (x_ref, out_ref.at[pl.ds(pl.multiple_of(me * rows, rows), rows)]),
                (near_ref, nears_ref.at[me]),
                (count_ref, counts_ref.at[me]),
            )
        )
    ]
    for one in own:
        one.start()
    loads = []
    if early:
        sources = [slot_hbm] + store_hbm
        for i, (source, target) in enumerate(zip(sources, (slot_ref, sk_ref, sv_ref, k_ref, v_ref))):
            loads.append(pltpu.make_async_copy(source, target, load_sem.at[i]))
    for one in loads:
        one.start()
    barrier = pltpu.get_barrier_semaphore()
    for k in range(1, n):
        pl.semaphore_signal(barrier, inc=1, device_id={"seq": lax.rem(me + k, n)}, device_id_type=MESH)
    for one in own:
        one.wait()
    pl.semaphore_wait(barrier, n - 1)

    def copy(way, step, piece):
        owner = ring_index(place - ways[way] * step, n)
        there = pl.ds(pl.multiple_of(owner * rows + piece * sub, sub), sub)
        return pltpu.make_async_remote_copy(
            src_ref=out_ref.at[there],
            dst_ref=out_ref.at[there],
            send_sem=send_sem.at[way, step, piece],
            recv_sem=recv_sem.at[way, step, piece],
            device_id={"seq": beside[way]},
            device_id_type=MESH,
        )

    def piece_of(way, spot):
        return spot if way == 0 else pieces - 1 - spot

    table_copies = []
    for t, target in enumerate((nears_ref, counts_ref)):
        for k in range(1, n):
            table_copies.append(
                pltpu.make_async_remote_copy(
                    src_ref=target.at[me],
                    dst_ref=target.at[me],
                    send_sem=tsend_sem.at[t, k],
                    recv_sem=trecv_sem.at[t, k],
                    device_id={"seq": lax.rem(me + k, n)},
                    device_id_type=MESH,
                )
            )
    for one in table_copies:
        one.start()
    started = []
    for spot in range(pieces):
        for way in range(2):
            one = copy(way, 0, piece_of(way, spot))
            one.start()
            started.append(one)

    def first_listed(owner, inner):
        degree = near_ref.shape[1]
        store_blocks = k_ref.shape[0]
        listed = count_smem[owner, 0, inner]

        def look_past(before):
            def look(i, best):
                e = degree - SCAN * (i + 1)
                for u in range(SCAN - 1, -1, -1):
                    spot = slot_ref[near_smem[owner, inner, e + u]] - me * store_blocks
                    kept = (spot >= 0) & (spot < store_blocks) & (e + u < listed)
                    for other in before:
                        kept = kept & (spot != other)
                    best = best + kept.astype(jnp.int32) * (spot - best)
                return best

            return lax.fori_loop(0, degree // SCAN, look, jnp.int32(-1))

        found = []
        for _ in range(AHEAD):
            found.append(look_past(found))
        return found

    def row_work(owner, inner, spots, mine):
        per_group = H // KVH
        taken = [jnp.maximum(spot, 0) for spot in spots]
        missing = [jnp.minimum(spot, 0).astype(jnp.float32) * -NEG for spot in spots]
        first_row = pl.multiple_of(owner * rows + inner * BLK, BLK)
        for g in range(k_ref.shape[2] // DH):
            cols = slice(g * DH, (g + 1) * DH)
            asked = asked_rows(out_ref, first_row, g, per_group)
            keys = [k_ref[i, :, cols] for i in taken]
            values = [v_ref[i, :, cols] for i in taken]
            if mine:
                near = pl.ds(pl.multiple_of(inner * BLK, BLK), BLK)
                keys = [sk_ref[near, cols]] + keys
                values = [sv_ref[near, cols]] + values
            s = scores_of(jnp.concatenate(keys, axis=0), asked)
            cuts = [s[i * BLK : (i + 1) * BLK] for i in range(len(keys))]
            for i, lack in enumerate(missing):
                if mine or i > 0:
                    at = i + 1 if mine else i
                    cuts[at] = cuts[at] + lack
            if mine:
                cuts[0] = jnp.where(causal_mask(s.shape[1]), cuts[0], NEG)
            s = jnp.concatenate(cuts, axis=0)
            m = jnp.max(s, axis=0, keepdims=True)
            p = jnp.exp2(s - m)
            total = jnp.sum(p, axis=0, keepdims=True)
            lse = m + jnp.log2(total)
            if not mine:
                lse = lse + missing[0]
            write_part(
                o_ref, lse_ref, owner * pieces + inner, g, weighed(jnp.concatenate(values, axis=0), p), total, lse
            )

    def row_at(way, step, spot):
        return ring_index(place - ways[way] * step, n), piece_of(way, spot)

    def scanned(step, spot):
        return [first_listed(*row_at(way, step, spot)) for way in range(2)] if early else None

    def arrived(step, spot, found):
        if early:
            for way in range(2):
                row_work(*row_at(way, step, spot), found[way], False)

    def own_rows():
        for one in table_copies:
            one.wait_recv()
        tables = [
            pltpu.make_async_copy(source, target, load_sem.at[5 + i])
            for i, (source, target) in enumerate(((nears_ref, near_smem), (counts_ref, count_smem)))
        ]
        for one in tables:
            one.start()
        for one in loads + tables:
            one.wait()
        for inner in range(pieces):
            row_work(me, inner, first_listed(me, inner), True)

    for step in range(1, half):
        for spot in range(pieces):
            first = step == 1 and spot == 0
            found = None if first else scanned(step, spot)
            for way in range(2):
                copy(way, step - 1, piece_of(way, spot)).wait_recv()
                if step < half - 1 or spot < pieces // 2:
                    one = copy(way, step, piece_of(way, spot))
                    one.start()
                    started.append(one)
            if early and first:
                own_rows()
                found = scanned(step, spot)
            arrived(step, spot, found)
    for spot in range(pieces // 2):
        found = scanned(half, spot)
        for way in range(2):
            copy(way, half - 1, piece_of(way, spot)).wait_recv()
            if early:
                row_work(*row_at(way, half, spot), found[way], False)
    for one in started:
        one.wait_send()
    for one in table_copies:
        if early:
            one.wait_send()
        else:
            one.wait()


def gathered(x, near, count, n, early):
    rows, width = x.shape
    pieces = rows // BLK
    vmem = pl.BlockSpec(memory_space=pltpu.VMEM)
    dma = pltpu.SemaphoreType.DMA
    kind = pltpu.VMEM if early else jax.ShapeDtypeStruct
    inputs = [x, near, count] + list(early)
    out_shape = [
        kind((n * rows, width), x.dtype),
        jax.ShapeDtypeStruct((n,) + near.shape, near.dtype),
        jax.ShapeDtypeStruct((n,) + count.shape, count.dtype),
    ]
    scratch = []
    held = [((n + 1, rows, width), x.dtype)]
    if early:
        slot, *stores = early
        kv_here = stores[2].shape[2] // DH
        part_shape = (n * pieces, kv_here, BLK, (H // KVH) * DH)
        out_shape += [kind(part_shape, x.dtype), kind((n * pieces, kv_here * (H // KVH), BLK), jnp.float32)]
        scratch += [pltpu.SMEM(slot.shape, slot.dtype)]
        scratch += [pltpu.SMEM(out_shape[1].shape, near.dtype), pltpu.SMEM(out_shape[2].shape, count.dtype)]
        scratch += [pltpu.VMEM(a.shape, a.dtype) for a in stores]
        scratch += [dma((7,))]
        held += [(part_shape, x.dtype)] + [(a.shape, a.dtype) for a in stores]
    scratch += [
        dma((3,)),
        dma((2, n // 2, pieces)),
        dma((2, n // 2, pieces)),
        dma((2, n)),
        dma((2, n)),
    ]
    return pl.pallas_call(
        functools.partial(gather_kernel, n, pieces, bool(early)),
        in_specs=[pl.BlockSpec(memory_space=pltpu.HBM)] * len(inputs),
        out_specs=[vmem] * len(out_shape),
        out_shape=out_shape,
        scratch_shapes=scratch,
        compiler_params=pltpu.CompilerParams(
            collective_id=0,
            has_side_effects=True,
            vmem_limit_bytes=grant(*held),
        ),
        cost_estimate=long_cost(),
    )(*(pltpu.with_memory_space_constraint(a, pltpu.HBM) for a in inputs))


def merge(lse_a, lse_b):
    top = jnp.maximum(lse_a, lse_b)
    a = jnp.exp2(lse_a - top)
    b = jnp.exp2(lse_b - top)
    total = a + b
    return a / total, b / total, top + jnp.log2(total)


def reduce_kernel(
    n,
    small,
    o_ref,
    lse_ref,
    out_ref,
    got,
    got_lse,
    own,
    own_sem,
    send_sem,
    recv_sem,
    lsend_sem,
    lrecv_sem,
    ready=None,
):
    me = lax.axis_index("seq")
    place = ring_place(me, n)
    groups, width = got.shape[2], got.shape[4]
    wide = width // CUTS
    ways = (1, -1)
    beside = [ring_index(place + way, n) for way in ways]
    if ready is None:
        barrier = pltpu.get_barrier_semaphore()
        for other in beside:
            pl.semaphore_signal(barrier, inc=1, device_id={"seq": other}, device_id_type=MESH)

    def home(way, step):
        return ring_index(place - ways[way] * (1 + step), n)

    def fetch(way, step):
        return pltpu.make_async_copy(
            o_ref.at[home(way, step) * 2 + way], own.at[way, lax.rem(step, 2)], own_sem.at[way, lax.rem(step, 2)]
        )

    def lse_copy(way, step, before):
        return pltpu.make_async_remote_copy(
            src_ref=lse_ref.at[home(way, step) * 2 + way] if before is None else got_lse.at[way, before],
            dst_ref=got_lse.at[way, step],
            send_sem=lsend_sem.at[way, step],
            recv_sem=lrecv_sem.at[way, step],
            device_id={"seq": beside[way]},
            device_id_type=MESH,
        )

    def copy(way, step, g, cut, before):
        part = (g, slice(None), pl.ds(cut * wide, wide))
        return pltpu.make_async_remote_copy(
            src_ref=o_ref.at[(home(way, step) * 2 + way,) + part]
            if before is None
            else got.at[(way, before) + part],
            dst_ref=got.at[(way, step) + part],
            send_sem=send_sem.at[way, step, g * CUTS + cut],
            recv_sem=recv_sem.at[way, step, g * CUTS + cut],
            device_id={"seq": beside[way]},
            device_id_type=MESH,
        )

    def shares_of(way, step):
        lse_copy(way, step - 1, step - 1).wait_recv()
        if not small:
            fetch(way, step).wait()
        return merge(got_lse[way, step - 1], lse_ref[home(way, step) * 2 + way])

    def merged(way, step, g, cut, theirs, ours):
        copy(way, step - 1, g, cut, step - 1).wait_recv()
        at = home(way, step) * 2 + way
        columns = []
        for r in range(cut * wide // DH, (cut + 1) * wide // DH):
            cols = slice(r * DH, (r + 1) * DH)
            head = g * (width // DH) + r
            mine = o_ref[at, g, :, cols] if small else own[way, lax.rem(step, 2), g, :, cols]
            value = (
                got[way, step - 1, g, :, cols].astype(jnp.float32) * theirs[head : head + 1]
                + mine.astype(jnp.float32) * ours[head : head + 1]
            )
            columns.append((r, value))
        return columns

    if not small:
        for way in range(2):
            fetch(way, 1).start()
    if ready is None:
        pl.semaphore_wait(barrier, 2)
    for way in range(2):
        lse_copy(way, 0, None).start()
    for g in range(groups):
        for cut in range(CUTS):
            for way in range(2):
                copy(way, 0, g, cut, None).start()

    def one_step(step, carry):
        if not small:
            for way in range(2):
                fetch(way, step + 1).start()
        shares = []
        for way in range(2):
            theirs, ours, lse = shares_of(way, step)
            got_lse[way, step - 1] = lse
            lse_copy(way, step, step - 1).start()
            shares.append((theirs, ours))
        for g in range(groups):
            for cut in range(CUTS):
                for way in range(2):
                    for r, value in merged(way, step, g, cut, *shares[way]):
                        got[way, step - 1, g, :, r * DH : (r + 1) * DH] = value.astype(jnp.bfloat16)
                    copy(way, step, g, cut, step - 1).start()
        return carry

    lax.fori_loop(1, n - 1, one_step, 0)
    for way in range(2):
        theirs, ours, _ = shares_of(way, n - 1)
        for g in range(groups):
            for cut in range(CUTS):
                for r, value in merged(way, n - 1, g, cut, theirs, ours):
                    at = g * width + r * DH
                    out_ref[way * BLK : (way + 1) * BLK, at : at + DH] = jnp.transpose(value).astype(jnp.bfloat16)
        if ready is not None:
            ready(way)

    def drain_all():
        def drain(step, before):
            for way in range(2):
                lse_copy(way, step, before).wait_send()
                for g in range(groups):
                    for cut in range(CUTS):
                        copy(way, step, g, cut, before).wait_send()

        drain(0, None)
        lax.fori_loop(1, n - 1, lambda step, carry: (drain(step, step - 1), carry)[1], 0)

    if ready is None:
        drain_all()
    return drain_all


def project_stages(
    n,
    heads,
    joined,
    x_ref,
    w_hbm,
    out_ref,
    w_ref,
    blocks,
    split,
    got,
    summed,
    landed,
    w_sem,
    wsend,
    wrecv,
    send_sem,
    recv_sem,
    hsend,
    hrecv,
    fsend,
    frecv,
):
    me = lax.axis_index("seq")
    mine = lax.axis_index("head")
    line = n // 2
    at, side = me // 2, lax.rem(me, 2)
    share = x_ref.shape[0] // heads
    columns = w_ref.shape[2]
    ways = (1, -1)
    early = min(2, line - 1)
    weights = pltpu.make_async_copy(w_hbm, w_ref.at[0], w_sem.at[0])
    weights.start()
    barrier = pltpu.get_barrier_semaphore()
    place = ring_place(me, n)
    for way in ways:
        other = ring_index(place + way, n)
        pl.semaphore_signal(barrier, inc=1, device_id={"seq": other}, device_id_type=MESH)
    for k in range(1, heads):
        pl.semaphore_signal(barrier, inc=1, device_id={"head": lax.rem(mine + k, heads)}, device_id_type=MESH)
    partner = at * 2 + 1 - side
    if not joined:
        for k in range(1, line):
            other = lax.rem(at + k, line) * 2 + side
            pl.semaphore_signal(barrier, inc=1, device_id={"seq": other}, device_id_type=MESH)
        pl.semaphore_signal(barrier, inc=1, device_id={"seq": partner}, device_id_type=MESH)
    pl.semaphore_wait(barrier, heads + 1 if joined else heads + line + 1)

    def inside(spot):
        return jnp.logical_and(spot >= 0, spot < line)

    def copy(way, step, piece, first):
        there = (at - ways[way] * step, pl.ds(pl.multiple_of(piece * share, share), share))
        return pltpu.make_async_remote_copy(
            src_ref=x_ref.at[there[1]] if first else blocks.at[there],
            dst_ref=blocks.at[there],
            send_sem=send_sem.at[way, step, piece],
            recv_sem=recv_sem.at[way, step, piece],
            device_id={"seq": (at + ways[way]) * 2 + side},
            device_id_type=MESH,
        )

    def leaves(way, step):
        return jnp.logical_and(inside(at - ways[way] * step), inside(at + ways[way]))

    def to_head(i, j, source, to):
        return pltpu.make_async_remote_copy(
            src_ref=split.at[i, j, to],
            dst_ref=got.at[i, j, source],
            send_sem=hsend.at[i, j, to],
            recv_sem=hrecv.at[i, j, source],
            device_id={"head": to},
            device_id_type=MESH,
        )

    def to_row(i, j, source):
        owner = source * 2 + (side if j == 0 else 1 - side)
        return pltpu.make_async_remote_copy(
            src_ref=summed.at[i, j],
            dst_ref=landed.at[owner],
            send_sem=fsend.at[i, j],
            recv_sem=frecv.at[source, j],
            device_id={"seq": i * 2 + side},
            device_id_type=MESH,
        )

    def unit(i, c, js, own):
        rows = pl.ds(pl.multiple_of(c * share, share), share)
        value = x_ref[rows] if own else blocks[i, rows]
        for j in js:
            split[i, j, c] = jnp.dot(value, w_ref[j], preferred_element_type=jnp.float32).astype(jnp.bfloat16)

            @pl.when(mine != c)
            def _():
                to_head(i, j, mine, c).start()

    def visit(step, c, js, arriving):
        for way in range(2):
            i = at - ways[way] * step

            @pl.when(inside(i))
            def _():
                if arriving:
                    copy(way, step - 1, c, False).wait_recv()

                    @pl.when(inside(at + ways[way]))
                    def _():
                        copy(way, step, c, False).start()

                unit(i, c, js, False)

    def total_of(i, j):
        total = split[i, j, mine].astype(jnp.float32)
        for k in range(1, heads):
            source = lax.rem(mine + k, heads)
            to_head(i, j, source, mine).wait_recv()
            total = total + got[i, j, source].astype(jnp.float32)
        return total.astype(jnp.bfloat16)

    def settle_own(j):
        landed[at * 2 + (side if j == 0 else 1 - side)] = total_of(at, j)

    def settle(step, js):
        for way in range(2):
            i = at - ways[way] * step

            @pl.when(inside(i))
            def _():
                for j in js:
                    summed[i, j] = total_of(i, j)
                    to_row(i, j, at).start()

    def each(function):
        lax.fori_loop(0, heads, lambda c, carry: (function(c), carry)[1], 0)

    def start_own(c):
        for way in range(2):

            @pl.when(inside(at + ways[way]))
            def _():
                copy(way, 0, c, True).start()

    def run():
        weights.wait()
        exchange = pltpu.make_async_remote_copy(
            src_ref=w_ref.at[0],
            dst_ref=w_ref.at[1],
            send_sem=wsend.at[0],
            recv_sem=wrecv.at[0],
            device_id={"seq": partner},
            device_id_type=MESH,
        )
        exchange.start()
        each(lambda c: unit(at, c, (0,), True))

        def first_steps(step, carry):
            each(lambda c: visit(step, c, (0,), True))

            @pl.when(step == 1)
            def _():
                settle_own(0)

            @pl.when(step > 1)
            def _():
                settle(step - 1, (0,))

            return carry

        lax.fori_loop(1, early + 1, first_steps, 0)
        exchange.wait()
        each(lambda c: unit(at, c, (1,), True))
        lax.fori_loop(1, early + 1, lambda t, carry: (each(lambda c: visit(t, c, (1,), False)), carry)[1], 0)
        settle(early, (0,))

        def settle_early():
            settle_own(1)
            lax.fori_loop(1, early + 1, lambda t, carry: (settle(t, (1,)), carry)[1], 0)

        def late_step(step, carry):
            def late_visit(c):
                visit(step, c, (0, 1), True)

                @pl.when(jnp.logical_and(c == 0, step == early + 1))
                def _():
                    settle_early()

                @pl.when(jnp.logical_and(c == 0, step > early + 1))
                def _():
                    settle(step - 1, (0, 1))

                @pl.when(jnp.logical_and(mine == c - 1, step == line - 1))
                def _():
                    settle(step, (0, 1))

            each(late_visit)
            return carry

        if line - 1 > early:
            lax.fori_loop(early + 1, line, late_step, 0)

            @pl.when(mine == heads - 1)
            def _():
                settle(line - 1, (0, 1))

        else:
            settle_early()

        for way in range(2):
            for step in range(2):

                def finish(c):
                    @pl.when(leaves(way, step))
                    def _():
                        copy(way, step, c, step == 0).wait_send()

                if step == 0:
                    each(finish)
                else:

                    def finish_rest(t, carry):
                        def one(c):
                            @pl.when(leaves(way, t))
                            def _():
                                copy(way, t, c, False).wait_send()

                        each(one)
                        return carry

                    lax.fori_loop(1, line, finish_rest, 0)

        def drain(i, carry):
            for j in range(2):
                for k in range(1, heads):
                    to_head(i, j, mine, lax.rem(mine + k, heads)).wait_send()

                @pl.when(i != at)
                def _():
                    to_row(i, j, at).wait_send()
                    to_row(at, j, i).wait_recv()

            return carry

        lax.fori_loop(0, line, drain, 0)
        for i in range(n):
            out_ref[:, i * columns : (i + 1) * columns] = landed[i]

    return start_own, each, run


def project_kernel(n, heads, *refs):
    start_own, each, run = project_stages(n, heads, False, *refs)
    each(start_own)
    run()


def join_kernel(n, heads, o_ref, lse_ref, w_hbm, out_ref, x_ref, *refs):
    start_own, _, run = project_stages(n, heads, True, x_ref, w_hbm, out_ref, *refs[8:])
    per_way = BLK * heads // x_ref.shape[0]

    def ready(way):
        for c in range(per_way):
            start_own(way * per_way + c)

    drain = reduce_kernel(n, True, o_ref, lse_ref, x_ref, *refs[:8], ready=ready)
    run()
    drain()


def project_plan(n, heads, rows, width, columns, dtype):
    share = rows // heads
    line = n // 2
    dma = pltpu.SemaphoreType.DMA
    scratch = [
        pltpu.VMEM((2, width, columns), dtype),
        pltpu.VMEM((line, rows, width), dtype),
        pltpu.VMEM((line, 2, heads, share, columns), dtype),
        pltpu.VMEM((line, 2, heads, share, columns), dtype),
        pltpu.VMEM((line, 2, share, columns), dtype),
        pltpu.VMEM((n, share, columns), dtype),
        dma((1,)),
        dma((1,)),
        dma((1,)),
        dma((2, line, heads)),
        dma((2, line, heads)),
        dma((line, 2, heads)),
        dma((line, 2, heads)),
        dma((line, 2)),
        dma((line, 2)),
    ]
    padded = max(columns, BLK)
    held = [
        ((2, width, padded), dtype),
        ((line + 2, rows, width), dtype),
        ((2, n, heads, share, padded), dtype),
        ((3, n, share, padded), dtype),
    ]
    return scratch, held


def reduce_plan(n, small, kv_here, group_width):
    heads_here = kv_here * (H // KVH)
    dma = pltpu.SemaphoreType.DMA((2, n - 1))
    dma_cuts = pltpu.SemaphoreType.DMA((2, n - 1, kv_here * CUTS))
    scratch = [
        pltpu.VMEM((2, n - 1, kv_here, BLK, group_width), jnp.bfloat16),
        pltpu.VMEM((2, n - 1, heads_here, BLK), jnp.float32),
        pltpu.VMEM((2, 2, 1 if small else kv_here, BLK, group_width), jnp.bfloat16),
        pltpu.SemaphoreType.DMA((2, 2)),
        dma_cuts,
        dma_cuts,
        dma,
        dma,
    ]
    held = [
        ((2, n + 1, kv_here, BLK, group_width), jnp.bfloat16),
        ((2, 2 * n - 1, heads_here, BLK), jnp.float32),
    ]
    return scratch, held


def mixed_from(parts, lse, weight, n, heads, rows, width, small):
    _, kv_here, _, group_width = parts.shape
    columns = weight.shape[1]
    vmem = pl.BlockSpec(memory_space=pltpu.VMEM)
    anywhere = pl.BlockSpec(memory_space=pl.ANY)
    reduce_scratch, reduce_held = reduce_plan(n, small, kv_here, group_width)
    project_scratch, project_held = project_plan(n, heads, rows, width, columns, parts.dtype)
    attended = jax.ShapeDtypeStruct((rows, width), parts.dtype)
    out = jax.ShapeDtypeStruct((rows // heads, n * columns), parts.dtype)

    def call(kernel, number, in_specs, out_shape, scratch, held):
        return pl.pallas_call(
            kernel,
            in_specs=in_specs,
            out_specs=vmem,
            out_shape=out_shape,
            scratch_shapes=scratch,
            compiler_params=pltpu.CompilerParams(
                collective_id=number, has_side_effects=True, vmem_limit_bytes=grant(*held)
            ),
            cost_estimate=long_cost(),
        )

    if small:
        scratch = [pltpu.VMEM((rows, width), parts.dtype)] + reduce_scratch + project_scratch
        held = reduce_held + project_held + [(parts.shape, parts.dtype)]
        kernel = functools.partial(join_kernel, n, heads)
        return call(kernel, 1, [vmem, vmem, anywhere], out, scratch, held)(parts, lse, weight)

    def kernel(*refs):
        reduce_kernel(n, small, *refs)

    x = call(kernel, 1, [anywhere, vmem], attended, reduce_scratch, reduce_held)(parts, lse)
    kernel = functools.partial(project_kernel, n, heads)
    return call(kernel, 2, [vmem, anywhere], out, project_scratch, project_held)(x, weight)


def body(
    queries,
    self_keys,
    self_values,
    store_keys,
    store_values,
    kv_slot,
    neighbours,
    counts,
    out_weight,
):
    n = lax.axis_size("seq")
    head_count = lax.axis_size("head")
    local_blocks, degree = neighbours.shape
    local_rows, width = queries.shape
    store_blocks = store_keys.shape[0] // BLK
    all_blocks = local_blocks * n
    kv_here = store_keys.shape[1] // DH
    group_width = (H // KVH) * DH
    rows = (H // KVH) * BLK
    small = queries.size * n * queries.dtype.itemsize <= 8 << 20
    count_row = counts.reshape(1, local_blocks)
    stores = (self_keys, self_values, store_keys, store_values)
    cut = tuple(a.reshape(store_blocks, BLK, -1) for a in stores[2:])
    smem = pl.BlockSpec(memory_space=pltpu.SMEM)
    vmem = pl.BlockSpec(memory_space=pltpu.VMEM)
    params = pltpu.CompilerParams(vmem_limit_bytes=28 << 20)
    cost = pl.CostEstimate(flops=2_000_000_000, bytes_accessed=12 << 20, transcendentals=4_000_000)
    scratch = [
        pltpu.SMEM((degree + 1,), jnp.int32),
        pltpu.VMEM((kv_here, DH, rows), jnp.float32),
        pltpu.VMEM((kv_here, rows), jnp.float32),
        pltpu.VMEM((kv_here, rows), jnp.float32),
    ]
    part_shape = (all_blocks, kv_here, BLK, group_width)
    lse_shape = (all_blocks, kv_here * (H // KVH), BLK)
    if small:
        all_queries, near, count, parts, lse = gathered(queries, neighbours, count_row, n, (kv_slot,) + stores[:2] + cut)
        parts, lse = pl.pallas_call(
            functools.partial(rest_kernel, local_blocks, store_blocks),
            in_specs=[smem] * 3 + [vmem] * 7,
            out_specs=[vmem, vmem],
            out_shape=[pltpu.VMEM(part_shape, jnp.bfloat16), pltpu.VMEM(lse_shape, jnp.float32)],
            scratch_shapes=scratch,
            input_output_aliases={8: 0, 9: 1},
            compiler_params=params,
            cost_estimate=cost,
        )(kv_slot, near, count, all_queries, *stores, parts, lse)
    else:
        all_queries, near, count = gathered(queries, neighbours, count_row, n, ())
        parts, lse = pl.pallas_call(
            functools.partial(part_kernel, local_blocks, store_blocks),
            grid=(all_blocks,),
            in_specs=[smem] * 3 + [pl.BlockSpec((BLK, width), lambda i: (i, 0))] + [vmem] * 4,
            out_specs=[
                pl.BlockSpec((1, kv_here, BLK, group_width), lambda i: (i, 0, 0, 0)),
                pl.BlockSpec((1, kv_here * (H // KVH), BLK), lambda i: (i, 0, 0)),
            ],
            out_shape=[
                jax.ShapeDtypeStruct(part_shape, jnp.bfloat16),
                jax.ShapeDtypeStruct(lse_shape, jnp.float32),
            ],
            scratch_shapes=scratch,
            compiler_params=params,
            cost_estimate=cost,
        )(kv_slot, near, count, all_queries, *stores)
    return mixed_from(parts, lse, out_weight, n, head_count, local_rows, width, small)


def solution(mesh):
    placed = (
        P("seq", "head"),
        P("seq", "head"),
        P("seq", "head"),
        P("seq", "head"),
        P("seq", "head"),
        P(),
        P("seq", None),
        P("seq"),
        P("head", "seq"),
    )
    return jax.shard_map(
        body, mesh=mesh, in_specs=placed, out_specs=P(("seq", "head"), None), check_vma=False
    )
```
